128 devices in a mesh: col: 2 (over core), row: 64 (over z, y, x).
Axes of the slice: x: 4, y: 4, z: 4, core: 2. Of those that a mesh axis runs over, the one named last changes fastest.
Arguments:
- f_rhs: float32 [1536, 48, 512], P('row', 'col')
- u_init: float32 [1536, 48, 512], P('row', 'col')
- kappa_cell: float32 [1536, 48], P('row', 'col')
- solve_mats: bfloat16 [64, 2, 576, 900], P('row', 'col')
- omega_relax: float32 [], replicated
Outputs:
- output: float32 [1536, 48, 512], P('row', 'col')
All inputs are finite; a program needn't handle non-finite values.
Results may differ from the reference program's by a relative error of at most 0.00135554.
Values are sent between devices in bfloat16 or wider.
A program may use at most 1 GiB of HBM per device.

```python
import jax
import jax.numpy as jnp
from jax import lax

SUB_SIZE = 24
MARGIN = 3
RHS_COUNT = 512
ROW_BLOCKS = 64
COL_BLOCKS = 2
SWEEPS = 6

EXT_SIZE = SUB_SIZE + 2 * MARGIN
GRID_ROWS = SUB_SIZE * ROW_BLOCKS
GRID_COLS = SUB_SIZE * COL_BLOCKS


def face_coeffs(kappa_cell):
    inner_v = 0.5 * (kappa_cell[1:, :] + kappa_cell[:-1, :])
    inner_h = 0.5 * (kappa_cell[:, 1:] + kappa_cell[:, :-1])
    face_n = jnp.concatenate([kappa_cell[:1, :], inner_v], axis=0)
    face_s = jnp.concatenate([inner_v, kappa_cell[-1:, :]], axis=0)
    face_w = jnp.concatenate([kappa_cell[:, :1], inner_h], axis=1)
    face_e = jnp.concatenate([inner_h, kappa_cell[:, -1:]], axis=1)
    return face_n, face_s, face_w, face_e


def apply_operator(values, face_set):
    face_n, face_s, face_w, face_e = face_set
    padded = jnp.pad(values, ((1, 1), (1, 1), (0, 0)))
    diag_sum = (face_n + face_s + face_w + face_e)[:, :, None]
    return (diag_sum * values
            - face_n[:, :, None] * padded[:-2, 1:-1]
            - face_s[:, :, None] * padded[2:, 1:-1]
            - face_w[:, :, None] * padded[1:-1, :-2]
            - face_e[:, :, None] * padded[1:-1, 2:])


def build_solve_mats(kappa_cell):
    face_n, face_s, face_w, face_e = face_coeffs(kappa_cell)
    diag_sum = face_n + face_s + face_w + face_e
    link_s = jnp.concatenate([face_s[:-1, :], jnp.zeros((1, GRID_COLS), jnp.float32)], axis=0)
    link_e = jnp.concatenate([face_e[:, :-1], jnp.zeros((GRID_ROWS, 1), jnp.float32)], axis=1)
    pad_cfg = ((MARGIN, MARGIN), (MARGIN, MARGIN))
    diag_pad = jnp.pad(diag_sum, pad_cfg, constant_values=1.0)
    south_pad = jnp.pad(link_s, pad_cfg)
    east_pad = jnp.pad(link_e, pad_cfg)
    ext_cells = EXT_SIZE * EXT_SIZE
    col_mask = (jnp.arange(EXT_SIZE) < EXT_SIZE - 1).astype(jnp.float32)

    def one_block(block_idx):
        corner_at = (block_idx // COL_BLOCKS * SUB_SIZE, block_idx % COL_BLOCKS * SUB_SIZE)
        diag_w = lax.dynamic_slice(diag_pad, corner_at, (EXT_SIZE, EXT_SIZE)).reshape(ext_cells)
        south_w = lax.dynamic_slice(south_pad, corner_at, (EXT_SIZE, EXT_SIZE)).reshape(ext_cells)
        east_w = (lax.dynamic_slice(east_pad, corner_at, (EXT_SIZE, EXT_SIZE)) * col_mask[None, :]).reshape(ext_cells)
        local_op = (jnp.diag(diag_w)
                    - jnp.diag(east_w[:-1], 1) - jnp.diag(east_w[:-1], -1)
                    - jnp.diag(south_w[:-EXT_SIZE], EXT_SIZE) - jnp.diag(south_w[:-EXT_SIZE], -EXT_SIZE))
        inverse = jnp.linalg.inv(local_op).reshape(EXT_SIZE, EXT_SIZE, ext_cells)
        rows_kept = inverse[MARGIN:MARGIN + SUB_SIZE, MARGIN:MARGIN + SUB_SIZE]
        return rows_kept.reshape(SUB_SIZE * SUB_SIZE, ext_cells)

    all_mats = lax.map(one_block, jnp.arange(ROW_BLOCKS * COL_BLOCKS))
    return all_mats.reshape(ROW_BLOCKS, COL_BLOCKS, SUB_SIZE * SUB_SIZE, ext_cells).astype(jnp.bfloat16)


def setup_inputs(seed: int = 0) -> dict:
    root_key = jax.random.key(seed)
    key_rhs, key_init, key_coef, key_omega = jax.random.split(root_key, 4)
    rhs_scale = 16.0 / (EXT_SIZE * EXT_SIZE)
    grid_shape = (GRID_ROWS, GRID_COLS, RHS_COUNT)
    f_rhs = rhs_scale * (1.0 + jax.random.normal(key_rhs, grid_shape, jnp.float32))
    u_init = jax.random.normal(key_init, grid_shape, jnp.float32)
    kappa_cell = jnp.exp(jax.random.uniform(key_coef, (GRID_ROWS, GRID_COLS), jnp.float32, -0.8, 0.8))
    omega_relax = jax.random.uniform(key_omega, (), jnp.float32, 0.7, 1.0)
    return dict(f_rhs=f_rhs, u_init=u_init, kappa_cell=kappa_cell,
                solve_mats=build_solve_mats(kappa_cell), omega_relax=omega_relax)


def local_solves(residual, solve_mats):
    padded = jnp.pad(residual.astype(jnp.bfloat16), ((MARGIN, MARGIN), (MARGIN, MARGIN), (0, 0)))

    def one_block(block_idx):
        blk_row = block_idx // COL_BLOCKS
        blk_col = block_idx % COL_BLOCKS
        window = lax.dynamic_slice(padded, (blk_row * SUB_SIZE, blk_col * SUB_SIZE, 0),
                                   (EXT_SIZE, EXT_SIZE, RHS_COUNT))
        product = jnp.dot(solve_mats[blk_row, blk_col], window.reshape(EXT_SIZE * EXT_SIZE, RHS_COUNT),
                          preferred_element_type=jnp.float32)
        return product.astype(jnp.bfloat16)

    blocks = lax.map(one_block, jnp.arange(ROW_BLOCKS * COL_BLOCKS))
    blocks = blocks.reshape(ROW_BLOCKS, COL_BLOCKS, SUB_SIZE, SUB_SIZE, RHS_COUNT)
    return blocks.transpose(0, 2, 1, 3, 4).reshape(GRID_ROWS, GRID_COLS, RHS_COUNT)


def reference(f_rhs, u_init, kappa_cell, solve_mats, omega_relax):
    face_set = face_coeffs(kappa_cell)
    residual = f_rhs - apply_operator(u_init, face_set)

    def one_sweep(state_pair, unused):
        u_cur, res_cur = state_pair
        correction = local_solves(res_cur, solve_mats).astype(jnp.float32)
        u_next = u_cur + omega_relax * correction
        res_next = res_cur - omega_relax * apply_operator(correction, face_set)
        return (u_next, res_next), None

    final_pair, unused_out = lax.scan(one_sweep, (u_init, residual), None, length=SWEEPS)
    return final_pair[0]
```

```python
import functools
import math

import jax
import jax.numpy as jnp
from jax import lax
from jax.experimental import pallas as pl
from jax.experimental.pallas import tpu as pltpu
from jax.sharding import PartitionSpec as P

SWEEPS = 6
LANES = 128
MESH = pl.DeviceIdType.MESH
F32 = jnp.float32
BF16 = jnp.bfloat16


def kernel(row_count, sub, halo, chunks,
           om_ref, f_hbm, u_hbm, kap_hbm, mat_hbm, out_hbm,
           u_sc, r_sc, v_sc, e_late, e_early, acc, m_raw, m_perm,
           k_raw, kb, fv, fw, fe, dg, i_send, i_recv, z_send, z_recv,
           load_sem, pair_send, pair_recv, mat_sem, kap_loc, kap_send, kap_recv,
           is_sem, ir_sem, zs_sem, zr_sem, out_loc, out_send, out_recv):
    wide = 2 * sub
    ext = sub + 2 * halo
    band = halo + 1
    late_k = 2 * band * 32
    early_rows = e_early.shape[1]
    half = chunks * LANES
    left = 8

    row = lax.axis_index('row')
    col = lax.axis_index('col')
    other = 1 - col
    has_up = row > 0
    has_dn = row < row_count - 1
    up_row = jnp.maximum(row - 1, 0)
    dn_row = jnp.minimum(row + 1, row_count - 1)
    my_cols = pl.ds(pl.multiple_of(col * sub, 8), sub)
    other_cols = pl.ds(pl.multiple_of(other * sub, 8), sub)

    def lanes_of(which, ch):
        return pl.ds(pl.multiple_of(which * half + ch * LANES, LANES), LANES)

    barrier = pltpu.get_barrier_semaphore()

    def greet(r_to, c_to):
        pl.semaphore_signal(barrier, inc=1, device_id=(c_to, r_to), device_id_type=MESH)

    greet(row, other)

    @pl.when(has_up)
    def _():
        greet(up_row, col)
        greet(up_row, other)

    @pl.when(has_dn)
    def _():
        greet(dn_row, col)
        greet(dn_row, other)

    own_rows = pl.ds(halo, sub)

    def u_load(ch):
        return pltpu.make_async_copy(u_hbm.at[:, :, lanes_of(col, ch)], u_sc.at[ch, :, my_cols, :], load_sem.at[0, ch])

    def f_load(ch):
        return pltpu.make_async_copy(f_hbm.at[:, :, lanes_of(col, ch)], r_sc.at[ch, own_rows, my_cols, :],
                                     load_sem.at[1, ch])

    mat_load = pltpu.make_async_copy(mat_hbm.at[0, 0], m_raw.at[col], mat_sem)
    kap_load = pltpu.make_async_copy(kap_hbm, k_raw.at[1, col], kap_loc)
    kap_load.start()
    for ch in range(chunks):
        u_load(ch).start()
        f_load(ch).start()
    mat_load.start()

    def u_pair(ch):
        return pltpu.make_async_remote_copy(
            src_ref=u_hbm.at[:, :, lanes_of(other, ch)], dst_ref=u_sc.at[ch, :, my_cols, :],
            send_sem=pair_send.at[0, ch], recv_sem=pair_recv.at[0, ch],
            device_id=(other, row), device_id_type=MESH)

    def u_pair_in(ch):
        return pltpu.make_async_remote_copy(
            src_ref=u_hbm.at[:, :, lanes_of(other, ch)], dst_ref=u_sc.at[ch, :, other_cols, :],
            send_sem=pair_send.at[0, ch], recv_sem=pair_recv.at[0, ch],
            device_id=(other, row), device_id_type=MESH)

    def f_pair(ch, cols):
        return pltpu.make_async_remote_copy(
            src_ref=f_hbm.at[:, :, lanes_of(other, ch)], dst_ref=r_sc.at[ch, own_rows, cols, :],
            send_sem=pair_send.at[1, ch], recv_sem=pair_recv.at[1, ch],
            device_id=(other, row), device_id_type=MESH)

    def mat_pair(slot):
        return pltpu.make_async_remote_copy(
            src_ref=mat_hbm.at[0, 0], dst_ref=m_raw.at[slot],
            send_sem=pair_send.at[2, 0], recv_sem=pair_recv.at[2, 0],
            device_id=(other, row), device_id_type=MESH)

    def kap_copy(band_slot, col_slot, sem_slot, r_to, c_to):
        return pltpu.make_async_remote_copy(
            src_ref=kap_hbm, dst_ref=k_raw.at[band_slot, col_slot],
            send_sem=kap_send.at[sem_slot], recv_sem=kap_recv.at[sem_slot],
            device_id=(c_to, r_to), device_id_type=MESH)

    for ch in range(chunks):
        def clear(i, carry):
            v_sc[ch, i] = jnp.zeros(v_sc.shape[2:], F32)
            return carry
        lax.fori_loop(0, ext + 2, clear, 0)
        e_early[ch, sub - 2:early_rows] = jnp.zeros((early_rows - sub + 2, wide, LANES), BF16)
    omega = om_ref[0]

    pl.semaphore_wait(barrier, 1 + 2 * has_up.astype(jnp.int32) + 2 * has_dn.astype(jnp.int32))

    kap_copy(1, col, 0, row, other).start()
    for ch in range(chunks):
        u_pair(ch).start()
        f_pair(ch, my_cols).start()

    @pl.when(has_up)
    def _():
        kap_copy(2, col, 1, up_row, col).start()
        kap_copy(2, col, 2, up_row, other).start()

    @pl.when(has_dn)
    def _():
        kap_copy(0, col, 3, dn_row, col).start()
        kap_copy(0, col, 4, dn_row, other).start()

    mat_pair(col).start()

    eye = lax.broadcasted_iota(jnp.int32, (sub, sub), 0) == lax.broadcasted_iota(jnp.int32, (sub, sub), 1)

    def spread_row(slot, k_row, at):
        parts = []
        for side in range(2):
            line = k_raw[slot, side, pl.ds(k_row, 1), :]
            picked = jnp.where(eye, jnp.broadcast_to(line, (sub, sub)), 0.0)
            column = jnp.sum(picked, axis=1, keepdims=True)
            parts.append(jnp.broadcast_to(column, (sub, LANES)))
        kb[at, left:left + sub] = parts[0]
        kb[at, left + sub:left + wide] = parts[1]
        kb[at, left - 1:left] = parts[0][0:1]
        kb[at, left + wide:left + wide + 1] = parts[1][sub - 1:sub]

    def side_faces(e):
        k_mid = kb[e + 1, left:left + wide]
        fw[e] = 0.5 * (k_mid + kb[e + 1, left - 1:left + wide - 1])
        fe[e] = 0.5 * (kb[e + 1, left + 1:left + wide + 1] + k_mid)

    def diag_row(e):
        dg[e] = fv[e] + fv[e + 1] + fw[e] + fe[e]

    def face_row(i):
        fv[i] = 0.5 * (kb[i + 1, left:left + wide] + kb[i, left:left + wide])

    kap_load.wait()
    kap_copy(1, other, 0, row, other).wait_recv()

    def own_spread(i, carry):
        spread_row(1, i, i + band)
        return carry
    lax.fori_loop(0, sub, own_spread, 0)

    fv[halo] = jnp.zeros((wide, LANES), F32)
    fv[halo + sub] = jnp.zeros((wide, LANES), F32)

    def own_face(i, carry):
        face_row(i)
        return carry
    lax.fori_loop(halo + 1, halo + sub, own_face, 0)

    def own_side(e, carry):
        side_faces(e)
        diag_row(e)
        return carry
    lax.fori_loop(halo, halo + sub, own_side, 0)

    def stencil(ch, e, n):
        rows = pl.ds(e, n)
        mid = pl.ds(e + 1, n)
        return (dg[rows] * v_sc[ch, mid, left:left + wide]
                - fv[rows] * v_sc[ch, pl.ds(e, n), left:left + wide]
                - fv[mid] * v_sc[ch, pl.ds(e + 2, n), left:left + wide]
                - fw[rows] * v_sc[ch, mid, left - 1:left + wide - 1]
                - fe[rows] * v_sc[ch, mid, left + 1:left + wide + 1])

    def init_copy(way, ch, r_to):
        return pltpu.make_async_remote_copy(
            src_ref=i_send.at[way, ch], dst_ref=i_recv.at[way, ch],
            send_sem=is_sem.at[way, ch], recv_sem=ir_sem.at[way, ch],
            device_id=(col, r_to), device_id_type=MESH)

    def first_residual(ch, carry):
        u_load(ch).wait()
        f_load(ch).wait()
        u_pair_in(ch).wait_recv()
        f_pair(ch, other_cols).wait_recv()

        def fill(i, c):
            v_sc[ch, i + band, left:left + wide] = u_sc[ch, i]
            return c
        lax.fori_loop(0, sub, fill, 0)

        def part(e0, n):
            r_sc[ch, pl.ds(e0, n)] = r_sc[ch, pl.ds(e0, n)] - stencil(ch, e0, n)

        part(halo, halo)
        i_send[0, ch, 0:halo] = r_sc[ch, halo:2 * halo]
        i_send[0, ch, halo] = u_sc[ch, 0]

        @pl.when(has_up)
        def _():
            init_copy(0, ch, up_row).start()
        part(sub, halo)
        i_send[1, ch, 0:halo] = r_sc[ch, sub:sub + halo]
        i_send[1, ch, halo] = u_sc[ch, sub - 1]

        @pl.when(has_dn)
        def _():
            init_copy(1, ch, dn_row).start()

        def middle(i, c):
            part(2 * halo + i * halo, halo)
            return c
        lax.fori_loop(0, (sub - 2 * halo) // halo, middle, 0)

        def to_e(i, c):
            e_early[ch, i] = r_sc[ch, i + band].astype(BF16)
            return c
        lax.fori_loop(0, sub - 2, to_e, 0)
        return carry

    lax.fori_loop(0, chunks, first_residual, 0)

    mat_load.wait()
    mat_pair(other).wait_recv()
    ext_cells = m_raw.shape[2]
    tile = 256
    spot = lax.broadcasted_iota(jnp.int32, (ext_cells, tile), 0)

    def permute(n_tile, carry):
        n_at = n_tile * tile + lax.broadcasted_iota(jnp.int32, (1, tile), 1)
        q = lax.shift_right_logical(n_at, 5)
        j = lax.bitwise_and(n_at, 31)
        line = jnp.where(q < band, q, jnp.where(q < 2 * band, q + (ext - 2 * band), q - band))
        out_at = pl.ds(pl.multiple_of(n_tile * tile, tile), tile)
        for side in range(2):
            ext_col = j + halo - 8 * side
            ok = (q < ext) & (ext_col >= 0) & (ext_col < ext)
            want = jnp.where(ok, line * ext + ext_col, -1)
            pick = jnp.where(spot == want, 1.0, 0.0).astype(BF16)
            moved = jnp.dot(m_raw[side], pick, preferred_element_type=F32)
            m_perm[side, :, out_at] = moved.astype(BF16)
        return carry
    lax.fori_loop(0, m_perm.shape[2] // tile, permute, 0)

    def early_dot(ch):
        for side in range(2):
            operand = e_early[ch, :, 16 * side:16 * side + 32, :].reshape(early_rows * 32, LANES)
            acc[ch, side] = jnp.dot(m_perm[side, :, late_k:late_k + early_rows * 32], operand,
                                    preferred_element_type=F32)

    def first_early(ch, carry):
        early_dot(ch)
        return carry
    lax.fori_loop(0, chunks, first_early, 0)

    @pl.when(has_up)
    def _():
        kap_copy(0, col, 3, row, other).wait_recv()
        kap_copy(0, other, 4, row, other).wait_recv()

        def spread(i, c):
            spread_row(0, sub - band + i, i)
            return c
        lax.fori_loop(0, band, spread, 0)

    @pl.when(jnp.logical_not(has_up))
    def _():
        for i in range(band):
            kb[i] = kb[band]

    @pl.when(has_dn)
    def _():
        kap_copy(2, col, 1, row, other).wait_recv()
        kap_copy(2, other, 2, row, other).wait_recv()

        def spread(i, c):
            spread_row(2, i, band + sub + i)
            return c
        lax.fori_loop(0, band, spread, 0)

    @pl.when(jnp.logical_not(has_dn))
    def _():
        for i in range(band):
            kb[band + sub + i] = kb[band + sub - 1]

    for i in range(halo + 1):
        face_row(i)
        face_row(halo + sub + i)
    for i in range(halo):
        side_faces(i)
        side_faces(halo + sub + i)
    for i in range(halo + 1):
        diag_row(i)
        diag_row(ext - 1 - i)

    def late_e(ch):
        e_late[ch, 0:band] = r_sc[ch, 0:band].astype(BF16)
        e_late[ch, band:2 * band] = r_sc[ch, ext - band:ext].astype(BF16)

    def late_first(ch):
        @pl.when(has_up)
        def _():
            init_copy(1, ch, up_row).wait_recv()
            r_sc[ch, 0:halo] = i_recv[1, ch, 0:halo]

        @pl.when(jnp.logical_not(has_up))
        def _():
            i_recv[1, ch, halo] = jnp.zeros((wide, LANES), F32)
            r_sc[ch, 0:halo] = jnp.zeros((halo, wide, LANES), F32)

        @pl.when(has_dn)
        def _():
            init_copy(0, ch, dn_row).wait_recv()
            r_sc[ch, halo + sub:ext] = i_recv[0, ch, 0:halo]

        @pl.when(jnp.logical_not(has_dn))
        def _():
            i_recv[0, ch, halo] = jnp.zeros((wide, LANES), F32)
            r_sc[ch, halo + sub:ext] = jnp.zeros((halo, wide, LANES), F32)

        flux = fv[halo] * (i_recv[1, ch, halo] - u_sc[ch, 0])
        r_sc[ch, halo - 1] = r_sc[ch, halo - 1] - flux
        r_sc[ch, halo] = r_sc[ch, halo] + flux
        flux = fv[halo + sub] * (i_recv[0, ch, halo] - u_sc[ch, sub - 1])
        r_sc[ch, halo + sub] = r_sc[ch, halo + sub] - flux
        r_sc[ch, halo + sub - 1] = r_sc[ch, halo + sub - 1] + flux
        late_e(ch)

    def z_copy(t, ch, way, r_to):
        return pltpu.make_async_remote_copy(
            src_ref=z_send.at[t, ch, way], dst_ref=z_recv.at[t, ch, way],
            send_sem=zs_sem.at[t, ch, way], recv_sem=zr_sem.at[t, ch, way],
            device_id=(col, r_to), device_id_type=MESH)

    def update(ch, e, n):
        r_new = r_sc[ch, pl.ds(e, n)] - omega * stencil(ch, e, n)
        r_sc[ch, pl.ds(e, n)] = r_new
        return r_new

    def late_next(t, ch):
        @pl.when(has_up)
        def _():
            z_copy(t, ch, 1, up_row).wait_recv()
            v_sc[ch, 0:band, left:left + wide] = z_recv[t, ch, 1].astype(F32)

        @pl.when(has_dn)
        def _():
            z_copy(t, ch, 0, dn_row).wait_recv()
            v_sc[ch, band + sub:band + sub + band, left:left + wide] = z_recv[t, ch, 0].astype(F32)

        e_late[ch, 0:band] = update(ch, 0, band).astype(BF16)
        e_late[ch, band:2 * band] = update(ch, ext - band, band).astype(BF16)

    def late_rows(ch, first, count):
        lo, n = first * sub, count * sub
        sides = []
        for side in range(2):
            operand = e_late[ch, :, 16 * side:16 * side + 32, :].reshape(late_k, LANES)
            part = acc[ch, side, lo:lo + n] + jnp.dot(m_perm[side, lo:lo + n, 0:late_k], operand,
                                                      preferred_element_type=F32)
            sides.append(part.reshape(count, sub, LANES))
        return jnp.concatenate(sides, axis=1).astype(BF16)

    def keep_z(ch, first, count, z_bf):
        v_sc[ch, band + first:band + first + count, left:left + wide] = z_bf.astype(F32)

    def solve_and_send(t, ch):
        z_top = late_rows(ch, 0, band)
        z_bot = late_rows(ch, sub - band, band)
        z_send[t, ch, 0] = z_top
        z_send[t, ch, 1] = z_bot

        @pl.when(has_up)
        def _():
            z_copy(t, ch, 0, up_row).start()

        @pl.when(has_dn)
        def _():
            z_copy(t, ch, 1, dn_row).start()

        keep_z(ch, 0, band, z_top)
        keep_z(ch, sub - band, band, z_bot)
        keep_z(ch, band, sub - 2 * band, late_rows(ch, band, sub - 2 * band))

        group = (sub - 2) // 2

        def inner(i, c):
            e_early[ch, pl.ds(i * group, group)] = update(ch, band + i * group, group).astype(BF16)
            return c
        lax.fori_loop(0, 2, inner, 0)
        add_u(ch)
        early_dot(ch)

    def add_u(ch):
        def add(i, c):
            rows = pl.ds(i * 6, 6)
            u_sc[ch, rows] = u_sc[ch, rows] + omega * v_sc[ch, pl.ds(i * 6 + band, 6), left:left + wide]
            return c
        lax.fori_loop(0, sub // 6, add, 0)

    def sweep_first(ch, carry):
        late_first(ch)
        solve_and_send(0, ch)
        return carry
    lax.fori_loop(0, chunks, sweep_first, 0)

    def sweep_next(step, carry):
        t = step // chunks
        ch = step % chunks
        late_next(t, ch)
        solve_and_send(t + 1, ch)
        return carry
    lax.fori_loop(0, (SWEEPS - 2) * chunks, sweep_next, 0)

    def out_own(ch):
        return pltpu.make_async_copy(u_sc.at[ch, :, my_cols, :], out_hbm.at[:, :, lanes_of(col, ch)], out_loc.at[ch])

    def out_pair(ch, which):
        return pltpu.make_async_remote_copy(
            src_ref=u_sc.at[ch, :, other_cols, :], dst_ref=out_hbm.at[:, :, lanes_of(which, ch)],
            send_sem=out_send.at[ch], recv_sem=out_recv.at[ch],
            device_id=(other, row), device_id_type=MESH)

    def sweep_last(ch, carry):
        late_next(SWEEPS - 2, ch)
        keep_z(ch, 0, sub, late_rows(ch, 0, sub))
        add_u(ch)
        out_pair(ch, col).start()
        out_own(ch).start()
        return carry
    lax.fori_loop(0, chunks, sweep_last, 0)

    kap_copy(1, col, 0, row, other).wait_send()
    mat_pair(col).wait_send()
    for ch in range(chunks):
        u_pair(ch).wait_send()
        f_pair(ch, my_cols).wait_send()

    @pl.when(has_up)
    def _():
        kap_copy(2, col, 1, up_row, col).wait_send()
        kap_copy(2, col, 2, up_row, other).wait_send()
        for ch in range(chunks):
            init_copy(0, ch, up_row).wait_send()
            for t in range(SWEEPS - 1):
                z_copy(t, ch, 0, up_row).wait_send()

    @pl.when(has_dn)
    def _():
        kap_copy(0, col, 3, dn_row, col).wait_send()
        kap_copy(0, col, 4, dn_row, other).wait_send()
        for ch in range(chunks):
            init_copy(1, ch, dn_row).wait_send()
            for t in range(SWEEPS - 1):
                z_copy(t, ch, 1, dn_row).wait_send()

    for ch in range(chunks):
        out_own(ch).wait()
        out_pair(ch, col).wait_send()
        out_pair(ch, other).wait_recv()


def solution(mesh):
    row_count = mesh.shape['row']
    grid_spec = P('row', 'col', None)

    def device_fn(f_blk, u_blk, kappa_blk, mat_blk, omega_relax):
        sub, _, rhs = u_blk.shape
        ext_cells = mat_blk.shape[3]
        ext = math.isqrt(ext_cells)
        halo = (ext - sub) // 2
        band = halo + 1
        chunks = rhs // (2 * LANES)
        wide = 2 * sub
        early_rows = 24
        hbm = pl.BlockSpec(memory_space=pl.ANY)
        dma = pltpu.SemaphoreType.DMA
        return pl.pallas_call(
            functools.partial(kernel, row_count, sub, halo, chunks),
            out_shape=jax.ShapeDtypeStruct(u_blk.shape, F32),
            in_specs=[pl.BlockSpec(memory_space=pltpu.SMEM), hbm, hbm, hbm, hbm],
            out_specs=hbm,
            scratch_shapes=[
                pltpu.VMEM((chunks, sub, wide, LANES), F32),
                pltpu.VMEM((chunks, ext, wide, LANES), F32),
                pltpu.VMEM((chunks, ext + 2, 64, LANES), F32),
                pltpu.VMEM((chunks, 2 * band, wide, LANES), BF16),
                pltpu.VMEM((chunks, early_rows, wide, LANES), BF16),
                pltpu.VMEM((chunks, 2, sub * sub, LANES), F32),
                pltpu.VMEM((2, sub * sub, ext_cells), BF16),
                pltpu.VMEM((2, sub * sub, 1024), BF16),
                pltpu.VMEM((3, 2, sub, sub), F32),
                pltpu.VMEM((ext + 2, 64, LANES), F32),
                pltpu.VMEM((ext + 1, wide, LANES), F32),
                pltpu.VMEM((ext, wide, LANES), F32),
                pltpu.VMEM((ext, wide, LANES), F32),
                pltpu.VMEM((ext, wide, LANES), F32),
                pltpu.VMEM((2, chunks, band, wide, LANES), F32),
                pltpu.VMEM((2, chunks, band, wide, LANES), F32),
                pltpu.VMEM((SWEEPS - 1, chunks, 2, band, wide, LANES), BF16),
                pltpu.VMEM((SWEEPS - 1, chunks, 2, band, wide, LANES), BF16),
                dma((2, chunks)), dma((3, chunks)), dma((3, chunks)), dma, dma, dma((5,)), dma((5,)),
                dma((2, chunks)), dma((2, chunks)),
                dma((SWEEPS - 1, chunks, 2)), dma((SWEEPS - 1, chunks, 2)),
                dma((chunks,)), dma((chunks,)), dma((chunks,)),
            ],
            compiler_params=pltpu.CompilerParams(collective_id=0, has_side_effects=True,
                                                 vmem_limit_bytes=48 * 1024 * 1024),
        )(omega_relax.reshape(1), f_blk, u_blk, kappa_blk, mat_blk)

    return jax.shard_map(device_fn, mesh=mesh,
                         in_specs=(grid_spec, grid_spec, P('row', 'col'), P('row', 'col', None, None), P()),
                         out_specs=grid_spec, check_vma=False)
```

```python
import functools
import math

import jax
import jax.numpy as jnp
from jax import lax
from jax.experimental import pallas as pl
from jax.experimental.pallas import tpu as pltpu
from jax.sharding import PartitionSpec as P

SWEEPS = 6
LANES = 128
MESH = pl.DeviceIdType.MESH
F32 = jnp.float32
BF16 = jnp.bfloat16


def kernel(row_count, sub, halo, chunks,
           om_ref, f_hbm, u_hbm, kap_hbm, mat_hbm, out_ref,
           u_sc, r_sc, v_sc, e_late, e_early, acc, m_raw, m_turn, m_perm,
           k_raw, kb, ko, fv, fw, fe, dg, u_band, pv, pw, pe, pd, i_send, i_recv, a_send, a_recv,
           z_send, z_recv, u_fin,
           load_sem, band_sem, pair_send, pair_recv, mat_sem, kap_loc, kap_send, kap_recv,
           is_sem, ir_sem, as_sem, ar_sem, zs_sem, zr_sem, out_send, out_recv):
    wide = 2 * sub
    ext = sub + 2 * halo
    band = halo + 1
    late_k = 2 * band * 32
    early_rows = e_early.shape[1]
    half = chunks * LANES
    left = 8

    row = lax.axis_index('row')
    col = lax.axis_index('col')
    other = 1 - col
    mine = lax.rem(row + col, 2)
    theirs = 1 - mine
    has_up = row > 0
    has_dn = row < row_count - 1
    ways = ((0, has_up, jnp.maximum(row - 1, 0)), (1, has_dn, jnp.minimum(row + 1, row_count - 1)))
    up_row, dn_row = ways[0][2], ways[1][2]
    col_spans = [pl.ds(side * sub, sub) for side in range(2)]
    my_cols = pl.ds(pl.multiple_of(col * sub, 8), sub)
    other_cols = pl.ds(pl.multiple_of(other * sub, 8), sub)
    own_rows = pl.ds(halo, sub)

    def lanes_of(which, ch):
        return pl.ds(pl.multiple_of(which * half + ch * LANES, LANES), LANES)

    barrier = pltpu.get_barrier_semaphore()

    def greet(r_to, c_to):
        pl.semaphore_signal(barrier, inc=1, device_id=(c_to, r_to), device_id_type=MESH)

    for _, present, r_to in ways:
        @pl.when(present)
        def _():
            greet(r_to, col)
            greet(r_to, other)
    greet(row, other)

    kap_load = pltpu.make_async_copy(kap_hbm, k_raw.at[col], kap_loc)
    kap_load.start()

    def band_loads(way, g):
        lanes = pl.ds(g * LANES, LANES)
        u_from = pl.ds(0 if way == 0 else sub - band, band)
        f_from = pl.ds(0 if way == 0 else sub - halo, halo)
        return (pltpu.make_async_copy(u_hbm.at[u_from, :, lanes], u_band.at[way, g, :, 8:8 + sub, :],
                                      band_sem.at[0, way, g]),
                pltpu.make_async_copy(f_hbm.at[f_from, :, lanes], i_send.at[way, g, 0:halo],
                                      band_sem.at[1, way, g]))

    for g in range(2 * chunks):
        for way in range(2):
            for load in band_loads(way, g):
                load.start()

    def u_load(ch):
        return pltpu.make_async_copy(u_hbm.at[:, :, lanes_of(mine, ch)], u_sc.at[ch, :, my_cols, :], load_sem.at[0, ch])

    def f_load(ch):
        return pltpu.make_async_copy(f_hbm.at[:, :, lanes_of(mine, ch)], r_sc.at[ch, own_rows, my_cols, :],
                                     load_sem.at[1, ch])

    mat_load = pltpu.make_async_copy(mat_hbm, m_raw.at[col], mat_sem)
    mat_load.start()
    for ch in range(chunks):
        u_load(ch).start()
        f_load(ch).start()

    def u_pair(ch, cols):
        return pltpu.make_async_remote_copy(
            src_ref=u_hbm.at[:, :, lanes_of(theirs, ch)], dst_ref=u_sc.at[ch, :, cols, :],
            send_sem=pair_send.at[0, ch], recv_sem=pair_recv.at[0, ch],
            device_id=(other, row), device_id_type=MESH)

    def f_pair(ch, cols):
        return pltpu.make_async_remote_copy(
            src_ref=f_hbm.at[:, :, lanes_of(theirs, ch)], dst_ref=r_sc.at[ch, own_rows, cols, :],
            send_sem=pair_send.at[1, ch], recv_sem=pair_recv.at[1, ch],
            device_id=(other, row), device_id_type=MESH)

    def mat_pair(slot):
        return pltpu.make_async_remote_copy(
            src_ref=mat_hbm, dst_ref=m_raw.at[slot],
            send_sem=pair_send.at[2, 0], recv_sem=pair_recv.at[2, 0],
            device_id=(other, row), device_id_type=MESH)

    def kap_pair(slot):
        return pltpu.make_async_remote_copy(
            src_ref=k_raw.at[col], dst_ref=k_raw.at[slot],
            send_sem=kap_send, recv_sem=kap_recv,
            device_id=(other, row), device_id_type=MESH)

    def core_for(h):
        return lax.rem(h + row + 1, 2)

    def init_send(way, r_to, h, ch):
        g = h * chunks + ch
        return pltpu.make_async_remote_copy(
            src_ref=i_send.at[way, g], dst_ref=i_recv.at[way, ch, :, my_cols, :],
            send_sem=is_sem.at[way, g], recv_sem=ir_sem.at[way, ch, col],
            device_id=(core_for(h), r_to), device_id_type=MESH)

    def init_wait(way, r_to, ch, side):
        pltpu.make_async_remote_copy(
            src_ref=i_send.at[way, ch], dst_ref=i_recv.at[way, ch, :, col_spans[side], :],
            send_sem=is_sem.at[way, ch], recv_sem=ir_sem.at[way, ch, side],
            device_id=(other, r_to), device_id_type=MESH).wait_recv()

    def aux_send(way, r_to, h):
        return pltpu.make_async_remote_copy(
            src_ref=a_send.at[way, h], dst_ref=a_recv.at[way, col],
            send_sem=as_sem.at[way, h], recv_sem=ar_sem.at[way, col],
            device_id=(core_for(h), r_to), device_id_type=MESH)

    def aux_wait(way, r_to, side):
        pltpu.make_async_remote_copy(
            src_ref=a_send.at[way, side], dst_ref=a_recv.at[way, side],
            send_sem=as_sem.at[way, side], recv_sem=ar_sem.at[way, side],
            device_id=(other, r_to), device_id_type=MESH).wait_recv()

    def z_copy(t, ch, way, r_to):
        return pltpu.make_async_remote_copy(
            src_ref=z_send.at[t, ch, way], dst_ref=z_recv.at[t, ch, way],
            send_sem=zs_sem.at[t, ch, way], recv_sem=zr_sem.at[t, ch, way],
            device_id=(other, r_to), device_id_type=MESH)

    omega = om_ref[0]
    for way in range(2):
        for g in range(2 * chunks):
            u_band[way, g, :, 0:8] = jnp.zeros((band, 8, LANES), F32)
            u_band[way, g, :, 8 + sub:16 + sub] = jnp.zeros((band, 8, LANES), F32)
        for h in range(2):
            a_send[way, h] = jnp.zeros((16, LANES), F32)

    eye = lax.broadcasted_iota(jnp.int32, (sub, sub), 0) == lax.broadcasted_iota(jnp.int32, (sub, sub), 1)

    def spread(line):
        picked = jnp.where(eye, jnp.broadcast_to(line, (sub, sub)), 0.0)
        return jnp.broadcast_to(jnp.sum(picked, axis=1, keepdims=True), (sub, LANES))

    kap_load.wait()
    for k in range(sub):
        line = spread(k_raw[col, k:k + 1, :])
        ko[k, 8:8 + sub] = line
        ko[k, 7:8] = line[0:1]
        ko[k, 8 + sub:9 + sub] = line[sub - 1:sub]
    spot_col = lax.broadcasted_iota(jnp.int32, (sub, LANES), 0)
    cut_w = (spot_col == 0) & (col == 1)
    cut_e = (spot_col == sub - 1) & (col == 0)
    for way in range(2):
        first = 0 if way == 0 else sub - halo
        for k in range(halo):
            at = first + k
            mid = ko[at, 8:8 + sub]
            pw[way, k] = jnp.where(cut_w, 0.0, 0.5 * (mid + ko[at, 7:7 + sub]))
            pe[way, k] = jnp.where(cut_e, 0.0, 0.5 * (ko[at, 9:9 + sub] + mid))
            total = pw[way, k] + pe[way, k]
            if at > 0:
                pv[way, k] = 0.5 * (mid + ko[at - 1, 8:8 + sub])
                total = total + pv[way, k]
            if at < sub - 1:
                pv[way, k + 1] = 0.5 * (ko[at + 1, 8:8 + sub] + mid)
                total = total + pv[way, k + 1]
            pd[way, k] = total

    for g in range(2 * chunks):
        for way in range(2):
            for load in band_loads(way, g):
                load.wait()
            shift = 0 if way == 0 else 1
            for k in range(halo):
                line = shift + k
                au = (pd[way, k] * u_band[way, g, line, 8:8 + sub]
                      - pw[way, k] * u_band[way, g, line, 7:7 + sub]
                      - pe[way, k] * u_band[way, g, line, 9:9 + sub])
                if line > 0:
                    au = au - pv[way, k] * u_band[way, g, line - 1, 8:8 + sub]
                if line < band - 1:
                    au = au - pv[way, k + 1] * u_band[way, g, line + 1, 8:8 + sub]
                i_send[way, g, k] = i_send[way, g, k] - au
                edge = jnp.where(col == 0, u_band[way, g, line, 7 + sub:8 + sub], u_band[way, g, line, 8:9])
                slot = halo * (g % chunks) + k
                a_send[way, g // chunks, slot:slot + 1] = edge
            i_send[way, g, halo] = u_band[way, g, 0 if way == 0 else halo, 8:8 + sub]

        for h in range(2):
            if g == 0:
                a_send[0, h, 8:8 + band, 0:sub] = k_raw[col, 0:band]
                a_send[1, h, 8:8 + band, 0:sub] = k_raw[col, sub - band:sub]

    pl.semaphore_wait(barrier, 1 + 2 * has_up.astype(jnp.int32) + 2 * has_dn.astype(jnp.int32))

    for way, present, r_to in ways:
        @pl.when(present)
        def _():
            for h in range(2):
                aux_send(way, r_to, h).start()
            for ch in range(chunks):
                for h in range(2):
                    init_send(way, r_to, h, ch).start()
    kap_pair(col).start()
    u_pair(0, my_cols).start()
    f_pair(0, my_cols).start()
    mat_pair(col).start()
    for ch in range(1, chunks):
        u_pair(ch, my_cols).start()
        f_pair(ch, my_cols).start()

    def clear(ch, carry):
        for i in list(range(band)) + list(range(band + sub, ext + 2)):
            v_sc[ch, i] = jnp.zeros(v_sc.shape[2:], F32)
        for i in range(band, band + sub):
            v_sc[ch, i, 0:8] = jnp.zeros((8, LANES), F32)
            v_sc[ch, i, 8 + wide:16 + wide] = jnp.zeros((8, LANES), F32)
        e_early[ch, sub - 2:early_rows] = jnp.zeros((early_rows - sub + 2, wide, LANES), BF16)
        return carry
    lax.fori_loop(0, chunks, clear, 0)

    ext_cells = m_raw.shape[1]
    tile = 256
    lines_per_tile = tile // 32

    def permute(side):
        m_turn[:, 896:1024] = jnp.zeros((sub * sub, 128), BF16)
        m_turn[:, 0:ext_cells] = m_raw[side].T
        for n_tile in range(m_perm.shape[2] // tile):
            if n_tile == 0:
                spans = [(0, 128), (768, 1024)]
            else:
                first = band + lines_per_tile * (n_tile - 1)
                last = min(first + lines_per_tile, ext - band)
                spans = [(first * ext // 128 * 128, -(-last * ext // 128) * 128)]
            n_at = n_tile * tile + lax.broadcasted_iota(jnp.int32, (1, tile), 1)
            q = lax.shift_right_logical(n_at, 5)
            j = lax.bitwise_and(n_at, 31)
            line = jnp.where(q < band, q, jnp.where(q < 2 * band, q + (ext - 2 * band), q - band))
            ext_col = j + (halo - 8 * side)
            ok = (q < ext) & (ext_col >= 0) & (ext_col < ext)
            want = jnp.where(ok, line * ext + ext_col, -1)
            moved = None
            for lo, hi in spans:
                spot = lo + lax.broadcasted_iota(jnp.int32, (hi - lo, tile), 0)
                pick = jnp.where(spot == want, 1.0, 0.0).astype(BF16)
                part = jnp.dot(m_turn[:, lo:hi], pick, preferred_element_type=F32)
                moved = part if moved is None else moved + part
            m_perm[side, :, n_tile * tile:(n_tile + 1) * tile] = moved.astype(BF16)

    mat_load.wait()
    permute(col)

    kap_pair(other).wait_recv()

    def put_rows(take, at, count):
        for k in range(count):
            for side in range(2):
                line = spread(take(side, k))
                kb[at + k, left + side * sub:left + (side + 1) * sub] = line
                if side == 0:
                    kb[at + k, left - 1:left] = line[0:1]
                else:
                    kb[at + k, left + wide:left + wide + 1] = line[sub - 1:sub]

    def side_faces(e):
        k_mid = kb[e + 1, left:left + wide]
        fw[e] = 0.5 * (k_mid + kb[e + 1, left - 1:left + wide - 1])
        fe[e] = 0.5 * (kb[e + 1, left + 1:left + wide + 1] + k_mid)

    def diag_row(e):
        dg[e] = fv[e] + fv[e + 1] + fw[e] + fe[e]

    def face_row(i):
        fv[i] = 0.5 * (kb[i + 1, left:left + wide] + kb[i, left:left + wide])

    put_rows(lambda side, k: k_raw[side, k:k + 1, :], band, sub)
    fv[halo] = jnp.zeros((wide, LANES), F32)
    fv[halo + sub] = jnp.zeros((wide, LANES), F32)

    def own_face(i, carry):
        face_row(i)
        return carry
    lax.fori_loop(halo + 1, halo + sub, own_face, 0)

    def own_side(e, carry):
        side_faces(e)
        diag_row(e)
        return carry
    lax.fori_loop(halo, halo + sub, own_side, 0)

    def stencil(ch, e, n):
        rows = pl.ds(e, n)
        mid = pl.ds(e + 1, n)
        return (dg[rows] * v_sc[ch, mid, left:left + wide]
                - fv[rows] * v_sc[ch, pl.ds(e, n), left:left + wide]
                - fv[mid] * v_sc[ch, pl.ds(e + 2, n), left:left + wide]
                - fw[rows] * v_sc[ch, mid, left - 1:left + wide - 1]
                - fe[rows] * v_sc[ch, mid, left + 1:left + wide + 1])

    def first_residual(ch):
        u_load(ch).wait()
        f_load(ch).wait()
        u_pair(ch, other_cols).wait_recv()
        f_pair(ch, other_cols).wait_recv()

        def fill(i, c):
            rows = pl.ds(i * 6, 6)
            v_sc[ch, pl.ds(i * 6 + band, 6), left:left + wide] = u_sc[ch, rows]
            return c
        lax.fori_loop(0, sub // 6, fill, 0)

        def part(i, c):
            rows = pl.ds(halo + i * 6, 6)
            r_sc[ch, rows] = r_sc[ch, rows] - stencil(ch, halo + i * 6, 6)
            return c
        lax.fori_loop(0, sub // 6, part, 0)
        group = (sub - 2) // 2

        def to_e(i, c):
            e_early[ch, pl.ds(i * group, group)] = r_sc[ch, pl.ds(i * group + band, group)].astype(BF16)
            return c
        lax.fori_loop(0, 2, to_e, 0)

    first_residual(0)

    mat_pair(other).wait_recv()
    permute(other)

    def early_dot(ch):
        for side in range(2):
            operand = e_early[ch, :, 16 * side:16 * side + 32, :].reshape(early_rows * 32, LANES)
            acc[ch, side] = jnp.dot(m_perm[side, :, late_k:late_k + early_rows * 32], operand,
                                    preferred_element_type=F32)

    for way, present, r_to in ways:
        @pl.when(present)
        def _():
            for side in range(2):
                aux_wait(1 - way, r_to, side)
            put_rows(lambda side, k: a_recv[1 - way, side, 8 + k:9 + k, 0:sub], 0 if way == 0 else band + sub, band)

        @pl.when(jnp.logical_not(present))
        def _():
            for side in range(2):
                a_recv[1 - way, side] = jnp.zeros((16, LANES), F32)
            for i in range(band):
                if way == 0:
                    kb[i] = kb[band]
                else:
                    kb[band + sub + i] = kb[band + sub - 1]

    for i in range(halo + 1):
        face_row(i)
        face_row(halo + sub + i)
    for i in range(halo):
        side_faces(i)
        side_faces(halo + sub + i)
    for i in range(halo + 1):
        diag_row(i)
        diag_row(ext - 1 - i)

    def late_first(ch):
        for way, present, r_to in ways:
            sent = 1 - way
            rows = pl.ds(0 if way == 0 else halo + sub, halo)

            @pl.when(present)
            def _():
                for side in range(2):
                    init_wait(sent, r_to, ch, side)
                r_sc[ch, rows] = i_recv[sent, ch, 0:halo]

            @pl.when(jnp.logical_not(present))
            def _():
                i_recv[sent, ch, halo] = jnp.zeros((wide, LANES), F32)
                r_sc[ch, rows] = jnp.zeros((halo, wide, LANES), F32)

            for k in range(halo):
                e = (0 if way == 0 else halo + sub) + k
                slot = pl.ds(halo * ch + k, 1)
                flux = fe[e, sub - 1:sub] * (a_recv[sent, 1, slot] - a_recv[sent, 0, slot])
                r_sc[ch, e, sub - 1:sub] = r_sc[ch, e, sub - 1:sub] + flux
                r_sc[ch, e, sub:sub + 1] = r_sc[ch, e, sub:sub + 1] - flux

        closed = jnp.where(ch > 0, 1.0, 0.0)
        flux = fv[halo] * (i_recv[1, ch, halo] - u_sc[ch, 0])
        r_sc[ch, halo - 1] = r_sc[ch, halo - 1] - flux
        r_sc[ch, halo] = r_sc[ch, halo] + (flux + closed * (fv[halo] * u_sc[ch, 0]))
        flux = fv[halo + sub] * (i_recv[0, ch, halo] - u_sc[ch, sub - 1])
        r_sc[ch, halo + sub] = r_sc[ch, halo + sub] - flux
        last = halo + sub - 1
        r_sc[ch, last] = r_sc[ch, last] + (flux + closed * (fv[halo + sub] * u_sc[ch, sub - 1]))
        e_late[ch, 0:band] = r_sc[ch, 0:band].astype(BF16)
        e_late[ch, band:2 * band] = r_sc[ch, ext - band:ext].astype(BF16)

    def update(ch, e, n):
        r_new = r_sc[ch, pl.ds(e, n)] - omega * stencil(ch, e, n)
        r_sc[ch, pl.ds(e, n)] = r_new
        return r_new

    def late_next(t, ch):
        for way, present, r_to in ways:
            @pl.when(present)
            def _():
                z_copy(t, ch, 1 - way, r_to).wait_recv()
                at = 0 if way == 0 else band + sub
                v_sc[ch, at:at + band, left:left + wide] = z_recv[t, ch, 1 - way].astype(F32)

        e_late[ch, 0:band] = update(ch, 0, band).astype(BF16)
        e_late[ch, band:2 * band] = update(ch, ext - band, band).astype(BF16)

    def solve(ch, side, first, count):
        lo, n = first * sub, count * sub
        cols = pl.ds(pl.multiple_of(16 * side, 16), 32)
        operand = e_late[ch, :, cols, :].reshape(late_k, LANES)
        part = acc[ch, side, lo:lo + n] + jnp.dot(m_perm[side, lo:lo + n, 0:late_k], operand,
                                                  preferred_element_type=F32)
        return part.reshape(count, sub, LANES)

    def solve_rows(ch, first, count):
        return jnp.concatenate([solve(ch, side, first, count) for side in range(2)], axis=1).astype(BF16)

    def keep_z(ch, first, count, z_bf):
        v_sc[ch, band + first:band + first + count, left:left + wide] = z_bf.astype(F32)

    def solve_and_send(t, ch):
        z_top = solve_rows(ch, 0, band)
        z_bot = solve_rows(ch, sub - band, band)
        z_send[t, ch, 0] = z_top
        z_send[t, ch, 1] = z_bot
        for way, present, r_to in ways:
            @pl.when(present)
            def _():
                z_copy(t, ch, way, r_to).start()

        keep_z(ch, 0, band, z_top)
        keep_z(ch, sub - band, band, z_bot)
        keep_z(ch, band, sub - 2 * band, solve_rows(ch, band, sub - 2 * band))

        group = (sub - 2) // 2

        def inner(i, c):
            e_early[ch, pl.ds(i * group, group)] = update(ch, band + i * group, group).astype(BF16)
            return c
        lax.fori_loop(0, 2, inner, 0)

        def add(i, c):
            rows = pl.ds(i * 6, 6)
            u_sc[ch, rows] = u_sc[ch, rows] + omega * v_sc[ch, pl.ds(i * 6 + band, 6), left:left + wide]
            return c
        lax.fori_loop(0, sub // 6, add, 0)
        early_dot(ch)

    def sweep_first(ch, carry):
        @pl.when(ch > 0)
        def _():
            first_residual(ch)
        early_dot(ch)
        late_first(ch)
        solve_and_send(0, ch)
        return carry
    lax.fori_loop(0, chunks, sweep_first, 0)

    def sweep_next(step, carry):
        t = step // chunks
        ch = step % chunks
        late_next(t, ch)
        solve_and_send(t + 1, ch)
        return carry
    lax.fori_loop(0, (SWEEPS - 2) * chunks, sweep_next, 0)

    pieces = 2
    piece = sub // pieces

    def out_pair(ch, n, which):
        rows = pl.ds(n * piece, piece)
        return pltpu.make_async_remote_copy(
            src_ref=u_fin.at[ch, rows], dst_ref=out_ref.at[rows, :, lanes_of(which, ch)],
            send_sem=out_send.at[ch, n], recv_sem=out_recv.at[ch, n],
            device_id=(other, row), device_id_type=MESH)

    def sweep_last(ch, carry):
        late_next(SWEEPS - 2, ch)
        for n in range(pieces):
            first = n * piece
            z = solve(ch, other, first, piece).astype(BF16).astype(F32)
            u_fin[ch, first:first + piece] = u_sc[ch, first:first + piece, other_cols] + omega * z
            out_pair(ch, n, mine).start()
        for n in range(pieces):
            first = n * piece
            z = solve(ch, col, first, piece).astype(BF16).astype(F32)
            out_ref[first:first + piece, :, lanes_of(mine, ch)] = u_sc[ch, first:first + piece, my_cols] + omega * z
        return carry
    lax.fori_loop(0, chunks, sweep_last, 0)

    kap_pair(col).wait_send()
    mat_pair(col).wait_send()
    for ch in range(chunks):
        u_pair(ch, my_cols).wait_send()
        f_pair(ch, my_cols).wait_send()
    for way, present, r_to in ways:
        @pl.when(present)
        def _():
            for h in range(2):
                aux_send(way, r_to, h).wait_send()
                for ch in range(chunks):
                    init_send(way, r_to, h, ch).wait_send()
            for ch in range(chunks):
                for t in range(SWEEPS - 1):
                    z_copy(t, ch, way, r_to).wait_send()
    for ch in range(chunks):
        for n in range(pieces):
            out_pair(ch, n, mine).wait_send()
            out_pair(ch, n, theirs).wait_recv()


def solution(mesh):
    row_count = mesh.shape['row']
    grid_spec = P('row', 'col', None)

    def device_fn(f_blk, u_blk, kappa_blk, mat_blk, omega_relax):
        sub, _, rhs = u_blk.shape
        ext_cells = mat_blk.shape[3]
        ext = math.isqrt(ext_cells)
        halo = (ext - sub) // 2
        band = halo + 1
        chunks = rhs // (2 * LANES)
        wide = 2 * sub
        early_rows = 24
        hbm = pl.BlockSpec(memory_space=pl.ANY)
        vmem = pltpu.VMEM
        dma = pltpu.SemaphoreType.DMA
        return pl.pallas_call(
            functools.partial(kernel, row_count, sub, halo, chunks),
            out_shape=pltpu.VMEM(u_blk.shape, F32),
            in_specs=[pl.BlockSpec(memory_space=pltpu.SMEM), hbm, hbm, hbm, hbm],
            out_specs=pl.BlockSpec(memory_space=pltpu.VMEM),
            scratch_shapes=[
                vmem((chunks, sub, wide, LANES), F32),
                vmem((chunks, ext, wide, LANES), F32),
                vmem((chunks, ext + 2, 64, LANES), F32),
                vmem((chunks, 2 * band, wide, LANES), BF16),
                vmem((chunks, early_rows, wide, LANES), BF16),
                vmem((chunks, 2, sub * sub, LANES), F32),
                vmem((2, ext_cells, sub * sub), BF16),
                vmem((sub * sub, 1024), BF16),
                vmem((2, sub * sub, 1024), BF16),
                vmem((2, sub, sub), F32),
                vmem((ext + 2, 64, LANES), F32),
                vmem((sub, 40, LANES), F32),
                vmem((ext + 1, wide, LANES), F32),
                vmem((ext, wide, LANES), F32),
                vmem((ext, wide, LANES), F32),
                vmem((ext, wide, LANES), F32),
                vmem((2, 2 * chunks, band, 40, LANES), F32),
                vmem((2, halo + 1, sub, LANES), F32),
                vmem((2, halo, sub, LANES), F32),
                vmem((2, halo, sub, LANES), F32),
                vmem((2, halo, sub, LANES), F32),
                vmem((2, 2 * chunks, band, sub, LANES), F32),
                vmem((2, chunks, band, wide, LANES), F32),
                vmem((2, 2, 16, LANES), F32),
                vmem((2, 2, 16, LANES), F32),
                vmem((SWEEPS - 1, chunks, 2, band, wide, LANES), BF16),
                vmem((SWEEPS - 1, chunks, 2, band, wide, LANES), BF16),
                vmem((chunks, sub, sub, LANES), F32),
                dma((2, chunks)), dma((2, 2, 2 * chunks)), dma((3, chunks)), dma((3, chunks)), dma, dma,
                dma, dma,
                dma((2, 2 * chunks)), dma((2, chunks, 2)), dma((2, 2)), dma((2, 2)),
                dma((SWEEPS - 1, chunks, 2)), dma((SWEEPS - 1, chunks, 2)),
                dma((chunks, 2)), dma((chunks, 2)),
            ],
            compiler_params=pltpu.CompilerParams(collective_id=0, has_side_effects=True,
                                                 vmem_limit_bytes=61000 * 1024),
        )(omega_relax.reshape(1), f_blk, u_blk, kappa_blk, mat_blk[0, 0].T)

    return jax.shard_map(device_fn, mesh=mesh,
                         in_specs=(grid_spec, grid_spec, P('row', 'col'), P('row', 'col', None, None), P()),
                         out_specs=grid_spec, check_vma=False)
```

```python
import functools
import math

import jax
import jax.numpy as jnp
from jax import lax
from jax.experimental import pallas as pl
from jax.experimental.pallas import tpu as pltpu
from jax.sharding import PartitionSpec as P

SWEEPS = 6
LANES = 128
MESH = pl.DeviceIdType.MESH
F32 = jnp.float32
BF16 = jnp.bfloat16


def kernel(row_count, sub, halo, chunks,
           om_ref, f_hbm, u_hbm, kap_hbm, mat_hbm, out_ref,
           u_sc, r_sc, v_sc, e_late, e_early, acc, m_raw, m_turn, m_perm,
           k_raw, kb, ko, fv, fw, fe, dg, u_band, pv, pw, pe, pd, i_send, i_recv, n_send, n_recv, a_send, a_recv,
           z_send, z_recv, u_fin,
           load_sem, band_sem, pair_send, pair_recv, mat_sem, mat_send, mat_recv, kap_loc, kap_send, kap_recv,
           is_sem, ns_sem, ir_sem, far_sem, as_sem, ar_sem, zs_sem, zr_sem, out_send, out_recv):
    wide = 2 * sub
    ext = sub + 2 * halo
    band = halo + 1
    late_k = 2 * band * 32
    early_rows = e_early.shape[0]
    half = chunks * LANES
    left = 8

    row = lax.axis_index('row')
    col = lax.axis_index('col')
    other = 1 - col
    mine = lax.rem(row + col, 2)
    theirs = 1 - mine
    has_up = row > 0
    has_dn = row < row_count - 1
    ways = ((0, has_up, jnp.maximum(row - 1, 0)), (1, has_dn, jnp.minimum(row + 1, row_count - 1)))
    up_row, dn_row = ways[0][2], ways[1][2]
    col_spans = [pl.ds(side * sub, sub) for side in range(2)]
    my_cols = pl.ds(pl.multiple_of(col * sub, 8), sub)
    other_cols = pl.ds(pl.multiple_of(other * sub, 8), sub)
    own_rows = pl.ds(halo, sub)

    def lanes_of(which, ch):
        return pl.ds(pl.multiple_of(which * half + ch * LANES, LANES), LANES)

    def local_bytes(ref, sem):
        return pltpu.make_async_copy(ref, ref, sem)

    def remote_bytes(ref, send_sem, recv_sem):
        return pltpu.make_async_remote_copy(src_ref=ref, dst_ref=ref, send_sem=send_sem, recv_sem=recv_sem,
                                            device_id=(other, row), device_id_type=MESH)

    barrier = pltpu.get_barrier_semaphore()

    def in_lanes(ch):
        return slice(ch * LANES, (ch + 1) * LANES)

    def greet(r_to, c_to):
        pl.semaphore_signal(barrier, inc=1, device_id=(c_to, r_to), device_id_type=MESH)

    for _, present, r_to in ways:
        @pl.when(present)
        def _():
            greet(r_to, col)
            greet(r_to, other)
    greet(row, other)

    kap_load = pltpu.make_async_copy(kap_hbm, k_raw.at[col], kap_loc)
    kap_load.start()

    def band_loads(way, g):
        lanes = pl.ds(g * LANES, LANES)
        u_from = pl.ds(0 if way == 0 else sub - band, band)
        f_from = pl.ds(0 if way == 0 else sub - halo, halo)
        return (pltpu.make_async_copy(u_hbm.at[u_from, :, lanes], u_band.at[way, g, :, 8:8 + sub, :],
                                      band_sem.at[0]),
                pltpu.make_async_copy(f_hbm.at[f_from, :, lanes], i_send.at[way, g, pl.ds(1 - way, halo)],
                                      band_sem.at[1]))

    for g in range(2 * chunks):
        for way in range(2):
            for load in band_loads(way, g):
                load.start()

    def u_load(ch):
        return pltpu.make_async_copy(u_hbm.at[:, :, lanes_of(mine, ch)], u_sc.at[ch, :, my_cols, :], load_sem.at[ch])

    def f_load(ch):
        return pltpu.make_async_copy(f_hbm.at[:, :, lanes_of(mine, ch)], r_sc.at[ch, own_rows, my_cols, :],
                                     load_sem.at[ch])

    mat_load = pltpu.make_async_copy(mat_hbm, m_raw.at[col], mat_sem)
    mat_load.start()
    for ch in range(chunks):
        u_load(ch).start()
        f_load(ch).start()

    def u_pair(ch, cols):
        return pltpu.make_async_remote_copy(
            src_ref=u_hbm.at[:, :, lanes_of(theirs, ch)], dst_ref=u_sc.at[ch, :, cols, :],
            send_sem=pair_send, recv_sem=pair_recv.at[ch],
            device_id=(other, row), device_id_type=MESH)

    def f_pair(ch, cols):
        return pltpu.make_async_remote_copy(
            src_ref=f_hbm.at[:, :, lanes_of(theirs, ch)], dst_ref=r_sc.at[ch, own_rows, cols, :],
            send_sem=pair_send, recv_sem=pair_recv.at[ch],
            device_id=(other, row), device_id_type=MESH)

    def mat_pair(slot):
        return pltpu.make_async_remote_copy(
            src_ref=mat_hbm, dst_ref=m_raw.at[slot],
            send_sem=mat_send, recv_sem=mat_recv,
            device_id=(other, row), device_id_type=MESH)

    def kap_pair(slot):
        return pltpu.make_async_remote_copy(
            src_ref=k_raw.at[col], dst_ref=k_raw.at[slot],
            send_sem=kap_send, recv_sem=kap_recv,
            device_id=(other, row), device_id_type=MESH)

    def core_for(h):
        return lax.rem(h + row + 1, 2)

    near_rows = (pl.ds(0, 2), pl.ds(2, 2))
    far_rows = (pl.ds(2, 2), pl.ds(0, 2))

    def init_send(way, r_to, h, ch, rows, recv_sem):
        g = h * chunks + ch
        return pltpu.make_async_remote_copy(
            src_ref=i_send.at[way, g, rows], dst_ref=i_recv.at[way, ch, rows, my_cols, :],
            send_sem=is_sem.at[way], recv_sem=recv_sem.at[way, ch],
            device_id=(core_for(h), r_to), device_id_type=MESH)

    def narrow_send(way, r_to, h, ch):
        return pltpu.make_async_remote_copy(
            src_ref=n_send.at[way, h * chunks + ch], dst_ref=n_recv.at[way, ch, col],
            send_sem=ns_sem.at[way], recv_sem=ir_sem.at[way, ch],
            device_id=(core_for(h), r_to), device_id_type=MESH)

    def aux_send(way, r_to, h):
        return pltpu.make_async_remote_copy(
            src_ref=a_send.at[way, h], dst_ref=a_recv.at[way, col],
            send_sem=as_sem.at[way], recv_sem=ar_sem.at[way],
            device_id=(core_for(h), r_to), device_id_type=MESH)

    def z_copy(t, ch, way, r_to):
        return pltpu.make_async_remote_copy(
            src_ref=z_send.at[way, t, ch], dst_ref=z_recv.at[way, t, ch],
            send_sem=zs_sem.at[way], recv_sem=zr_sem.at[t % 2, ch, way],
            device_id=(other, r_to), device_id_type=MESH)

    omega = om_ref[0]
    for way in range(2):
        for g in range(2 * chunks):
            u_band[way, g, :, 0:8] = jnp.zeros((band, 8, LANES), F32)
            u_band[way, g, :, 8 + sub:16 + sub] = jnp.zeros((band, 8, LANES), F32)
        for h in range(2):
            a_send[way, h] = jnp.zeros((16, LANES), F32)

    eye = lax.broadcasted_iota(jnp.int32, (sub, sub), 0) == lax.broadcasted_iota(jnp.int32, (sub, sub), 1)

    def spread(line):
        picked = jnp.where(eye, jnp.broadcast_to(line, (sub, sub)), 0.0)
        return jnp.broadcast_to(jnp.sum(picked, axis=1, keepdims=True), (sub, LANES))

    kap_load.wait()
    for k in range(sub):
        line = spread(k_raw[col, k:k + 1, :])
        ko[k, 8:8 + sub] = line
        ko[k, 7:8] = line[0:1]
        ko[k, 8 + sub:9 + sub] = line[sub - 1:sub]
    spot_col = lax.broadcasted_iota(jnp.int32, (sub, LANES), 0)
    cut_w = (spot_col == 0) & (col == 1)
    cut_e = (spot_col == sub - 1) & (col == 0)
    for way in range(2):
        first = 0 if way == 0 else sub - halo
        for k in range(halo):
            at = first + k
            mid = ko[at, 8:8 + sub]
            pw[way, k] = jnp.where(cut_w, 0.0, 0.5 * (mid + ko[at, 7:7 + sub]))
            pe[way, k] = jnp.where(cut_e, 0.0, 0.5 * (ko[at, 9:9 + sub] + mid))
            total = pw[way, k] + pe[way, k]
            if at > 0:
                pv[way, k] = 0.5 * (mid + ko[at - 1, 8:8 + sub])
                total = total + pv[way, k]
            if at < sub - 1:
                pv[way, k + 1] = 0.5 * (ko[at + 1, 8:8 + sub] + mid)
                total = total + pv[way, k + 1]
            pd[way, k] = total

    local_bytes(i_send, band_sem.at[0]).wait()
    local_bytes(i_send.at[:, :, 0:halo], band_sem.at[1]).wait()
    for way in range(2):
        for h in range(2):
            first = 0 if way == 0 else sub - band
            a_send[way, h, 12:12 + band, 0:sub] = k_raw[col, first:first + band]
    for g in range(2 * chunks):
        h, ch = g // chunks, g % chunks
        for way in range(2):
            shift = way
            for k in range(halo):
                line = shift + k
                at = k + 1 - way
                au = (pd[way, k] * u_band[way, g, line, 8:8 + sub]
                      - pw[way, k] * u_band[way, g, line, 7:7 + sub]
                      - pe[way, k] * u_band[way, g, line, 9:9 + sub])
                if line > 0:
                    au = au - pv[way, k] * u_band[way, g, line - 1, 8:8 + sub]
                if line < band - 1:
                    au = au - pv[way, k + 1] * u_band[way, g, line + 1, 8:8 + sub]
                part = i_send[way, g, at] - au
                i_send[way, g, at] = part
                edge = jnp.where(col == 0, u_band[way, g, line, 7 + sub:8 + sub], u_band[way, g, line, 8:9])
                slot = 5 * ch + k
                a_send[way, h, slot:slot + 1] = edge
                far = k - 1 + way
                if 0 <= far < 2:
                    n_send[way, g, far] = part.astype(BF16)
                    slot = 5 * ch + halo + far
                    a_send[way, h, slot:slot + 1] = jnp.where(col == 0, part[sub - 1:sub], part[0:1])
            i_send[way, g, halo * way] = u_band[way, g, halo * way, 8:8 + sub]

    pl.semaphore_wait(barrier, 1 + 2 * has_up.astype(jnp.int32) + 2 * has_dn.astype(jnp.int32))

    for way, present, r_to in ways:
        @pl.when(present)
        def _():
            for h in range(2):
                aux_send(way, r_to, h).start()
            for h in range(2):
                for ch in range(chunks):
                    init_send(way, r_to, h, ch, near_rows[way], ir_sem).start()
                    narrow_send(way, r_to, h, ch).start()
            for ch in range(chunks):
                for h in range(2):
                    init_send(way, r_to, h, ch, far_rows[way], far_sem).start()
    kap_pair(col).start()
    u_pair(0, my_cols).start()
    f_pair(0, my_cols).start()
    mat_pair(col).start()
    for ch in range(1, chunks):
        u_pair(ch, my_cols).start()
        f_pair(ch, my_cols).start()

    def clear(ch, carry):
        for i in list(range(band)) + list(range(band + sub, ext + 2)):
            v_sc[ch, i] = jnp.zeros(v_sc.shape[2:], F32)
        for i in range(band, band + sub):
            v_sc[ch, i, 0:8] = jnp.zeros((8, LANES), F32)
            v_sc[ch, i, 8 + wide:16 + wide] = jnp.zeros((8, LANES), F32)
        return carry
    lax.fori_loop(0, chunks, clear, 0)
    e_early[sub - 2:early_rows] = jnp.zeros((early_rows - sub + 2, wide, half), BF16)

    ext_cells = m_raw.shape[1]
    tile = 256
    lines_per_tile = tile // 32

    def permute(side):
        m_turn[:, 896:1024] = jnp.zeros((sub * sub, 128), BF16)
        m_turn[:, 0:ext_cells] = m_raw[side].T
        for n_tile in range(m_perm.shape[2] // tile):
            if n_tile == 0:
                spans = [(0, 128), (768, 1024)]
            else:
                first = band + lines_per_tile * (n_tile - 1)
                last = min(first + lines_per_tile, ext - band)
                spans = [(first * ext // 128 * 128, -(-last * ext // 128) * 128)]
            n_at = n_tile * tile + lax.broadcasted_iota(jnp.int32, (1, tile), 1)
            q = lax.shift_right_logical(n_at, 5)
            j = lax.bitwise_and(n_at, 31)
            line = jnp.where(q < band, q, jnp.where(q < 2 * band, q + (ext - 2 * band), q - band))
            ext_col = j + (halo - 8 * side)
            ok = (q < ext) & (ext_col >= 0) & (ext_col < ext)
            want = jnp.where(ok, line * ext + ext_col, -1)
            moved = None
            for lo, hi in spans:
                spot = lo + lax.broadcasted_iota(jnp.int32, (hi - lo, tile), 0)
                pick = jnp.where(spot == want, 1.0, 0.0).astype(BF16)
                part = jnp.dot(m_turn[:, lo:hi], pick, preferred_element_type=F32)
                moved = part if moved is None else moved + part
            m_perm[side, :, n_tile * tile:(n_tile + 1) * tile] = moved.astype(BF16)

    mat_load.wait()
    permute(col)

    kap_pair(other).wait_recv()

    def put_rows(take, at, count):
        for k in range(count):
            for side in range(2):
                line = spread(take(side, k))
                kb[at + k, left + side * sub:left + (side + 1) * sub] = line
                if side == 0:
                    kb[at + k, left - 1:left] = line[0:1]
                else:
                    kb[at + k, left + wide:left + wide + 1] = line[sub - 1:sub]

    def side_faces(e):
        k_mid = kb[e + 1, left:left + wide]
        fw[e] = 0.5 * (k_mid + kb[e + 1, left - 1:left + wide - 1])
        fe[e] = 0.5 * (kb[e + 1, left + 1:left + wide + 1] + k_mid)

    def diag_row(e):
        dg[e] = fv[e] + fv[e + 1] + fw[e] + fe[e]

    def face_row(i):
        fv[i] = 0.5 * (kb[i + 1, left:left + wide] + kb[i, left:left + wide])

    put_rows(lambda side, k: k_raw[side, k:k + 1, :], band, sub)
    fv[halo] = jnp.zeros((wide, LANES), F32)
    fv[halo + sub] = jnp.zeros((wide, LANES), F32)

    def own_face(i, carry):
        face_row(i)
        return carry
    lax.fori_loop(halo + 1, halo + sub, own_face, 0)

    def own_side(e, carry):
        side_faces(e)
        diag_row(e)
        return carry
    lax.fori_loop(halo, halo + sub, own_side, 0)

    def stencil(ch, e, n):
        rows = pl.ds(e, n)
        mid = pl.ds(e + 1, n)
        return (dg[rows] * v_sc[ch, mid, left:left + wide]
                - fv[rows] * v_sc[ch, pl.ds(e, n), left:left + wide]
                - fv[mid] * v_sc[ch, pl.ds(e + 2, n), left:left + wide]
                - fw[rows] * v_sc[ch, mid, left - 1:left + wide - 1]
                - fe[rows] * v_sc[ch, mid, left + 1:left + wide + 1])

    def first_residual(ch):
        local_bytes(u_fin, load_sem.at[ch]).wait()
        remote_bytes(u_fin, pair_send, pair_recv.at[ch]).wait_recv()

        def fill(i, c):
            rows = pl.ds(i * 6, 6)
            v_sc[ch, pl.ds(i * 6 + band, 6), left:left + wide] = u_sc[ch, rows]
            return c
        lax.fori_loop(0, sub // 6, fill, 0)

        def part(i, c):
            rows = pl.ds(halo + i * 6, 6)
            r_sc[ch, rows] = r_sc[ch, rows] - stencil(ch, halo + i * 6, 6)
            return c
        lax.fori_loop(0, sub // 6, part, 0)
        group = (sub - 2) // 2

        def to_e(i, c):
            e_early[pl.ds(i * group, group), :, in_lanes(ch)] = r_sc[ch, pl.ds(i * group + band, group)].astype(BF16)
            return c
        lax.fori_loop(0, 2, to_e, 0)

    first_residual(0)

    mat_pair(other).wait_recv()
    permute(other)

    for ch in range(1, chunks):
        first_residual(ch)

    def early_dot():
        for side in range(2):
            operand = e_early[:, 16 * side:16 * side + 32, :].reshape(early_rows * 32, half)
            acc[side] = jnp.dot(m_perm[side, :, late_k:late_k + early_rows * 32], operand,
                                preferred_element_type=F32)

    early_dot()

    for way, present, r_to in ways:
        @pl.when(present)
        def _():
            remote_bytes(a_recv.at[1 - way], as_sem.at[way], ar_sem.at[1 - way]).wait_recv()
            put_rows(lambda side, k: a_recv[1 - way, side, 12 + k:13 + k, 0:sub], 0 if way == 0 else band + sub, band)

        @pl.when(jnp.logical_not(present))
        def _():
            for side in range(2):
                a_recv[1 - way, side] = jnp.zeros((16, LANES), F32)
            for i in range(band):
                if way == 0:
                    kb[i] = kb[band]
                else:
                    kb[band + sub + i] = kb[band + sub - 1]

    for i in range(halo + 1):
        face_row(i)
        face_row(halo + sub + i)
    for i in range(halo):
        side_faces(i)
        side_faces(halo + sub + i)
    for i in range(halo + 1):
        diag_row(i)
        diag_row(ext - 1 - i)

    def side_flux(sent, ch, k, e):
        slot = pl.ds(5 * ch + k, 1)
        return fe[e, sub - 1:sub] * (a_recv[sent, 1, slot] - a_recv[sent, 0, slot])

    def near_far(way):
        if way == 0:
            return (halo - 1, halo - 1), ((0, 0), (1, 1))
        return (halo + sub, 0), ((halo + sub + 1, 1), (halo + sub + 2, 2))

    wide_col = lax.broadcasted_iota(jnp.int32, (wide, LANES), 0)

    def late_first(ch):
        for way, present, r_to in ways:
            sent = 1 - way
            (e_near, k_near), far = near_far(way)
            near_at, u_at = (2, 3) if way == 0 else (1, 0)

            @pl.when(present)
            def _():
                remote_bytes(i_recv.at[sent, ch, 0:3], is_sem.at[way], ir_sem.at[sent, ch]).wait_recv()
                r_sc[ch, e_near] = i_recv[sent, ch, near_at]
                flux = side_flux(sent, ch, k_near, e_near)
                r_sc[ch, e_near, sub - 1:sub] = r_sc[ch, e_near, sub - 1:sub] + flux
                r_sc[ch, e_near, sub:sub + 1] = r_sc[ch, e_near, sub:sub + 1] - flux
                for n in range(2):
                    e, k = far[n]
                    flux = side_flux(sent, ch, k, e)
                    slot = pl.ds(5 * ch + halo + n, 1)
                    got = jnp.concatenate([n_recv[sent, ch, side, n].astype(F32) for side in range(2)], axis=0)
                    got = jnp.where(wide_col == sub - 1, a_recv[sent, 0, slot] + flux, got)
                    got = jnp.where(wide_col == sub, a_recv[sent, 1, slot] - flux, got)
                    e_late[e if way == 0 else e - (ext - 2 * band), :, in_lanes(ch)] = got.astype(BF16)

            @pl.when(jnp.logical_not(present))
            def _():
                i_recv[sent, ch, u_at] = jnp.zeros((wide, LANES), F32)
                rows = pl.ds(0 if way == 0 else halo + sub, halo)
                r_sc[ch, rows] = jnp.zeros((halo, wide, LANES), F32)
                rows = pl.ds(0 if way == 0 else 2 * band - 2, 2)
                e_late[rows, :, in_lanes(ch)] = jnp.zeros((2, wide, LANES), BF16)

        flux = fv[halo] * (i_recv[1, ch, 3] - u_sc[ch, 0])
        near = r_sc[ch, halo - 1] - flux
        own = r_sc[ch, halo] + flux
        r_sc[ch, halo - 1] = near
        r_sc[ch, halo] = own
        e_late[halo - 1, :, in_lanes(ch)] = near.astype(BF16)
        e_late[halo, :, in_lanes(ch)] = own.astype(BF16)
        flux = fv[halo + sub] * (i_recv[0, ch, 0] - u_sc[ch, sub - 1])
        near = r_sc[ch, halo + sub] - flux
        own = r_sc[ch, halo + sub - 1] + flux
        r_sc[ch, halo + sub] = near
        r_sc[ch, halo + sub - 1] = own
        e_late[band, :, in_lanes(ch)] = own.astype(BF16)
        e_late[band + 1, :, in_lanes(ch)] = near.astype(BF16)

    def far_residual(ch):
        for way, present, r_to in ways:
            sent = 1 - way
            _, far = near_far(way)

            @pl.when(present)
            def _():
                remote_bytes(i_recv.at[sent, ch, 0:2], is_sem.at[way], far_sem.at[sent, ch]).wait_recv()
                for n in range(2):
                    e, k = far[n]
                    flux = side_flux(sent, ch, k, e)
                    r_sc[ch, e] = i_recv[sent, ch, n + 2 * way]
                    r_sc[ch, e, sub - 1:sub] = r_sc[ch, e, sub - 1:sub] + flux
                    r_sc[ch, e, sub:sub + 1] = r_sc[ch, e, sub:sub + 1] - flux

    def update(ch, e, n):
        r_new = r_sc[ch, pl.ds(e, n)] - omega * stencil(ch, e, n)
        r_sc[ch, pl.ds(e, n)] = r_new
        return r_new

    def late_next(t, ch):
        for way, present, r_to in ways:
            @pl.when(present)
            def _():
                z_copy(t, ch, 1 - way, r_to).wait_recv()
                at = 0 if way == 0 else band + sub
                v_sc[ch, at:at + band, left:left + wide] = z_recv[1 - way, t, ch].astype(F32)

        e_late[0:band, :, in_lanes(ch)] = update(ch, 0, band).astype(BF16)
        e_late[band:2 * band, :, in_lanes(ch)] = update(ch, ext - band, band).astype(BF16)

    def solve(lanes, side, first, count):
        lo, n = first * sub, count * sub
        cols = pl.ds(pl.multiple_of(16 * side, 16), 32)
        operand = e_late[:, cols, lanes]
        width = operand.shape[2]
        part = acc[side, lo:lo + n, lanes] + jnp.dot(m_perm[side, lo:lo + n, 0:late_k],
                                                     operand.reshape(late_k, width), preferred_element_type=F32)
        return part.reshape(count, sub, width)

    def solve_rows(lanes, first, count):
        return jnp.concatenate([solve(lanes, side, first, count) for side in range(2)], axis=1).astype(BF16)

    def keep_z(ch, first, count, z_bf):
        v_sc[ch, band + first:band + first + count, left:left + wide] = z_bf.astype(F32)

    def solve_and_send(t, ch):
        z_top = solve_rows(in_lanes(ch), 0, band)
        z_bot = solve_rows(in_lanes(ch), sub - band, band)
        z_send[0, t, ch] = z_top
        z_send[1, t, ch] = z_bot
        for way, present, r_to in ways:
            @pl.when(present)
            def _():
                z_copy(t, ch, way, r_to).start()

        keep_z(ch, 0, band, z_top)
        keep_z(ch, sub - band, band, z_bot)

    def interior():
        z_mid = solve_rows(slice(0, half), band, sub - 2 * band)
        for ch in range(chunks):
            keep_z(ch, band, sub - 2 * band, z_mid[:, :, in_lanes(ch)])
        group = (sub - 2) // 2
        for ch in range(chunks):
            def inner(i, c):
                e_early[pl.ds(i * group, group), :, in_lanes(ch)] = update(ch, band + i * group, group).astype(BF16)
                return c
            lax.fori_loop(0, 2, inner, 0)

            def add(i, c):
                rows = pl.ds(i * 6, 6)
                u_sc[ch, rows] = u_sc[ch, rows] + omega * v_sc[ch, pl.ds(i * 6 + band, 6), left:left + wide]
                return c
            lax.fori_loop(0, sub // 6, add, 0)
        early_dot()

    for ch in range(chunks):
        late_first(ch)
        solve_and_send(0, ch)
    interior()

    def sweep_next(t, carry):
        @pl.when(t == 0)
        def _():
            for ch in range(chunks):
                far_residual(ch)
        for ch in range(chunks):
            late_next(t, ch)
            solve_and_send(t + 1, ch)
        interior()
        return carry
    lax.fori_loop(0, SWEEPS - 2, sweep_next, 0)

    pieces = 2
    piece = sub // pieces

    def out_pair(ch, n, which):
        rows = pl.ds(n * piece, piece)
        return pltpu.make_async_remote_copy(
            src_ref=u_fin.at[ch, rows], dst_ref=out_ref.at[rows, :, lanes_of(which, ch)],
            send_sem=out_send, recv_sem=out_recv,
            device_id=(other, row), device_id_type=MESH)

    for ch in range(chunks):
        late_next(SWEEPS - 2, ch)
        for n in range(pieces):
            first = n * piece
            z = solve(in_lanes(ch), other, first, piece).astype(BF16).astype(F32)
            u_fin[ch, first:first + piece] = u_sc[ch, first:first + piece, other_cols] + omega * z
            out_pair(ch, n, mine).start()
    z_own = solve(slice(0, half), col, 0, sub).astype(BF16).astype(F32)
    for ch in range(chunks):
        out_ref[:, :, lanes_of(mine, ch)] = u_sc[ch, :, my_cols] + omega * z_own[:, :, in_lanes(ch)]

    kap_pair(col).wait_send()
    mat_pair(col).wait_send()
    remote_bytes(u_sc, pair_send, pair_recv.at[0]).wait_send()
    for way, present, r_to in ways:
        @pl.when(present)
        def _():
            remote_bytes(a_send.at[way], as_sem.at[way], ar_sem.at[way]).wait_send()
            remote_bytes(i_send.at[way], is_sem.at[way], ir_sem.at[way, 0]).wait_send()
            remote_bytes(n_send.at[way], ns_sem.at[way], ir_sem.at[way, 0]).wait_send()
            remote_bytes(z_send.at[way], zs_sem.at[way], zr_sem.at[0, 0, way]).wait_send()
    remote_bytes(u_fin, out_send, out_recv).wait_send()
    remote_bytes(u_fin, out_send, out_recv).wait_recv()


def solution(mesh):
    row_count = mesh.shape['row']
    grid_spec = P('row', 'col', None)

    def device_fn(f_blk, u_blk, kappa_blk, mat_blk, omega_relax):
        sub, _, rhs = u_blk.shape
        ext_cells = mat_blk.shape[3]
        ext = math.isqrt(ext_cells)
        halo = (ext - sub) // 2
        band = halo + 1
        chunks = rhs // (2 * LANES)
        wide = 2 * sub
        early_rows = 24
        hbm = pl.BlockSpec(memory_space=pl.ANY)
        vmem = pltpu.VMEM
        dma = pltpu.SemaphoreType.DMA
        return pl.pallas_call(
            functools.partial(kernel, row_count, sub, halo, chunks),
            out_shape=pltpu.VMEM(u_blk.shape, F32),
            in_specs=[pl.BlockSpec(memory_space=pltpu.SMEM), hbm, hbm, hbm, hbm],
            out_specs=pl.BlockSpec(memory_space=pltpu.VMEM),
            scratch_shapes=[
                vmem((chunks, sub, wide, LANES), F32),
                vmem((chunks, ext, wide, LANES), F32),
                vmem((chunks, ext + 2, 64, LANES), F32),
                vmem((2 * band, wide, chunks * LANES), BF16),
                vmem((early_rows, wide, chunks * LANES), BF16),
                vmem((2, sub * sub, chunks * LANES), F32),
                vmem((2, ext_cells, sub * sub), BF16),
                vmem((sub * sub, 1024), BF16),
                vmem((2, sub * sub, 1024), BF16),
                vmem((2, sub, sub), F32),
                vmem((ext + 2, 64, LANES), F32),
                vmem((sub, 40, LANES), F32),
                vmem((ext + 1, wide, LANES), F32),
                vmem((ext, wide, LANES), F32),
                vmem((ext, wide, LANES), F32),
                vmem((ext, wide, LANES), F32),
                vmem((2, 2 * chunks, band, 40, LANES), F32),
                vmem((2, halo + 1, sub, LANES), F32),
                vmem((2, halo, sub, LANES), F32),
                vmem((2, halo, sub, LANES), F32),
                vmem((2, halo, sub, LANES), F32),
                vmem((2, 2 * chunks, band, sub, LANES), F32),
                vmem((2, chunks, band, wide, LANES), F32),
                vmem((2, 2 * chunks, 2, sub, LANES), BF16),
                vmem((2, chunks, 2, 2, sub, LANES), BF16),
                vmem((2, 2, 16, LANES), F32),
                vmem((2, 2, 16, LANES), F32),
                vmem((2, SWEEPS - 1, chunks, band, wide, LANES), BF16),
                vmem((2, SWEEPS - 1, chunks, band, wide, LANES), BF16),
                vmem((chunks, sub, sub, LANES), F32),
                dma((chunks,)), dma((2,)), dma, dma((chunks,)), dma, dma, dma, dma, dma, dma,
                dma((2,)), dma((2,)), dma((2, chunks)), dma((2, chunks)), dma((2,)), dma((2,)),
                dma((2,)), dma((2, chunks, 2)), dma, dma,
            ],
            compiler_params=pltpu.CompilerParams(collective_id=0, has_side_effects=True,
                                                 vmem_limit_bytes=61000 * 1024),
        )(omega_relax.reshape(1), f_blk, u_blk, kappa_blk, mat_blk[0, 0].T)

    return jax.shard_map(device_fn, mesh=mesh,
                         in_specs=(grid_spec, grid_spec, P('row', 'col'), P('row', 'col', None, None), P()),
                         out_specs=grid_spec, check_vma=False)
```

```python
import functools
import math

import jax
import jax.numpy as jnp
from jax import lax
from jax.experimental import pallas as pl
from jax.experimental.pallas import tpu as pltpu
from jax.sharding import PartitionSpec as P

SWEEPS = 6
ORDER = (((1, 0, 0), (1, 0, 1), (0, 0, 0), (1, 1, 0), (1, 1, 1), (0, 0, 1), (0, 1, 0), (0, 1, 1)), ((1, 1, 0), (1, 1, 1), (1, 0, 0), (1, 0, 1), (0, 1, 0), (0, 1, 1), (0, 0, 0), (0, 0, 1)))
LANES = 128
MESH = pl.DeviceIdType.MESH
F32 = jnp.float32
BF16 = jnp.bfloat16


def kernel(row_count, sub, halo, chunks,
           om_ref, f_hbm, u_hbm, kap_hbm, mat_hbm, out_ref,
           u_sc, r_sc, v_sc, e_late, e_early, acc, m_raw, m_turn, m_perm,
           k_raw, kb, ko, fv, fw, fe, dg, u_band, pv, pw, pe, pd, i_send, i_recv, n_send, n_recv, a_send, a_recv,
           z_send, z_recv, u_fin,
           load_sem, band_sem, pair_send, pair_recv, mat_sem, mat_send, mat_recv, kap_loc, kap_send, kap_recv,
           ici_sem, ir_sem, far_sem, ar_sem, zr_sem, out_recv):
    wide = 2 * sub
    ext = sub + 2 * halo
    band = halo + 1
    late_k = 2 * band * 32
    early_rows = e_early.shape[0]
    half = chunks * LANES
    left = 8

    row = lax.axis_index('row')
    col = lax.axis_index('col')
    other = 1 - col
    mine = lax.rem(row + col, 2)
    theirs = 1 - mine
    has_up = row > 0
    has_dn = row < row_count - 1
    ways = ((0, has_up, jnp.maximum(row - 1, 0)), (1, has_dn, jnp.minimum(row + 1, row_count - 1)))
    up_row, dn_row = ways[0][2], ways[1][2]
    col_spans = [pl.ds(side * sub, sub) for side in range(2)]
    my_cols = pl.ds(pl.multiple_of(col * sub, 8), sub)
    other_cols = pl.ds(pl.multiple_of(other * sub, 8), sub)
    own_rows = pl.ds(halo, sub)

    def lanes_of(which, ch):
        return pl.ds(pl.multiple_of(which * half + ch * LANES, LANES), LANES)

    def local_bytes(ref, sem):
        return pltpu.make_async_copy(ref, ref, sem)

    def remote_bytes(ref, send_sem, recv_sem):
        return pltpu.make_async_remote_copy(src_ref=ref, dst_ref=ref, send_sem=send_sem, recv_sem=recv_sem,
                                            device_id=(other, row), device_id_type=MESH)

    barrier = pltpu.get_barrier_semaphore()

    def in_lanes(ch):
        return slice(ch * LANES, (ch + 1) * LANES)

    def greet(r_to, c_to):
        pl.semaphore_signal(barrier, inc=1, device_id=(c_to, r_to), device_id_type=MESH)

    for _, present, r_to in ways:
        @pl.when(present)
        def _():
            greet(r_to, col)
            greet(r_to, other)
    greet(row, other)

    kap_load = pltpu.make_async_copy(kap_hbm, k_raw.at[col], kap_loc)
    kap_load.start()

    def band_loads(way, g):
        lanes = pl.ds(g * LANES, LANES)
        u_from = pl.ds(0 if way == 0 else sub - band, band)
        f_from = pl.ds(0 if way == 0 else sub - halo, halo)
        return (pltpu.make_async_copy(u_hbm.at[u_from, :, lanes], u_band.at[way, g, :, 8:8 + sub, :],
                                      band_sem),
                pltpu.make_async_copy(f_hbm.at[f_from, :, lanes], i_send.at[way, g, pl.ds(1 - way, halo)],
                                      band_sem))

    for g in range(2 * chunks):
        for way in range(2):
            for load in band_loads(way, g):
                load.start()

    def u_load(ch):
        return pltpu.make_async_copy(u_hbm.at[:, :, lanes_of(mine, ch)], u_sc.at[ch, :, my_cols, :], load_sem)

    def f_load(ch):
        return pltpu.make_async_copy(f_hbm.at[:, :, lanes_of(mine, ch)], r_sc.at[ch, own_rows, my_cols, :],
                                     load_sem)

    mat_load = pltpu.make_async_copy(mat_hbm, m_raw.at[col], mat_sem)
    mat_load.start()
    for ch in range(chunks):
        u_load(ch).start()
        f_load(ch).start()

    def u_pair(ch, cols):
        return pltpu.make_async_remote_copy(
            src_ref=u_hbm.at[:, :, lanes_of(theirs, ch)], dst_ref=u_sc.at[ch, :, cols, :],
            send_sem=pair_send, recv_sem=pair_recv.at[ch],
            device_id=(other, row), device_id_type=MESH)

    def f_pair(ch, cols):
        return pltpu.make_async_remote_copy(
            src_ref=f_hbm.at[:, :, lanes_of(theirs, ch)], dst_ref=r_sc.at[ch, own_rows, cols, :],
            send_sem=pair_send, recv_sem=pair_recv.at[ch],
            device_id=(other, row), device_id_type=MESH)

    def mat_pair(slot):
        return pltpu.make_async_remote_copy(
            src_ref=mat_hbm, dst_ref=m_raw.at[slot],
            send_sem=mat_send, recv_sem=mat_recv,
            device_id=(other, row), device_id_type=MESH)

    def kap_pair(slot):
        return pltpu.make_async_remote_copy(
            src_ref=k_raw.at[col], dst_ref=k_raw.at[slot],
            send_sem=kap_send, recv_sem=kap_recv,
            device_id=(other, row), device_id_type=MESH)

    def half_at(core):
        return lax.rem(core + row + 1, 2)

    near_rows = (pl.ds(0, 2), pl.ds(2, 2))
    far_rows = (pl.ds(2, 2), pl.ds(0, 2))

    def init_send(way, r_to, core, ch, rows, recv_sem):
        g = half_at(core) * chunks + ch
        return pltpu.make_async_remote_copy(
            src_ref=i_send.at[way, g, rows], dst_ref=i_recv.at[way, ch, rows, my_cols, :],
            send_sem=ici_sem.at[way], recv_sem=recv_sem,
            device_id=(core, r_to), device_id_type=MESH)

    def narrow_send(way, r_to, core, ch):
        return pltpu.make_async_remote_copy(
            src_ref=n_send.at[way, half_at(core) * chunks + ch], dst_ref=n_recv.at[way, ch, col],
            send_sem=ici_sem.at[way], recv_sem=ir_sem.at[way, ch],
            device_id=(core, r_to), device_id_type=MESH)

    def aux_send(way, r_to, core):
        return pltpu.make_async_remote_copy(
            src_ref=a_send.at[way, half_at(core)], dst_ref=a_recv.at[way, col],
            send_sem=ici_sem.at[way], recv_sem=ar_sem.at[way],
            device_id=(core, r_to), device_id_type=MESH)

    def z_copy(t, ch, way, r_to):
        return pltpu.make_async_remote_copy(
            src_ref=z_send.at[way, t, ch], dst_ref=z_recv.at[way, t, ch],
            send_sem=ici_sem.at[way], recv_sem=zr_sem.at[t % 2, ch, way],
            device_id=(other, r_to), device_id_type=MESH)

    omega = om_ref[0]
    for way in range(2):
        for g in range(2 * chunks):
            u_band[way, g, :, 0:8] = jnp.zeros((band, 8, LANES), F32)
            u_band[way, g, :, 8 + sub:16 + sub] = jnp.zeros((band, 8, LANES), F32)
        for h in range(2):
            a_send[way, h] = jnp.zeros((16, LANES), F32)

    eye = lax.broadcasted_iota(jnp.int32, (sub, sub), 0) == lax.broadcasted_iota(jnp.int32, (sub, sub), 1)

    def spread(line):
        picked = jnp.where(eye, jnp.broadcast_to(line, (sub, sub)), 0.0)
        return jnp.broadcast_to(jnp.sum(picked, axis=1, keepdims=True), (sub, LANES))

    kap_load.wait()
    for k in range(sub):
        line = spread(k_raw[col, k:k + 1, :])
        ko[k, 8:8 + sub] = line
        ko[k, 7:8] = line[0:1]
        ko[k, 8 + sub:9 + sub] = line[sub - 1:sub]
    spot_col = lax.broadcasted_iota(jnp.int32, (sub, LANES), 0)
    cut_w = (spot_col == 0) & (col == 1)
    cut_e = (spot_col == sub - 1) & (col == 0)
    for way in range(2):
        first = 0 if way == 0 else sub - halo
        for k in range(halo):
            at = first + k
            mid = ko[at, 8:8 + sub]
            pw[way, k] = jnp.where(cut_w, 0.0, 0.5 * (mid + ko[at, 7:7 + sub]))
            pe[way, k] = jnp.where(cut_e, 0.0, 0.5 * (ko[at, 9:9 + sub] + mid))
            total = pw[way, k] + pe[way, k]
            if at > 0:
                pv[way, k] = 0.5 * (mid + ko[at - 1, 8:8 + sub])
                total = total + pv[way, k]
            if at < sub - 1:
                pv[way, k + 1] = 0.5 * (ko[at + 1, 8:8 + sub] + mid)
                total = total + pv[way, k + 1]
            pd[way, k] = total

    local_bytes(v_sc.at[0, 0:21], band_sem).wait()
    for way in range(2):
        for h in range(2):
            first = 0 if way == 0 else sub - band
            a_send[way, h, 12:12 + band, 0:sub] = k_raw[col, first:first + band]
    for g in range(2 * chunks):
        h, ch = g // chunks, g % chunks
        for way in range(2):
            shift = way
            for k in range(halo):
                line = shift + k
                at = k + 1 - way
                au = (pd[way, k] * u_band[way, g, line, 8:8 + sub]
                      - pw[way, k] * u_band[way, g, line, 7:7 + sub]
                      - pe[way, k] * u_band[way, g, line, 9:9 + sub])
                if line > 0:
                    au = au - pv[way, k] * u_band[way, g, line - 1, 8:8 + sub]
                if line < band - 1:
                    au = au - pv[way, k + 1] * u_band[way, g, line + 1, 8:8 + sub]
                part = i_send[way, g, at] - au
                i_send[way, g, at] = part
                edge = jnp.where(col == 0, u_band[way, g, line, 7 + sub:8 + sub], u_band[way, g, line, 8:9])
                slot = 5 * ch + k
                a_send[way, h, slot:slot + 1] = edge
                far = k - 1 + way
                if 0 <= far < 2:
                    n_send[way, g, far] = part.astype(BF16)
                    slot = 5 * ch + halo + far
                    a_send[way, h, slot:slot + 1] = jnp.where(col == 0, part[sub - 1:sub], part[0:1])
            i_send[way, g, halo * way] = u_band[way, g, halo * way, 8:8 + sub]

    pl.semaphore_wait(barrier, 1 + 2 * has_up.astype(jnp.int32) + 2 * has_dn.astype(jnp.int32))

    for way, present, r_to in ways:
        @pl.when(present)
        def _():
            for core in range(2):
                aux_send(way, r_to, core).start()
            for near, core, ch in ORDER[way]:
                if near:
                    init_send(way, r_to, core, ch, near_rows[way], ir_sem.at[way, ch]).start()
                    narrow_send(way, r_to, core, ch).start()
                else:
                    init_send(way, r_to, core, ch, far_rows[way], far_sem.at[way]).start()
    kap_pair(col).start()
    u_pair(0, my_cols).start()
    f_pair(0, my_cols).start()
    mat_pair(col).start()
    for ch in range(1, chunks):
        u_pair(ch, my_cols).start()
        f_pair(ch, my_cols).start()

    def clear(ch, carry):
        for i in list(range(band)) + list(range(band + sub, ext + 2)):
            v_sc[ch, i] = jnp.zeros(v_sc.shape[2:], F32)
        for i in range(band, band + sub):
            v_sc[ch, i, 0:8] = jnp.zeros((8, LANES), F32)
            v_sc[ch, i, 8 + wide:16 + wide] = jnp.zeros((8, LANES), F32)
        return carry
    lax.fori_loop(0, chunks, clear, 0)
    e_early[sub - 2:early_rows] = jnp.zeros((early_rows - sub + 2, wide, half), BF16)

    ext_cells = m_raw.shape[1]
    tile = 256
    lines_per_tile = tile // 32

    def permute(side):
        m_turn[:, 896:1024] = jnp.zeros((sub * sub, 128), BF16)
        m_turn[:, 0:ext_cells] = m_raw[side].T
        for n_tile in range(m_perm.shape[2] // tile):
            if n_tile == 0:
                spans = [(0, 128), (768, 1024)]
            else:
                first = band + lines_per_tile * (n_tile - 1)
                last = min(first + lines_per_tile, ext - band)
                spans = [(first * ext // 128 * 128, -(-last * ext // 128) * 128)]
            n_at = n_tile * tile + lax.broadcasted_iota(jnp.int32, (1, tile), 1)
            q = lax.shift_right_logical(n_at, 5)
            j = lax.bitwise_and(n_at, 31)
            line = jnp.where(q < band, q, jnp.where(q < 2 * band, q + (ext - 2 * band), q - band))
            ext_col = j + (halo - 8 * side)
            ok = (q < ext) & (ext_col >= 0) & (ext_col < ext)
            want = jnp.where(ok, line * ext + ext_col, -1)
            moved = None
            for lo, hi in spans:
                spot = lo + lax.broadcasted_iota(jnp.int32, (hi - lo, tile), 0)
                pick = jnp.where(spot == want, 1.0, 0.0).astype(BF16)
                part = jnp.dot(m_turn[:, lo:hi], pick, preferred_element_type=F32)
                moved = part if moved is None else moved + part
            m_perm[side, :, n_tile * tile:(n_tile + 1) * tile] = moved.astype(BF16)

    mat_load.wait()
    permute(col)

    kap_pair(other).wait_recv()

    def put_rows(take, at, count):
        for k in range(count):
            for side in range(2):
                line = spread(take(side, k))
                kb[at + k, left + side * sub:left + (side + 1) * sub] = line
                if side == 0:
                    kb[at + k, left - 1:left] = line[0:1]
                else:
                    kb[at + k, left + wide:left + wide + 1] = line[sub - 1:sub]

    def side_faces(e):
        k_mid = kb[e + 1, left:left + wide]
        fw[e] = 0.5 * (k_mid + kb[e + 1, left - 1:left + wide - 1])
        fe[e] = 0.5 * (kb[e + 1, left + 1:left + wide + 1] + k_mid)

    def diag_row(e):
        dg[e] = fv[e] + fv[e + 1] + fw[e] + fe[e]

    def face_row(i):
        fv[i] = 0.5 * (kb[i + 1, left:left + wide] + kb[i, left:left + wide])

    put_rows(lambda side, k: k_raw[side, k:k + 1, :], band, sub)
    fv[halo] = jnp.zeros((wide, LANES), F32)
    fv[halo + sub] = jnp.zeros((wide, LANES), F32)

    def own_face(i, carry):
        face_row(i)
        return carry
    lax.fori_loop(halo + 1, halo + sub, own_face, 0)

    def own_side(e, carry):
        side_faces(e)
        diag_row(e)
        return carry
    lax.fori_loop(halo, halo + sub, own_side, 0)

    def stencil(ch, e, n):
        rows = pl.ds(e, n)
        mid = pl.ds(e + 1, n)
        return (dg[rows] * v_sc[ch, mid, left:left + wide]
                - fv[rows] * v_sc[ch, pl.ds(e, n), left:left + wide]
                - fv[mid] * v_sc[ch, pl.ds(e + 2, n), left:left + wide]
                - fw[rows] * v_sc[ch, mid, left - 1:left + wide - 1]
                - fe[rows] * v_sc[ch, mid, left + 1:left + wide + 1])

    local_bytes(u_sc, load_sem).wait()

    def first_residual(ch):
        remote_bytes(u_fin, pair_send, pair_recv.at[ch]).wait_recv()

        def fill(i, c):
            rows = pl.ds(i * 6, 6)
            v_sc[ch, pl.ds(i * 6 + band, 6), left:left + wide] = u_sc[ch, rows]
            return c
        lax.fori_loop(0, sub // 6, fill, 0)

        def part(i, c):
            rows = pl.ds(halo + i * 6, 6)
            r_sc[ch, rows] = r_sc[ch, rows] - stencil(ch, halo + i * 6, 6)
            return c
        lax.fori_loop(0, sub // 6, part, 0)
        group = (sub - 2) // 2

        def to_e(i, c):
            e_early[pl.ds(i * group, group), :, in_lanes(ch)] = r_sc[ch, pl.ds(i * group + band, group)].astype(BF16)
            return c
        lax.fori_loop(0, 2, to_e, 0)

    first_residual(0)

    mat_pair(other).wait_recv()
    permute(other)

    for ch in range(1, chunks):
        first_residual(ch)

    def early_dot():
        for side in range(2):
            operand = e_early[:, 16 * side:16 * side + 32, :].reshape(early_rows * 32, half)
            acc[side] = jnp.dot(m_perm[side, :, late_k:late_k + early_rows * 32], operand,
                                preferred_element_type=F32)

    early_dot()

    for way, present, r_to in ways:
        @pl.when(present)
        def _():
            remote_bytes(a_recv.at[1 - way], ici_sem.at[way], ar_sem.at[1 - way]).wait_recv()
            put_rows(lambda side, k: a_recv[1 - way, side, 12 + k:13 + k, 0:sub], 0 if way == 0 else band + sub, band)

        @pl.when(jnp.logical_not(present))
        def _():
            for side in range(2):
                a_recv[1 - way, side] = jnp.zeros((16, LANES), F32)
            for i in range(band):
                if way == 0:
                    kb[i] = kb[band]
                else:
                    kb[band + sub + i] = kb[band + sub - 1]

    for i in range(halo + 1):
        face_row(i)
        face_row(halo + sub + i)
    for i in range(halo):
        side_faces(i)
        side_faces(halo + sub + i)
    for i in range(halo + 1):
        diag_row(i)
        diag_row(ext - 1 - i)

    def side_flux(sent, ch, k, e):
        slot = pl.ds(5 * ch + k, 1)
        return fe[e, sub - 1:sub] * (a_recv[sent, 1, slot] - a_recv[sent, 0, slot])

    def near_far(way):
        if way == 0:
            return (halo - 1, halo - 1), ((0, 0), (1, 1))
        return (halo + sub, 0), ((halo + sub + 1, 1), (halo + sub + 2, 2))

    wide_col = lax.broadcasted_iota(jnp.int32, (wide, LANES), 0)

    def late_first(ch):
        for way, present, r_to in ways:
            sent = 1 - way
            (e_near, k_near), far = near_far(way)
            near_at, u_at = (2, 3) if way == 0 else (1, 0)

            @pl.when(present)
            def _():
                remote_bytes(i_recv.at[sent, ch, 0:3], ici_sem.at[way], ir_sem.at[sent, ch]).wait_recv()
                r_sc[ch, e_near] = i_recv[sent, ch, near_at]
                flux = side_flux(sent, ch, k_near, e_near)
                r_sc[ch, e_near, sub - 1:sub] = r_sc[ch, e_near, sub - 1:sub] + flux
                r_sc[ch, e_near, sub:sub + 1] = r_sc[ch, e_near, sub:sub + 1] - flux
                for n in range(2):
                    e, k = far[n]
                    flux = side_flux(sent, ch, k, e)
                    slot = pl.ds(5 * ch + halo + n, 1)
                    got = jnp.concatenate([n_recv[sent, ch, side, n].astype(F32) for side in range(2)], axis=0)
                    got = jnp.where(wide_col == sub - 1, a_recv[sent, 0, slot] + flux, got)
                    got = jnp.where(wide_col == sub, a_recv[sent, 1, slot] - flux, got)
                    e_late[e if way == 0 else e - (ext - 2 * band), :, in_lanes(ch)] = got.astype(BF16)

            @pl.when(jnp.logical_not(present))
            def _():
                i_recv[sent, ch, u_at] = jnp.zeros((wide, LANES), F32)
                rows = pl.ds(0 if way == 0 else halo + sub, halo)
                r_sc[ch, rows] = jnp.zeros((halo, wide, LANES), F32)
                rows = pl.ds(0 if way == 0 else 2 * band - 2, 2)
                e_late[rows, :, in_lanes(ch)] = jnp.zeros((2, wide, LANES), BF16)

        flux = fv[halo] * (i_recv[1, ch, 3] - u_sc[ch, 0])
        near = r_sc[ch, halo - 1] - flux
        own = r_sc[ch, halo] + flux
        r_sc[ch, halo - 1] = near
        r_sc[ch, halo] = own
        e_late[halo - 1, :, in_lanes(ch)] = near.astype(BF16)
        e_late[halo, :, in_lanes(ch)] = own.astype(BF16)
        flux = fv[halo + sub] * (i_recv[0, ch, 0] - u_sc[ch, sub - 1])
        near = r_sc[ch, halo + sub] - flux
        own = r_sc[ch, halo + sub - 1] + flux
        r_sc[ch, halo + sub] = near
        r_sc[ch, halo + sub - 1] = own
        e_late[band, :, in_lanes(ch)] = own.astype(BF16)
        e_late[band + 1, :, in_lanes(ch)] = near.astype(BF16)

    def far_wait():
        for way, present, r_to in ways:
            @pl.when(present)
            def _():
                remote_bytes(i_recv.at[1 - way, :, 0:2], ici_sem.at[way], far_sem.at[1 - way]).wait_recv()

    def far_residual():
        for way, present, r_to in ways:
            sent = 1 - way
            _, far = near_far(way)

            @pl.when(present)
            def _():
                for ch in range(chunks):
                    for n in range(2):
                        e, k = far[n]
                        flux = side_flux(sent, ch, k, e)
                        r_sc[ch, e] = i_recv[sent, ch, n + 2 * way]
                        r_sc[ch, e, sub - 1:sub] = r_sc[ch, e, sub - 1:sub] + flux
                        r_sc[ch, e, sub:sub + 1] = r_sc[ch, e, sub:sub + 1] - flux

    def update(ch, e, n):
        r_new = r_sc[ch, pl.ds(e, n)] - omega * stencil(ch, e, n)
        r_sc[ch, pl.ds(e, n)] = r_new
        return r_new

    def late_next(t, ch):
        for way, present, r_to in ways:
            @pl.when(present)
            def _():
                z_copy(t, ch, 1 - way, r_to).wait_recv()
                at = 0 if way == 0 else band + sub
                v_sc[ch, at:at + band, left:left + wide] = z_recv[1 - way, t, ch].astype(F32)

        e_late[0:band, :, in_lanes(ch)] = update(ch, 0, band).astype(BF16)
        e_late[band:2 * band, :, in_lanes(ch)] = update(ch, ext - band, band).astype(BF16)

    def solve(lanes, side, first, count):
        lo, n = first * sub, count * sub
        cols = pl.ds(pl.multiple_of(16 * side, 16), 32)
        operand = e_late[:, cols, lanes]
        width = operand.shape[2]
        part = acc[side, lo:lo + n, lanes] + jnp.dot(m_perm[side, lo:lo + n, 0:late_k],
                                                     operand.reshape(late_k, width), preferred_element_type=F32)
        return part.reshape(count, sub, width)

    def solve_rows(lanes, first, count):
        return jnp.concatenate([solve(lanes, side, first, count) for side in range(2)], axis=1).astype(BF16)

    def keep_z(ch, first, count, z_bf):
        v_sc[ch, band + first:band + first + count, left:left + wide] = z_bf.astype(F32)

    def solve_and_send(t, ch):
        z_top = solve_rows(in_lanes(ch), 0, band)
        z_bot = solve_rows(in_lanes(ch), sub - band, band)
        z_send[0, t, ch] = z_top
        z_send[1, t, ch] = z_bot
        for way, present, r_to in ways:
            @pl.when(present)
            def _():
                z_copy(t, ch, way, r_to).start()

        keep_z(ch, 0, band, z_top)
        keep_z(ch, sub - band, band, z_bot)

    def interior():
        z_mid = solve_rows(slice(0, half), band, sub - 2 * band)
        for ch in range(chunks):
            keep_z(ch, band, sub - 2 * band, z_mid[:, :, in_lanes(ch)])
        group = (sub - 2) // 2
        for ch in range(chunks):
            def inner(i, c):
                e_early[pl.ds(i * group, group), :, in_lanes(ch)] = update(ch, band + i * group, group).astype(BF16)
                return c
            lax.fori_loop(0, 2, inner, 0)

            def add(i, c):
                rows = pl.ds(i * 6, 6)
                u_sc[ch, rows] = u_sc[ch, rows] + omega * v_sc[ch, pl.ds(i * 6 + band, 6), left:left + wide]
                return c
            lax.fori_loop(0, sub // 6, add, 0)
        early_dot()

    for ch in range(chunks):
        late_first(ch)
        solve_and_send(0, ch)
    interior()

    def sweep_next(t, carry):
        @pl.when(t == 0)
        def _():
            far_wait()
            far_residual()
        for ch in range(chunks):
            late_next(t, ch)
            solve_and_send(t + 1, ch)
        interior()
        return carry
    lax.fori_loop(0, SWEEPS - 2, sweep_next, 0)

    pieces = 2
    piece = sub // pieces

    def out_pair(ch, n, which):
        rows = pl.ds(n * piece, piece)
        return pltpu.make_async_remote_copy(
            src_ref=u_fin.at[ch, rows], dst_ref=out_ref.at[rows, :, lanes_of(which, ch)],
            send_sem=pair_send, recv_sem=out_recv,
            device_id=(other, row), device_id_type=MESH)

    for ch in range(chunks):
        late_next(SWEEPS - 2, ch)
        for n in range(pieces):
            first = n * piece
            z = solve(in_lanes(ch), other, first, piece).astype(BF16).astype(F32)
            u_fin[ch, first:first + piece] = u_sc[ch, first:first + piece, other_cols] + omega * z
            out_pair(ch, n, mine).start()
    z_own = solve(slice(0, half), col, 0, sub).astype(BF16).astype(F32)
    for ch in range(chunks):
        out_ref[:, :, lanes_of(mine, ch)] = u_sc[ch, :, my_cols] + omega * z_own[:, :, in_lanes(ch)]

    kap_pair(col).wait_send()
    mat_pair(col).wait_send()
    for way, present, r_to in ways:
        @pl.when(present)
        def _():
            remote_bytes(v_sc.at[0, 0:23], ici_sem.at[way], ar_sem.at[way]).wait_send()
    remote_bytes(u_fin, pair_send, out_recv).wait_recv()
    remote_bytes(v_sc.at[:, 0:27], pair_send, out_recv).wait_send()


def solution(mesh):
    row_count = mesh.shape['row']
    grid_spec = P('row', 'col', None)

    def device_fn(f_blk, u_blk, kappa_blk, mat_blk, omega_relax):
        sub, _, rhs = u_blk.shape
        ext_cells = mat_blk.shape[3]
        ext = math.isqrt(ext_cells)
        halo = (ext - sub) // 2
        band = halo + 1
        chunks = rhs // (2 * LANES)
        wide = 2 * sub
        early_rows = 24
        hbm = pl.BlockSpec(memory_space=pl.ANY)
        vmem = pltpu.VMEM
        dma = pltpu.SemaphoreType.DMA
        return pl.pallas_call(
            functools.partial(kernel, row_count, sub, halo, chunks),
            out_shape=pltpu.VMEM(u_blk.shape, F32),
            in_specs=[pl.BlockSpec(memory_space=pltpu.SMEM), hbm, hbm, hbm, hbm],
            out_specs=pl.BlockSpec(memory_space=pltpu.VMEM),
            scratch_shapes=[
                vmem((chunks, sub, wide, LANES), F32),
                vmem((chunks, ext, wide, LANES), F32),
                vmem((chunks, ext + 2, 64, LANES), F32),
                vmem((2 * band, wide, chunks * LANES), BF16),
                vmem((early_rows, wide, chunks * LANES), BF16),
                vmem((2, sub * sub, chunks * LANES), F32),
                vmem((2, ext_cells, sub * sub), BF16),
                vmem((sub * sub, 1024), BF16),
                vmem((2, sub * sub, 1024), BF16),
                vmem((2, sub, sub), F32),
                vmem((ext + 2, 64, LANES), F32),
                vmem((sub, 40, LANES), F32),
                vmem((ext + 1, wide, LANES), F32),
                vmem((ext, wide, LANES), F32),
                vmem((ext, wide, LANES), F32),
                vmem((ext, wide, LANES), F32),
                vmem((2, 2 * chunks, band, 40, LANES), F32),
                vmem((2, halo + 1, sub, LANES), F32),
                vmem((2, halo, sub, LANES), F32),
                vmem((2, halo, sub, LANES), F32),
                vmem((2, halo, sub, LANES), F32),
                vmem((2, 2 * chunks, band, sub, LANES), F32),
                vmem((2, chunks, band, wide, LANES), F32),
                vmem((2, 2 * chunks, 2, sub, LANES), BF16),
                vmem((2, chunks, 2, 2, sub, LANES), BF16),
                vmem((2, 2, 16, LANES), F32),
                vmem((2, 2, 16, LANES), F32),
                vmem((2, SWEEPS - 1, chunks, band, wide, LANES), BF16),
                vmem((2, SWEEPS - 1, chunks, band, wide, LANES), BF16),
                vmem((chunks, sub, sub, LANES), F32),
                dma, dma, dma, dma((chunks,)), dma, dma, dma, dma, dma, dma,
                dma((2,)), dma((2, chunks)), dma((2,)), dma((2,)), dma((2, chunks, 2)), dma,
            ],
            compiler_params=pltpu.CompilerParams(collective_id=0, has_side_effects=True,
                                                 vmem_limit_bytes=61000 * 1024),
        )(omega_relax.reshape(1), f_blk, u_blk, kappa_blk, mat_blk[0, 0].T)

    return jax.shard_map(device_fn, mesh=mesh,
                         in_specs=(grid_spec, grid_spec, P('row', 'col'), P('row', 'col', None, None), P()),
                         out_specs=grid_spec, check_vma=False)
```

```python
import functools
import math

import jax
import jax.numpy as jnp
from jax import lax
from jax.experimental import pallas as pl
from jax.experimental.pallas import tpu as pltpu
from jax.sharding import PartitionSpec as P

SWEEPS = 6
ORDER = (((1, 0, 0), (1, 0, 1), (0, 0, 0), (1, 1, 0), (1, 1, 1), (0, 0, 1), (0, 1, 0), (0, 1, 1)), ((1, 1, 0), (1, 1, 1), (1, 0, 0), (1, 0, 1), (0, 1, 0), (0, 1, 1), (0, 0, 0), (0, 0, 1)))
LANES = 128
MESH = pl.DeviceIdType.MESH
F32 = jnp.float32
BF16 = jnp.bfloat16


def kernel(row_count, sub, halo, chunks,
           om_ref, f_hbm, u_hbm, kap_hbm, mat_hbm, out_ref,
           u_sc, r_sc, v_sc, e_late, e_early, acc, m_raw, m_turn, m_perm,
           k_raw, kb, ko, fv, fw, fe, dg, u_band, pv, pw, pe, pd, i_send, i_recv, n_send, n_recv, a_send, a_recv,
           z_send, z_recv, u_fin,
           load_sem, band_sem, pair_send, pair_recv, mat_sem, mat_send, mat_recv, kap_loc, kap_send, kap_recv,
           ici_sem, ir_sem, far_sem, ar_sem, zr_sem, out_recv):
    wide = 2 * sub
    ext = sub + 2 * halo
    band = halo + 1
    late_k = 2 * band * 32
    early_rows = e_early.shape[0]
    half = chunks * LANES
    left = 8

    row = lax.axis_index('row')
    col = lax.axis_index('col')
    other = 1 - col
    mine = lax.rem(row + col, 2)
    theirs = 1 - mine
    has_up = row > 0
    has_dn = row < row_count - 1
    ways = ((0, has_up, jnp.maximum(row - 1, 0)), (1, has_dn, jnp.minimum(row + 1, row_count - 1)))
    up_row, dn_row = ways[0][2], ways[1][2]
    col_spans = [pl.ds(side * sub, sub) for side in range(2)]
    my_cols = pl.ds(pl.multiple_of(col * sub, 8), sub)
    other_cols = pl.ds(pl.multiple_of(other * sub, 8), sub)
    own_rows = pl.ds(halo, sub)

    def lanes_of(which, ch):
        return pl.ds(pl.multiple_of(which * half + ch * LANES, LANES), LANES)

    def local_bytes(ref, sem):
        return pltpu.make_async_copy(ref, ref, sem)

    def remote_bytes(ref, send_sem, recv_sem):
        return pltpu.make_async_remote_copy(src_ref=ref, dst_ref=ref, send_sem=send_sem, recv_sem=recv_sem,
                                            device_id=(other, row), device_id_type=MESH)

    barrier = pltpu.get_barrier_semaphore()

    def in_lanes(ch):
        return slice(ch * LANES, (ch + 1) * LANES)

    def greet(r_to, c_to):
        pl.semaphore_signal(barrier, inc=1, device_id=(c_to, r_to), device_id_type=MESH)

    for _, present, r_to in ways:
        @pl.when(present)
        def _():
            greet(r_to, col)
            greet(r_to, other)
    greet(row, other)

    kap_load = pltpu.make_async_copy(kap_hbm, k_raw.at[col], kap_loc)
    kap_load.start()

    def band_loads(way, g):
        lanes = pl.ds(g * LANES, LANES)
        u_from = pl.ds(0 if way == 0 else sub - band, band)
        f_from = pl.ds(0 if way == 0 else sub - halo, halo)
        return (pltpu.make_async_copy(u_hbm.at[u_from, :, lanes], u_band.at[way, g, :, 8:8 + sub, :],
                                      band_sem),
                pltpu.make_async_copy(f_hbm.at[f_from, :, lanes], i_send.at[way, g, pl.ds(1 - way, halo)],
                                      band_sem))

    for g in range(2 * chunks):
        for way in range(2):
            for load in band_loads(way, g):
                load.start()

    def u_load(ch):
        return pltpu.make_async_copy(u_hbm.at[:, :, lanes_of(mine, ch)], u_sc.at[ch, :, my_cols, :], load_sem)

    def f_load(ch):
        return pltpu.make_async_copy(f_hbm.at[:, :, lanes_of(mine, ch)], r_sc.at[ch, own_rows, my_cols, :],
                                     load_sem)

    mat_load = pltpu.make_async_copy(mat_hbm, m_raw.at[col], mat_sem)
    mat_load.start()
    for ch in range(chunks):
        u_load(ch).start()
        f_load(ch).start()

    def u_pair(ch, cols):
        return pltpu.make_async_remote_copy(
            src_ref=u_hbm.at[:, :, lanes_of(theirs, ch)], dst_ref=u_sc.at[ch, :, cols, :],
            send_sem=pair_send, recv_sem=pair_recv.at[ch],
            device_id=(other, row), device_id_type=MESH)

    def f_pair(ch, cols):
        return pltpu.make_async_remote_copy(
            src_ref=f_hbm.at[:, :, lanes_of(theirs, ch)], dst_ref=r_sc.at[ch, own_rows, cols, :],
            send_sem=pair_send, recv_sem=pair_recv.at[ch],
            device_id=(other, row), device_id_type=MESH)

    def mat_pair(slot):
        return pltpu.make_async_remote_copy(
            src_ref=mat_hbm, dst_ref=m_raw.at[slot],
            send_sem=mat_send, recv_sem=mat_recv,
            device_id=(other, row), device_id_type=MESH)

    def kap_pair(slot):
        return pltpu.make_async_remote_copy(
            src_ref=k_raw.at[col], dst_ref=k_raw.at[slot],
            send_sem=kap_send, recv_sem=kap_recv,
            device_id=(other, row), device_id_type=MESH)

    def half_at(core):
        return lax.rem(core + row + 1, 2)

    near_rows = (pl.ds(0, 2), pl.ds(2, 2))
    far_rows = (pl.ds(2, 2), pl.ds(0, 2))

    def init_send(way, r_to, core, ch, rows, recv_sem):
        g = half_at(core) * chunks + ch
        return pltpu.make_async_remote_copy(
            src_ref=i_send.at[way, g, rows], dst_ref=i_recv.at[way, ch, rows, my_cols, :],
            send_sem=ici_sem.at[way], recv_sem=recv_sem,
            device_id=(core, r_to), device_id_type=MESH)

    def narrow_send(way, r_to, core, ch):
        return pltpu.make_async_remote_copy(
            src_ref=n_send.at[way, half_at(core) * chunks + ch], dst_ref=n_recv.at[way, ch, col],
            send_sem=ici_sem.at[way], recv_sem=ir_sem.at[way, ch],
            device_id=(core, r_to), device_id_type=MESH)

    def aux_send(way, r_to, core):
        return pltpu.make_async_remote_copy(
            src_ref=a_send.at[way, half_at(core)], dst_ref=a_recv.at[way, col],
            send_sem=ici_sem.at[way], recv_sem=ar_sem.at[way],
            device_id=(core, r_to), device_id_type=MESH)

    def z_copy(t, ch, way, r_to):
        return pltpu.make_async_remote_copy(
            src_ref=z_send.at[way, t, ch], dst_ref=z_recv.at[way, t, ch],
            send_sem=ici_sem.at[way], recv_sem=zr_sem.at[t % 2, ch, way],
            device_id=(other, r_to), device_id_type=MESH)

    omega = om_ref[0]
    for way in range(2):
        for g in range(2 * chunks):
            u_band[way, g, :, 0:8] = jnp.zeros((band, 8, LANES), F32)
            u_band[way, g, :, 8 + sub:16 + sub] = jnp.zeros((band, 8, LANES), F32)
        for h in range(2):
            a_send[way, h] = jnp.zeros((16, LANES), F32)

    eye = lax.broadcasted_iota(jnp.int32, (sub, sub), 0) == lax.broadcasted_iota(jnp.int32, (sub, sub), 1)

    def spread(line):
        picked = jnp.where(eye, jnp.broadcast_to(line, (sub, sub)), 0.0)
        return jnp.broadcast_to(jnp.sum(picked, axis=1, keepdims=True), (sub, LANES))

    kap_load.wait()
    for k in range(sub):
        line = spread(k_raw[col, k:k + 1, :])
        ko[k, 8:8 + sub] = line
        ko[k, 7:8] = line[0:1]
        ko[k, 8 + sub:9 + sub] = line[sub - 1:sub]
    spot_col = lax.broadcasted_iota(jnp.int32, (sub, LANES), 0)
    cut_w = (spot_col == 0) & (col == 1)
    cut_e = (spot_col == sub - 1) & (col == 0)
    for way in range(2):
        first = 0 if way == 0 else sub - halo
        for k in range(halo):
            at = first + k
            mid = ko[at, 8:8 + sub]
            pw[way, k] = jnp.where(cut_w, 0.0, 0.5 * (mid + ko[at, 7:7 + sub]))
            pe[way, k] = jnp.where(cut_e, 0.0, 0.5 * (ko[at, 9:9 + sub] + mid))
            total = pw[way, k] + pe[way, k]
            if at > 0:
                pv[way, k] = 0.5 * (mid + ko[at - 1, 8:8 + sub])
                total = total + pv[way, k]
            if at < sub - 1:
                pv[way, k + 1] = 0.5 * (ko[at + 1, 8:8 + sub] + mid)
                total = total + pv[way, k + 1]
            pd[way, k] = total

    local_bytes(v_sc.at[0, 0:21], band_sem).wait()
    for way in range(2):
        for h in range(2):
            first = 0 if way == 0 else sub - band
            a_send[way, h, 12:12 + band, 0:sub] = k_raw[col, first:first + band]
    for g in range(2 * chunks):
        h, ch = g // chunks, g % chunks
        for way in range(2):
            shift = way
            for k in range(halo):
                line = shift + k
                at = k + 1 - way
                au = (pd[way, k] * u_band[way, g, line, 8:8 + sub]
                      - pw[way, k] * u_band[way, g, line, 7:7 + sub]
                      - pe[way, k] * u_band[way, g, line, 9:9 + sub])
                if line > 0:
                    au = au - pv[way, k] * u_band[way, g, line - 1, 8:8 + sub]
                if line < band - 1:
                    au = au - pv[way, k + 1] * u_band[way, g, line + 1, 8:8 + sub]
                part = i_send[way, g, at] - au
                i_send[way, g, at] = part
                edge = jnp.where(col == 0, u_band[way, g, line, 7 + sub:8 + sub], u_band[way, g, line, 8:9])
                slot = 5 * ch + k
                a_send[way, h, slot:slot + 1] = edge
                far = k - 1 + way
                if 0 <= far < 2:
                    n_send[way, g, far] = part.astype(BF16)
                    slot = 5 * ch + halo + far
                    a_send[way, h, slot:slot + 1] = jnp.where(col == 0, part[sub - 1:sub], part[0:1])
            i_send[way, g, halo * way] = u_band[way, g, halo * way, 8:8 + sub]

    pl.semaphore_wait(barrier, 1 + 2 * has_up.astype(jnp.int32) + 2 * has_dn.astype(jnp.int32))

    for way, present, r_to in ways:
        @pl.when(present)
        def _():
            for core in range(2):
                aux_send(way, r_to, core).start()
            for near, core, ch in ORDER[way]:
                if near:
                    init_send(way, r_to, core, ch, near_rows[way], ir_sem.at[way, ch]).start()
                    narrow_send(way, r_to, core, ch).start()
                else:
                    init_send(way, r_to, core, ch, far_rows[way], far_sem.at[way]).start()
    kap_pair(col).start()
    u_pair(0, my_cols).start()
    f_pair(0, my_cols).start()
    mat_pair(col).start()
    for ch in range(1, chunks):
        u_pair(ch, my_cols).start()
        f_pair(ch, my_cols).start()

    def clear(ch, carry):
        for i in list(range(band)) + list(range(band + sub, ext + 2)):
            v_sc[ch, i] = jnp.zeros(v_sc.shape[2:], F32)
        for i in range(band, band + sub):
            v_sc[ch, i, 0:8] = jnp.zeros((8, LANES), F32)
            v_sc[ch, i, 8 + wide:16 + wide] = jnp.zeros((8, LANES), F32)
        return carry
    lax.fori_loop(0, chunks, clear, 0)
    e_early[sub - 2:early_rows] = jnp.zeros((early_rows - sub + 2, wide, half), BF16)

    ext_cells = m_raw.shape[1]
    tile = 256
    lines_per_tile = tile // 32

    def permute(side):
        m_turn[:, 896:1024] = jnp.zeros((sub * sub, 128), BF16)
        m_turn[:, 0:ext_cells] = m_raw[side].T
        for n_tile in range(m_perm.shape[2] // tile):
            if n_tile == 0:
                spans = [(0, 128), (768, 1024)]
            else:
                first = band + lines_per_tile * (n_tile - 1)
                last = min(first + lines_per_tile, ext - band)
                spans = [(first * ext // 128 * 128, -(-last * ext // 128) * 128)]
            n_at = n_tile * tile + lax.broadcasted_iota(jnp.int32, (1, tile), 1)
            q = lax.shift_right_logical(n_at, 5)
            j = lax.bitwise_and(n_at, 31)
            line = jnp.where(q < band, q, jnp.where(q < 2 * band, q + (ext - 2 * band), q - band))
            ext_col = j + (halo - 8 * side)
            ok = (q < ext) & (ext_col >= 0) & (ext_col < ext)
            want = jnp.where(ok, line * ext + ext_col, -1)
            moved = None
            for lo, hi in spans:
                spot = lo + lax.broadcasted_iota(jnp.int32, (hi - lo, tile), 0)
                pick = jnp.where(spot == want, 1.0, 0.0).astype(BF16)
                part = jnp.dot(m_turn[:, lo:hi], pick, preferred_element_type=F32)
                moved = part if moved is None else moved + part
            m_perm[side, :, n_tile * tile:(n_tile + 1) * tile] = moved.astype(BF16)

    mat_load.wait()
    permute(col)

    kap_pair(other).wait_recv()

    def put_rows(take, at, count):
        for k in range(count):
            for side in range(2):
                line = spread(take(side, k))
                kb[at + k, left + side * sub:left + (side + 1) * sub] = line
                if side == 0:
                    kb[at + k, left - 1:left] = line[0:1]
                else:
                    kb[at + k, left + wide:left + wide + 1] = line[sub - 1:sub]

    def side_faces(e):
        k_mid = kb[e + 1, left:left + wide]
        fw[e] = 0.5 * (k_mid + kb[e + 1, left - 1:left + wide - 1])
        fe[e] = 0.5 * (kb[e + 1, left + 1:left + wide + 1] + k_mid)

    def diag_row(e):
        dg[e] = fv[e] + fv[e + 1] + fw[e] + fe[e]

    def face_row(i):
        fv[i] = 0.5 * (kb[i + 1, left:left + wide] + kb[i, left:left + wide])

    put_rows(lambda side, k: k_raw[side, k:k + 1, :], band, sub)
    fv[halo] = jnp.zeros((wide, LANES), F32)
    fv[halo + sub] = jnp.zeros((wide, LANES), F32)

    def own_face(i, carry):
        face_row(i)
        return carry
    lax.fori_loop(halo + 1, halo + sub, own_face, 0)

    def own_side(e, carry):
        side_faces(e)
        diag_row(e)
        return carry
    lax.fori_loop(halo, halo + sub, own_side, 0)

    def stencil(ch, e, n):
        rows = pl.ds(e, n)
        mid = pl.ds(e + 1, n)
        return (dg[rows] * v_sc[ch, mid, left:left + wide]
                - fv[rows] * v_sc[ch, pl.ds(e, n), left:left + wide]
                - fv[mid] * v_sc[ch, pl.ds(e + 2, n), left:left + wide]
                - fw[rows] * v_sc[ch, mid, left - 1:left + wide - 1]
                - fe[rows] * v_sc[ch, mid, left + 1:left + wide + 1])

    local_bytes(u_sc, load_sem).wait()

    def first_residual(ch):
        remote_bytes(u_fin, pair_send, pair_recv.at[ch]).wait_recv()

        def fill(i, c):
            rows = pl.ds(i * 6, 6)
            v_sc[ch, pl.ds(i * 6 + band, 6), left:left + wide] = u_sc[ch, rows]
            return c
        lax.fori_loop(0, sub // 6, fill, 0)

        def part(i, c):
            rows = pl.ds(halo + i * 6, 6)
            r_sc[ch, rows] = r_sc[ch, rows] - stencil(ch, halo + i * 6, 6)
            return c
        lax.fori_loop(0, sub // 6, part, 0)
        group = (sub - 2) // 2

        def to_e(i, c):
            e_early[pl.ds(i * group, group), :, in_lanes(ch)] = r_sc[ch, pl.ds(i * group + band, group)].astype(BF16)
            return c
        lax.fori_loop(0, 2, to_e, 0)

    first_residual(0)

    mat_pair(other).wait_recv()
    permute(other)

    for ch in range(1, chunks):
        first_residual(ch)

    def early_dot():
        for side in range(2):
            operand = e_early[:, 16 * side:16 * side + 32, :].reshape(early_rows * 32, half)
            acc[side] = jnp.dot(m_perm[side, :, late_k:late_k + early_rows * 32], operand,
                                preferred_element_type=F32)

    early_dot()

    for way, present, r_to in ways:
        @pl.when(present)
        def _():
            remote_bytes(a_recv.at[1 - way], ici_sem.at[way], ar_sem.at[1 - way]).wait_recv()
            put_rows(lambda side, k: a_recv[1 - way, side, 12 + k:13 + k, 0:sub], 0 if way == 0 else band + sub, band)

        @pl.when(jnp.logical_not(present))
        def _():
            for side in range(2):
                a_recv[1 - way, side] = jnp.zeros((16, LANES), F32)
            for i in range(band):
                if way == 0:
                    kb[i] = kb[band]
                else:
                    kb[band + sub + i] = kb[band + sub - 1]

    for i in range(halo + 1):
        face_row(i)
        face_row(halo + sub + i)
    for i in range(halo):
        side_faces(i)
        side_faces(halo + sub + i)
    for i in range(halo + 1):
        diag_row(i)
        diag_row(ext - 1 - i)

    def side_flux(sent, ch, k, e):
        slot = pl.ds(5 * ch + k, 1)
        return fe[e, sub - 1:sub] * (a_recv[sent, 1, slot] - a_recv[sent, 0, slot])

    def near_far(way):
        if way == 0:
            return (halo - 1, halo - 1), ((0, 0), (1, 1))
        return (halo + sub, 0), ((halo + sub + 1, 1), (halo + sub + 2, 2))

    wide_col = lax.broadcasted_iota(jnp.int32, (wide, LANES), 0)

    def late_first(ch):
        for way, present, r_to in ways:
            sent = 1 - way
            (e_near, k_near), far = near_far(way)
            near_at, u_at = (2, 3) if way == 0 else (1, 0)

            @pl.when(present)
            def _():
                remote_bytes(i_recv.at[sent, ch, 0:3], ici_sem.at[way], ir_sem.at[sent, ch]).wait_recv()
                r_sc[ch, e_near] = i_recv[sent, ch, near_at]
                flux = side_flux(sent, ch, k_near, e_near)
                r_sc[ch, e_near, sub - 1:sub] = r_sc[ch, e_near, sub - 1:sub] + flux
                r_sc[ch, e_near, sub:sub + 1] = r_sc[ch, e_near, sub:sub + 1] - flux
                for n in range(2):
                    e, k = far[n]
                    flux = side_flux(sent, ch, k, e)
                    slot = pl.ds(5 * ch + halo + n, 1)
                    got = jnp.concatenate([n_recv[sent, ch, side, n].astype(F32) for side in range(2)], axis=0)
                    got = jnp.where(wide_col == sub - 1, a_recv[sent, 0, slot] + flux, got)
                    got = jnp.where(wide_col == sub, a_recv[sent, 1, slot] - flux, got)
                    e_late[e if way == 0 else e - (ext - 2 * band), :, in_lanes(ch)] = got.astype(BF16)

            @pl.when(jnp.logical_not(present))
            def _():
                i_recv[sent, ch, u_at] = jnp.zeros((wide, LANES), F32)
                rows = pl.ds(0 if way == 0 else halo + sub, halo)
                r_sc[ch, rows] = jnp.zeros((halo, wide, LANES), F32)
                rows = pl.ds(0 if way == 0 else 2 * band - 2, 2)
                e_late[rows, :, in_lanes(ch)] = jnp.zeros((2, wide, LANES), BF16)

        flux = fv[halo] * (i_recv[1, ch, 3] - u_sc[ch, 0])
        near = r_sc[ch, halo - 1] - flux
        own = r_sc[ch, halo] + flux
        r_sc[ch, halo - 1] = near
        r_sc[ch, halo] = own
        e_late[halo - 1, :, in_lanes(ch)] = near.astype(BF16)
        e_late[halo, :, in_lanes(ch)] = own.astype(BF16)
        flux = fv[halo + sub] * (i_recv[0, ch, 0] - u_sc[ch, sub - 1])
        near = r_sc[ch, halo + sub] - flux
        own = r_sc[ch, halo + sub - 1] + flux
        r_sc[ch, halo + sub] = near
        r_sc[ch, halo + sub - 1] = own
        e_late[band, :, in_lanes(ch)] = own.astype(BF16)
        e_late[band + 1, :, in_lanes(ch)] = near.astype(BF16)

    def far_wait():
        for way, present, r_to in ways:
            @pl.when(present)
            def _():
                remote_bytes(i_recv.at[1 - way, :, 0:2], ici_sem.at[way], far_sem.at[1 - way]).wait_recv()

    def far_residual():
        for way, present, r_to in ways:
            sent = 1 - way
            _, far = near_far(way)

            @pl.when(present)
            def _():
                for ch in range(chunks):
                    for n in range(2):
                        e, k = far[n]
                        flux = side_flux(sent, ch, k, e)
                        r_sc[ch, e] = i_recv[sent, ch, n + 2 * way]
                        r_sc[ch, e, sub - 1:sub] = r_sc[ch, e, sub - 1:sub] + flux
                        r_sc[ch, e, sub:sub + 1] = r_sc[ch, e, sub:sub + 1] - flux

    def update(ch, e, n):
        r_new = r_sc[ch, pl.ds(e, n)] - omega * stencil(ch, e, n)
        r_sc[ch, pl.ds(e, n)] = r_new
        return r_new

    slow = lax.rem(row, 2)

    def towards(way):
        return jnp.where(way == 0, has_up, has_dn), jnp.where(way == 0, up_row, dn_row)

    def late_next(t, ch):
        for way in (1 - slow, slow):
            present, r_to = towards(way)

            @pl.when(present)
            def _():
                z_copy(t, ch, 1 - way, r_to).wait_recv()
                v_sc[ch, pl.ds(way * (band + sub), band), left:left + wide] = z_recv[1 - way, t, ch].astype(F32)

            e_late[pl.ds(way * band, band), :, in_lanes(ch)] = update(ch, way * (ext - band), band).astype(BF16)

    def solve(lanes, side, first, count):
        n = count * sub
        rows = pl.ds(first * sub if isinstance(first, int) else pl.multiple_of(first * sub, 32), n)
        cols = pl.ds(pl.multiple_of(16 * side, 16), 32)
        operand = e_late[:, cols, lanes]
        width = operand.shape[2]
        part = acc[side, rows, lanes] + jnp.dot(m_perm[side, rows, 0:late_k],
                                                     operand.reshape(late_k, width), preferred_element_type=F32)
        return part.reshape(count, sub, width)

    def solve_rows(lanes, first, count):
        return jnp.concatenate([solve(lanes, side, first, count) for side in range(2)], axis=1).astype(BF16)

    def keep_z(ch, first, count, z_bf):
        v_sc[ch, pl.ds(band + first, count), left:left + wide] = z_bf.astype(F32)

    def solve_and_send(t, ch):
        for way in (slow, 1 - slow):
            present, r_to = towards(way)
            first = way * (sub - band)
            z_bf = solve_rows(in_lanes(ch), first, band)
            z_send[way, t, ch] = z_bf

            @pl.when(present)
            def _():
                z_copy(t, ch, way, r_to).start()

            keep_z(ch, first, band, z_bf)

    def interior():
        z_mid = solve_rows(slice(0, half), band, sub - 2 * band)
        for ch in range(chunks):
            keep_z(ch, band, sub - 2 * band, z_mid[:, :, in_lanes(ch)])
        group = (sub - 2) // 2
        for ch in range(chunks):
            def inner(i, c):
                e_early[pl.ds(i * group, group), :, in_lanes(ch)] = update(ch, band + i * group, group).astype(BF16)
                return c
            lax.fori_loop(0, 2, inner, 0)

            def add(i, c):
                rows = pl.ds(i * 6, 6)
                u_sc[ch, rows] = u_sc[ch, rows] + omega * v_sc[ch, pl.ds(i * 6 + band, 6), left:left + wide]
                return c
            lax.fori_loop(0, sub // 6, add, 0)
        early_dot()

    for ch in range(chunks):
        late_first(ch)
        solve_and_send(0, ch)
    interior()

    def sweep_next(t, carry):
        @pl.when(t == 0)
        def _():
            far_wait()
            far_residual()
        for ch in range(chunks):
            late_next(t, ch)
            solve_and_send(t + 1, ch)
        interior()
        return carry
    lax.fori_loop(0, SWEEPS - 2, sweep_next, 0)

    cuts = (0, 16, sub)

    def out_pair(ch, n, which):
        rows = pl.ds(cuts[n], cuts[n + 1] - cuts[n])
        return pltpu.make_async_remote_copy(
            src_ref=u_fin.at[ch, rows], dst_ref=out_ref.at[rows, :, lanes_of(which, ch)],
            send_sem=pair_send, recv_sem=out_recv,
            device_id=(other, row), device_id_type=MESH)

    for ch in range(chunks):
        late_next(SWEEPS - 2, ch)
        for n in range(2):
            first, past = cuts[n], cuts[n + 1]
            z = solve(in_lanes(ch), other, first, past - first).astype(BF16).astype(F32)
            u_fin[ch, first:past] = u_sc[ch, first:past, other_cols] + omega * z
            out_pair(ch, n, mine).start()
    z_own = solve(slice(0, half), col, 0, sub).astype(BF16).astype(F32)
    for ch in range(chunks):
        out_ref[:, :, lanes_of(mine, ch)] = u_sc[ch, :, my_cols] + omega * z_own[:, :, in_lanes(ch)]

    kap_pair(col).wait_send()
    mat_pair(col).wait_send()
    for way, present, r_to in ways:
        @pl.when(present)
        def _():
            remote_bytes(v_sc.at[0, 0:23], ici_sem.at[way], ar_sem.at[way]).wait_send()
    remote_bytes(u_fin, pair_send, out_recv).wait_recv()
    remote_bytes(v_sc.at[:, 0:27], pair_send, out_recv).wait_send()


def solution(mesh):
    row_count = mesh.shape['row']
    grid_spec = P('row', 'col', None)

    def device_fn(f_blk, u_blk, kappa_blk, mat_blk, omega_relax):
        sub, _, rhs = u_blk.shape
        ext_cells = mat_blk.shape[3]
        ext = math.isqrt(ext_cells)
        halo = (ext - sub) // 2
        band = halo + 1
        chunks = rhs // (2 * LANES)
        wide = 2 * sub
        early_rows = 24
        hbm = pl.BlockSpec(memory_space=pl.ANY)
        vmem = pltpu.VMEM
        dma = pltpu.SemaphoreType.DMA
        return pl.pallas_call(
            functools.partial(kernel, row_count, sub, halo, chunks),
            out_shape=pltpu.VMEM(u_blk.shape, F32),
            in_specs=[pl.BlockSpec(memory_space=pltpu.SMEM), hbm, hbm, hbm, hbm],
            out_specs=pl.BlockSpec(memory_space=pltpu.VMEM),
            scratch_shapes=[
                vmem((chunks, sub, wide, LANES), F32),
                vmem((chunks, ext, wide, LANES), F32),
                vmem((chunks, ext + 2, 64, LANES), F32),
                vmem((2 * band, wide, chunks * LANES), BF16),
                vmem((early_rows, wide, chunks * LANES), BF16),
                vmem((2, sub * sub, chunks * LANES), F32),
                vmem((2, ext_cells, sub * sub), BF16),
                vmem((sub * sub, 1024), BF16),
                vmem((2, sub * sub, 1024), BF16),
                vmem((2, sub, sub), F32),
                vmem((ext + 2, 64, LANES), F32),
                vmem((sub, 40, LANES), F32),
                vmem((ext + 1, wide, LANES), F32),
                vmem((ext, wide, LANES), F32),
                vmem((ext, wide, LANES), F32),
                vmem((ext, wide, LANES), F32),
                vmem((2, 2 * chunks, band, 40, LANES), F32),
                vmem((2, halo + 1, sub, LANES), F32),
                vmem((2, halo, sub, LANES), F32),
                vmem((2, halo, sub, LANES), F32),
                vmem((2, halo, sub, LANES), F32),
                vmem((2, 2 * chunks, band, sub, LANES), F32),
                vmem((2, chunks, band, wide, LANES), F32),
                vmem((2, 2 * chunks, 2, sub, LANES), BF16),
                vmem((2, chunks, 2, 2, sub, LANES), BF16),
                vmem((2, 2, 16, LANES), F32),
                vmem((2, 2, 16, LANES), F32),
                vmem((2, SWEEPS - 1, chunks, band, wide, LANES), BF16),
                vmem((2, SWEEPS - 1, chunks, band, wide, LANES), BF16),
                vmem((chunks, sub, sub, LANES), F32),
                dma, dma, dma, dma((chunks,)), dma, dma, dma, dma, dma, dma,
                dma((2,)), dma((2, chunks)), dma((2,)), dma((2,)), dma((2, chunks, 2)), dma,
            ],
            compiler_params=pltpu.CompilerParams(collective_id=0, has_side_effects=True,
                                                 vmem_limit_bytes=61000 * 1024),
        )(omega_relax.reshape(1), f_blk, u_blk, kappa_blk, mat_blk[0, 0].T)

    return jax.shard_map(device_fn, mesh=mesh,
                         in_specs=(grid_spec, grid_spec, P('row', 'col'), P('row', 'col', None, None), P()),
                         out_specs=grid_spec, check_vma=False)
```

```python
import functools
import math

import jax
import jax.numpy as jnp
from jax import lax
from jax.experimental import pallas as pl
from jax.experimental.pallas import tpu as pltpu
from jax.sharding import PartitionSpec as P

SWEEPS = 6
LANES = 128
MESH = pl.DeviceIdType.MESH
F32 = jnp.float32
BF16 = jnp.bfloat16


def kernel(row_count, sub, halo, chunks,
           om_ref, f_hbm, u_hbm, kap_hbm, mat_hbm, out_ref,
           u_sc, r_sc, v_sc, e_late, e_early, acc, m_raw, m_turn, m_perm,
           k_raw, kb, ko, fv, fw, fe, dg, u_band, pv, pw, pe, pd, i_send, i_recv, n_send, n_recv, a_send, a_recv,
           z_send, z_recv, u_fin,
           load_sem, band_sem, pair_send, pair_recv, mat_sem, mat_send, mat_recv, kap_loc, kap_send, kap_recv,
           ici_sem, ir_sem, far_sem, ar_sem, zr_sem, out_recv):
    wide = 2 * sub
    ext = sub + 2 * halo
    band = halo + 1
    late_k = 2 * band * 32
    early_rows = e_early.shape[0]
    half = chunks * LANES
    left = 8

    row = lax.axis_index('row')
    col = lax.axis_index('col')
    other = 1 - col
    mine = lax.rem(row + col, 2)
    theirs = 1 - mine
    has_up = row > 0
    has_dn = row < row_count - 1
    ways = ((0, has_up, jnp.maximum(row - 1, 0)), (1, has_dn, jnp.minimum(row + 1, row_count - 1)))
    up_row, dn_row = ways[0][2], ways[1][2]
    col_spans = [pl.ds(side * sub, sub) for side in range(2)]
    my_cols = pl.ds(pl.multiple_of(col * sub, 8), sub)
    other_cols = pl.ds(pl.multiple_of(other * sub, 8), sub)
    own_rows = pl.ds(halo, sub)

    def lanes_of(which, ch):
        return pl.ds(pl.multiple_of(which * half + ch * LANES, LANES), LANES)

    def local_bytes(ref, sem):
        return pltpu.make_async_copy(ref, ref, sem)

    def remote_bytes(ref, send_sem, recv_sem):
        return pltpu.make_async_remote_copy(src_ref=ref, dst_ref=ref, send_sem=send_sem, recv_sem=recv_sem,
                                            device_id=(other, row), device_id_type=MESH)

    barrier = pltpu.get_barrier_semaphore()

    def in_lanes(ch):
        return slice(ch * LANES, (ch + 1) * LANES)

    def greet(r_to, c_to):
        pl.semaphore_signal(barrier, inc=1, device_id=(c_to, r_to), device_id_type=MESH)

    for _, present, r_to in ways:
        @pl.when(present)
        def _():
            greet(r_to, col)
            greet(r_to, other)
    greet(row, other)

    kap_load = pltpu.make_async_copy(kap_hbm, k_raw.at[col], kap_loc)
    kap_load.start()

    def band_loads(way, g):
        lanes = pl.ds(g * LANES, LANES)
        u_from = pl.ds(0 if way == 0 else sub - band, band)
        f_from = pl.ds(0 if way == 0 else sub - halo, halo)
        return (pltpu.make_async_copy(u_hbm.at[u_from, :, lanes], u_band.at[way, g, :, 8:8 + sub, :],
                                      band_sem),
                pltpu.make_async_copy(f_hbm.at[f_from, :, lanes], i_send.at[way, g, pl.ds(1 - way, halo)],
                                      band_sem))

    for g in range(2 * chunks):
        for way in range(2):
            for load in band_loads(way, g):
                load.start()

    def u_load(ch):
        return pltpu.make_async_copy(u_hbm.at[:, :, lanes_of(mine, ch)], u_sc.at[ch, :, my_cols, :], load_sem)

    def f_load(ch):
        return pltpu.make_async_copy(f_hbm.at[:, :, lanes_of(mine, ch)], r_sc.at[ch, own_rows, my_cols, :],
                                     load_sem)

    mat_load = pltpu.make_async_copy(mat_hbm, m_raw.at[col], mat_sem)
    mat_load.start()
    for ch in range(chunks):
        u_load(ch).start()
        f_load(ch).start()

    def u_pair(ch, cols):
        return pltpu.make_async_remote_copy(
            src_ref=u_hbm.at[:, :, lanes_of(theirs, ch)], dst_ref=u_sc.at[ch, :, cols, :],
            send_sem=pair_send, recv_sem=pair_recv.at[ch],
            device_id=(other, row), device_id_type=MESH)

    def f_pair(ch, cols):
        return pltpu.make_async_remote_copy(
            src_ref=f_hbm.at[:, :, lanes_of(theirs, ch)], dst_ref=r_sc.at[ch, own_rows, cols, :],
            send_sem=pair_send, recv_sem=pair_recv.at[ch],
            device_id=(other, row), device_id_type=MESH)

    def mat_pair(slot):
        return pltpu.make_async_remote_copy(
            src_ref=mat_hbm, dst_ref=m_raw.at[slot],
            send_sem=mat_send, recv_sem=mat_recv,
            device_id=(other, row), device_id_type=MESH)

    def kap_pair(slot):
        return pltpu.make_async_remote_copy(
            src_ref=k_raw.at[col], dst_ref=k_raw.at[slot],
            send_sem=kap_send, recv_sem=kap_recv,
            device_id=(other, row), device_id_type=MESH)

    def half_at(core):
        return lax.rem(core + row + 1, 2)

    near_rows = (pl.ds(0, 2), pl.ds(2, 2))
    far_rows = (pl.ds(2, 2), pl.ds(0, 2))

    def init_send(way, r_to, core, ch, rows, recv_sem):
        g = half_at(core) * chunks + ch
        return pltpu.make_async_remote_copy(
            src_ref=i_send.at[way, g, rows], dst_ref=i_recv.at[way, ch, rows, my_cols, :],
            send_sem=ici_sem.at[way], recv_sem=recv_sem,
            device_id=(core, r_to), device_id_type=MESH)

    def narrow_send(way, r_to, core, ch):
        return pltpu.make_async_remote_copy(
            src_ref=n_send.at[way, half_at(core) * chunks + ch], dst_ref=n_recv.at[way, ch, col],
            send_sem=ici_sem.at[way], recv_sem=ir_sem.at[way, ch],
            device_id=(core, r_to), device_id_type=MESH)

    def aux_send(way, r_to, core):
        return pltpu.make_async_remote_copy(
            src_ref=a_send.at[way, half_at(core)], dst_ref=a_recv.at[way, col],
            send_sem=ici_sem.at[way], recv_sem=ar_sem.at[way],
            device_id=(core, r_to), device_id_type=MESH)

    def z_copy(t, ch, way, r_to):
        return pltpu.make_async_remote_copy(
            src_ref=z_send.at[way, t, ch], dst_ref=z_recv.at[way, t, ch],
            send_sem=ici_sem.at[way], recv_sem=zr_sem.at[t % 2, ch, way],
            device_id=(other, r_to), device_id_type=MESH)

    omega = om_ref[0]
    for way in range(2):
        for g in range(2 * chunks):
            u_band[way, g, :, 0:8] = jnp.zeros((band, 8, LANES), F32)
            u_band[way, g, :, 8 + sub:16 + sub] = jnp.zeros((band, 8, LANES), F32)
        for h in range(2):
            a_send[way, h] = jnp.zeros((16, LANES), F32)

    eye = lax.broadcasted_iota(jnp.int32, (sub, sub), 0) == lax.broadcasted_iota(jnp.int32, (sub, sub), 1)

    def spread(line):
        picked = jnp.where(eye, jnp.broadcast_to(line, (sub, sub)), 0.0)
        return jnp.broadcast_to(jnp.sum(picked, axis=1, keepdims=True), (sub, LANES))

    kap_load.wait()
    for k in range(sub):
        line = spread(k_raw[col, k:k + 1, :])
        ko[k, 8:8 + sub] = line
        ko[k, 7:8] = line[0:1]
        ko[k, 8 + sub:9 + sub] = line[sub - 1:sub]
    spot_col = lax.broadcasted_iota(jnp.int32, (sub, LANES), 0)
    cut_w = (spot_col == 0) & (col == 1)
    cut_e = (spot_col == sub - 1) & (col == 0)
    for way in range(2):
        first = 0 if way == 0 else sub - halo
        for k in range(halo):
            at = first + k
            mid = ko[at, 8:8 + sub]
            pw[way, k] = jnp.where(cut_w, 0.0, 0.5 * (mid + ko[at, 7:7 + sub]))
            pe[way, k] = jnp.where(cut_e, 0.0, 0.5 * (ko[at, 9:9 + sub] + mid))
            total = pw[way, k] + pe[way, k]
            if at > 0:
                pv[way, k] = 0.5 * (mid + ko[at - 1, 8:8 + sub])
                total = total + pv[way, k]
            if at < sub - 1:
                pv[way, k + 1] = 0.5 * (ko[at + 1, 8:8 + sub] + mid)
                total = total + pv[way, k + 1]
            pd[way, k] = total

    local_bytes(v_sc.at[0, 0:21], band_sem).wait()
    for way in range(2):
        for h in range(2):
            first = 0 if way == 0 else sub - band
            a_send[way, h, 12:12 + band, 0:sub] = k_raw[col, first:first + band]
    for g in range(2 * chunks):
        h, ch = g // chunks, g % chunks
        for way in range(2):
            shift = way
            for k in range(halo):
                line = shift + k
                at = k + 1 - way
                au = (pd[way, k] * u_band[way, g, line, 8:8 + sub]
                      - pw[way, k] * u_band[way, g, line, 7:7 + sub]
                      - pe[way, k] * u_band[way, g, line, 9:9 + sub])
                if line > 0:
                    au = au - pv[way, k] * u_band[way, g, line - 1, 8:8 + sub]
                if line < band - 1:
                    au = au - pv[way, k + 1] * u_band[way, g, line + 1, 8:8 + sub]
                part = i_send[way, g, at] - au
                i_send[way, g, at] = part
                edge = jnp.where(col == 0, u_band[way, g, line, 7 + sub:8 + sub], u_band[way, g, line, 8:9])
                slot = 5 * ch + k
                a_send[way, h, slot:slot + 1] = edge
                far = k - 1 + way
                if 0 <= far < 2:
                    n_send[way, g, far] = part.astype(BF16)
                    slot = 5 * ch + halo + far
                    a_send[way, h, slot:slot + 1] = jnp.where(col == 0, part[sub - 1:sub], part[0:1])
            i_send[way, g, halo * way] = u_band[way, g, halo * way, 8:8 + sub]

    pl.semaphore_wait(barrier, 1 + 2 * has_up.astype(jnp.int32) + 2 * has_dn.astype(jnp.int32))

    for way, present, r_to in ways:
        @pl.when(present)
        def _():
            def near(core, ch):
                init_send(way, r_to, core, ch, near_rows[way], ir_sem.at[way, ch]).start()
                narrow_send(way, r_to, core, ch).start()

            def far(core, ch, n):
                rows = pl.ds((2, 0)[way] + n, 1)
                init_send(way, r_to, core, ch, rows, far_sem.at[way]).start()

            first, second = way, 1 - way
            aux_send(way, r_to, first).start()
            for ch in range(chunks):
                near(first, ch)
            far(first, 0, 0)
            aux_send(way, r_to, second).start()
            for ch in range(chunks):
                near(second, ch)
            far(first, 0, 1)
            for ch in range(1, chunks):
                far(first, ch, 0)
                far(first, ch, 1)
            for ch in range(chunks):
                far(second, ch, 0)
                far(second, ch, 1)
    kap_pair(col).start()
    u_pair(0, my_cols).start()
    f_pair(0, my_cols).start()
    mat_pair(col).start()
    for ch in range(1, chunks):
        u_pair(ch, my_cols).start()
        f_pair(ch, my_cols).start()

    def clear(ch, carry):
        for i in list(range(band)) + list(range(band + sub, ext + 2)):
            v_sc[ch, i] = jnp.zeros(v_sc.shape[2:], F32)
        for i in range(band, band + sub):
            v_sc[ch, i, 0:8] = jnp.zeros((8, LANES), F32)
            v_sc[ch, i, 8 + wide:16 + wide] = jnp.zeros((8, LANES), F32)
        return carry
    lax.fori_loop(0, chunks, clear, 0)
    e_early[sub - 2:early_rows] = jnp.zeros((early_rows - sub + 2, wide, half), BF16)

    ext_cells = m_raw.shape[1]
    tile = 256
    lines_per_tile = tile // 32

    def permute(side):
        m_turn[:, 896:1024] = jnp.zeros((sub * sub, 128), BF16)
        m_turn[:, 0:ext_cells] = m_raw[side].T
        for n_tile in range(m_perm.shape[2] // tile):
            if n_tile == 0:
                spans = [(0, 128), (768, 1024)]
            else:
                first = band + lines_per_tile * (n_tile - 1)
                last = min(first + lines_per_tile, ext - band)
                spans = [(first * ext // 128 * 128, -(-last * ext // 128) * 128)]
            n_at = n_tile * tile + lax.broadcasted_iota(jnp.int32, (1, tile), 1)
            q = lax.shift_right_logical(n_at, 5)
            j = lax.bitwise_and(n_at, 31)
            line = jnp.where(q < band, q, jnp.where(q < 2 * band, q + (ext - 2 * band), q - band))
            ext_col = j + (halo - 8 * side)
            ok = (q < ext) & (ext_col >= 0) & (ext_col < ext)
            want = jnp.where(ok, line * ext + ext_col, -1)
            moved = None
            for lo, hi in spans:
                spot = lo + lax.broadcasted_iota(jnp.int32, (hi - lo, tile), 0)
                pick = jnp.where(spot == want, 1.0, 0.0).astype(BF16)
                part = jnp.dot(m_turn[:, lo:hi], pick, preferred_element_type=F32)
                moved = part if moved is None else moved + part
            m_perm[side, :, n_tile * tile:(n_tile + 1) * tile] = moved.astype(BF16)

    mat_load.wait()
    permute(col)

    kap_pair(other).wait_recv()

    def put_rows(take, at, count):
        for k in range(count):
            for side in range(2):
                line = spread(take(side, k))
                kb[at + k, left + side * sub:left + (side + 1) * sub] = line
                if side == 0:
                    kb[at + k, left - 1:left] = line[0:1]
                else:
                    kb[at + k, left + wide:left + wide + 1] = line[sub - 1:sub]

    def side_faces(e):
        k_mid = kb[e + 1, left:left + wide]
        fw[e] = 0.5 * (k_mid + kb[e + 1, left - 1:left + wide - 1])
        fe[e] = 0.5 * (kb[e + 1, left + 1:left + wide + 1] + k_mid)

    def diag_row(e):
        dg[e] = fv[e] + fv[e + 1] + fw[e] + fe[e]

    def face_row(i):
        fv[i] = 0.5 * (kb[i + 1, left:left + wide] + kb[i, left:left + wide])

    put_rows(lambda side, k: k_raw[side, k:k + 1, :], band, sub)
    fv[halo] = jnp.zeros((wide, LANES), F32)
    fv[halo + sub] = jnp.zeros((wide, LANES), F32)

    def own_face(i, carry):
        face_row(i)
        return carry
    lax.fori_loop(halo + 1, halo + sub, own_face, 0)

    def own_side(e, carry):
        side_faces(e)
        diag_row(e)
        return carry
    lax.fori_loop(halo, halo + sub, own_side, 0)

    def stencil(ch, e, n):
        rows = pl.ds(e, n)
        mid = pl.ds(e + 1, n)
        return (dg[rows] * v_sc[ch, mid, left:left + wide]
                - fv[rows] * v_sc[ch, pl.ds(e, n), left:left + wide]
                - fv[mid] * v_sc[ch, pl.ds(e + 2, n), left:left + wide]
                - fw[rows] * v_sc[ch, mid, left - 1:left + wide - 1]
                - fe[rows] * v_sc[ch, mid, left + 1:left + wide + 1])

    local_bytes(u_sc, load_sem).wait()

    def first_residual(ch):
        remote_bytes(u_fin, pair_send, pair_recv.at[ch]).wait_recv()

        def fill(i, c):
            rows = pl.ds(i * 6, 6)
            v_sc[ch, pl.ds(i * 6 + band, 6), left:left + wide] = u_sc[ch, rows]
            return c
        lax.fori_loop(0, sub // 6, fill, 0)

        def part(i, c):
            rows = pl.ds(halo + i * 6, 6)
            r_sc[ch, rows] = r_sc[ch, rows] - stencil(ch, halo + i * 6, 6)
            return c
        lax.fori_loop(0, sub // 6, part, 0)
        group = (sub - 2) // 2

        def to_e(i, c):
            e_early[pl.ds(i * group, group), :, in_lanes(ch)] = r_sc[ch, pl.ds(i * group + band, group)].astype(BF16)
            return c
        lax.fori_loop(0, 2, to_e, 0)

    first_residual(0)

    mat_pair(other).wait_recv()
    permute(other)

    for ch in range(1, chunks):
        first_residual(ch)

    def early_dot():
        for side in range(2):
            operand = e_early[:, 16 * side:16 * side + 32, :].reshape(early_rows * 32, half)
            acc[side] = jnp.dot(m_perm[side, :, late_k:late_k + early_rows * 32], operand,
                                preferred_element_type=F32)

    early_dot()

    for way, present, r_to in ways:
        @pl.when(present)
        def _():
            remote_bytes(a_recv.at[1 - way], ici_sem.at[way], ar_sem.at[1 - way]).wait_recv()
            put_rows(lambda side, k: a_recv[1 - way, side, 12 + k:13 + k, 0:sub], 0 if way == 0 else band + sub, band)

        @pl.when(jnp.logical_not(present))
        def _():
            for side in range(2):
                a_recv[1 - way, side] = jnp.zeros((16, LANES), F32)
            for i in range(band):
                if way == 0:
                    kb[i] = kb[band]
                else:
                    kb[band + sub + i] = kb[band + sub - 1]

    for i in range(halo + 1):
        face_row(i)
        face_row(halo + sub + i)
    for i in range(halo):
        side_faces(i)
        side_faces(halo + sub + i)
    for i in range(halo + 1):
        diag_row(i)
        diag_row(ext - 1 - i)

    def side_flux(sent, ch, k, e):
        slot = pl.ds(5 * ch + k, 1)
        return fe[e, sub - 1:sub] * (a_recv[sent, 1, slot] - a_recv[sent, 0, slot])

    def near_far(way):
        if way == 0:
            return (halo - 1, halo - 1), ((0, 0), (1, 1))
        return (halo + sub, 0), ((halo + sub + 1, 1), (halo + sub + 2, 2))

    wide_col = lax.broadcasted_iota(jnp.int32, (wide, LANES), 0)

    def late_first(ch):
        for way, present, r_to in ways:
            sent = 1 - way
            (e_near, k_near), far = near_far(way)
            near_at, u_at = (2, 3) if way == 0 else (1, 0)

            @pl.when(present)
            def _():
                remote_bytes(i_recv.at[sent, ch, 0:3], ici_sem.at[way], ir_sem.at[sent, ch]).wait_recv()
                r_sc[ch, e_near] = i_recv[sent, ch, near_at]
                flux = side_flux(sent, ch, k_near, e_near)
                r_sc[ch, e_near, sub - 1:sub] = r_sc[ch, e_near, sub - 1:sub] + flux
                r_sc[ch, e_near, sub:sub + 1] = r_sc[ch, e_near, sub:sub + 1] - flux
                for n in range(2):
                    e, k = far[n]
                    flux = side_flux(sent, ch, k, e)
                    slot = pl.ds(5 * ch + halo + n, 1)
                    got = jnp.concatenate([n_recv[sent, ch, side, n].astype(F32) for side in range(2)], axis=0)
                    got = jnp.where(wide_col == sub - 1, a_recv[sent, 0, slot] + flux, got)
                    got = jnp.where(wide_col == sub, a_recv[sent, 1, slot] - flux, got)
                    e_late[e if way == 0 else e - (ext - 2 * band), :, in_lanes(ch)] = got.astype(BF16)

            @pl.when(jnp.logical_not(present))
            def _():
                i_recv[sent, ch, u_at] = jnp.zeros((wide, LANES), F32)
                rows = pl.ds(0 if way == 0 else halo + sub, halo)
                r_sc[ch, rows] = jnp.zeros((halo, wide, LANES), F32)
                rows = pl.ds(0 if way == 0 else 2 * band - 2, 2)
                e_late[rows, :, in_lanes(ch)] = jnp.zeros((2, wide, LANES), BF16)

        flux = fv[halo] * (i_recv[1, ch, 3] - u_sc[ch, 0])
        near = r_sc[ch, halo - 1] - flux
        own = r_sc[ch, halo] + flux
        r_sc[ch, halo - 1] = near
        r_sc[ch, halo] = own
        e_late[halo - 1, :, in_lanes(ch)] = near.astype(BF16)
        e_late[halo, :, in_lanes(ch)] = own.astype(BF16)
        flux = fv[halo + sub] * (i_recv[0, ch, 0] - u_sc[ch, sub - 1])
        near = r_sc[ch, halo + sub] - flux
        own = r_sc[ch, halo + sub - 1] + flux
        r_sc[ch, halo + sub] = near
        r_sc[ch, halo + sub - 1] = own
        e_late[band, :, in_lanes(ch)] = own.astype(BF16)
        e_late[band + 1, :, in_lanes(ch)] = near.astype(BF16)

    def far_wait():
        for way, present, r_to in ways:
            @pl.when(present)
            def _():
                remote_bytes(i_recv.at[1 - way, :, 0:2], ici_sem.at[way], far_sem.at[1 - way]).wait_recv()

    def far_residual():
        for way, present, r_to in ways:
            sent = 1 - way
            _, far = near_far(way)

            @pl.when(present)
            def _():
                for ch in range(chunks):
                    for n in range(2):
                        e, k = far[n]
                        flux = side_flux(sent, ch, k, e)
                        r_sc[ch, e] = i_recv[sent, ch, n + 2 * way]
                        r_sc[ch, e, sub - 1:sub] = r_sc[ch, e, sub - 1:sub] + flux
                        r_sc[ch, e, sub:sub + 1] = r_sc[ch, e, sub:sub + 1] - flux

    def update(ch, e, n):
        r_new = r_sc[ch, pl.ds(e, n)] - omega * stencil(ch, e, n)
        r_sc[ch, pl.ds(e, n)] = r_new
        return r_new

    slow = lax.rem(row, 2)

    def towards(way):
        return jnp.where(way == 0, has_up, has_dn), jnp.where(way == 0, up_row, dn_row)

    def late_next(t, ch):
        for way in (1 - slow, slow):
            present, r_to = towards(way)

            @pl.when(present)
            def _():
                z_copy(t, ch, 1 - way, r_to).wait_recv()
                v_sc[ch, pl.ds(way * (band + sub), band), left:left + wide] = z_recv[1 - way, t, ch].astype(F32)

            e_late[pl.ds(way * band, band), :, in_lanes(ch)] = update(ch, way * (ext - band), band).astype(BF16)

    def solve(lanes, side, first, count):
        n = count * sub
        rows = pl.ds(first * sub if isinstance(first, int) else pl.multiple_of(first * sub, 32), n)
        cols = pl.ds(pl.multiple_of(16 * side, 16), 32)
        operand = e_late[:, cols, lanes]
        width = operand.shape[2]
        part = acc[side, rows, lanes] + jnp.dot(m_perm[side, rows, 0:late_k],
                                                     operand.reshape(late_k, width), preferred_element_type=F32)
        return part.reshape(count, sub, width)

    def solve_rows(lanes, first, count):
        return jnp.concatenate([solve(lanes, side, first, count) for side in range(2)], axis=1).astype(BF16)

    def keep_z(ch, first, count, z_bf):
        v_sc[ch, pl.ds(band + first, count), left:left + wide] = z_bf.astype(F32)

    def solve_and_send(t, ch):
        for way in (slow, 1 - slow):
            present, r_to = towards(way)
            first = way * (sub - band)
            z_bf = solve_rows(in_lanes(ch), first, band)
            z_send[way, t, ch] = z_bf

            @pl.when(present)
            def _():
                z_copy(t, ch, way, r_to).start()

            keep_z(ch, first, band, z_bf)

    def interior():
        z_mid = solve_rows(slice(0, half), band, sub - 2 * band)
        for ch in range(chunks):
            keep_z(ch, band, sub - 2 * band, z_mid[:, :, in_lanes(ch)])
        group = (sub - 2) // 2
        for ch in range(chunks):
            def inner(i, c):
                e_early[pl.ds(i * group, group), :, in_lanes(ch)] = update(ch, band + i * group, group).astype(BF16)
                return c
            lax.fori_loop(0, 2, inner, 0)

            def add(i, c):
                rows = pl.ds(i * 6, 6)
                u_sc[ch, rows] = u_sc[ch, rows] + omega * v_sc[ch, pl.ds(i * 6 + band, 6), left:left + wide]
                return c
            lax.fori_loop(0, sub // 6, add, 0)
        early_dot()

    for ch in range(chunks):
        late_first(ch)
        solve_and_send(0, ch)
    interior()

    def sweep_next(t, carry):
        @pl.when(t == 0)
        def _():
            far_wait()
            far_residual()
        for ch in range(chunks):
            late_next(t, ch)
            solve_and_send(t + 1, ch)
        interior()
        return carry
    lax.fori_loop(0, SWEEPS - 2, sweep_next, 0)

    cuts = (0, 16, sub)

    def out_pair(ch, n, which):
        rows = pl.ds(cuts[n], cuts[n + 1] - cuts[n])
        return pltpu.make_async_remote_copy(
            src_ref=u_fin.at[ch, rows], dst_ref=out_ref.at[rows, :, lanes_of(which, ch)],
            send_sem=pair_send, recv_sem=out_recv,
            device_id=(other, row), device_id_type=MESH)

    for ch in range(chunks):
        late_next(SWEEPS - 2, ch)
        for n in range(2):
            first, past = cuts[n], cuts[n + 1]
            z = solve(in_lanes(ch), other, first, past - first).astype(BF16).astype(F32)
            u_fin[ch, first:past] = u_sc[ch, first:past, other_cols] + omega * z
            out_pair(ch, n, mine).start()
    z_own = solve(slice(0, half), col, 0, sub).astype(BF16).astype(F32)
    for ch in range(chunks):
        out_ref[:, :, lanes_of(mine, ch)] = u_sc[ch, :, my_cols] + omega * z_own[:, :, in_lanes(ch)]

    kap_pair(col).wait_send()
    mat_pair(col).wait_send()
    for way, present, r_to in ways:
        @pl.when(present)
        def _():
            remote_bytes(v_sc.at[0, 0:23], ici_sem.at[way], ar_sem.at[way]).wait_send()
    remote_bytes(u_fin, pair_send, out_recv).wait_recv()
    remote_bytes(v_sc.at[:, 0:27], pair_send, out_recv).wait_send()


def solution(mesh):
    row_count = mesh.shape['row']
    grid_spec = P('row', 'col', None)

    def device_fn(f_blk, u_blk, kappa_blk, mat_blk, omega_relax):
        sub, _, rhs = u_blk.shape
        ext_cells = mat_blk.shape[3]
        ext = math.isqrt(ext_cells)
        halo = (ext - sub) // 2
        band = halo + 1
        chunks = rhs // (2 * LANES)
        wide = 2 * sub
        early_rows = 24
        hbm = pl.BlockSpec(memory_space=pl.ANY)
        vmem = pltpu.VMEM
        dma = pltpu.SemaphoreType.DMA
        return pl.pallas_call(
            functools.partial(kernel, row_count, sub, halo, chunks),
            out_shape=pltpu.VMEM(u_blk.shape, F32),
            in_specs=[pl.BlockSpec(memory_space=pltpu.SMEM), hbm, hbm, hbm, hbm],
            out_specs=pl.BlockSpec(memory_space=pltpu.VMEM),
            scratch_shapes=[
                vmem((chunks, sub, wide, LANES), F32),
                vmem((chunks, ext, wide, LANES), F32),
                vmem((chunks, ext + 2, 64, LANES), F32),
                vmem((2 * band, wide, chunks * LANES), BF16),
                vmem((early_rows, wide, chunks * LANES), BF16),
                vmem((2, sub * sub, chunks * LANES), F32),
                vmem((2, ext_cells, sub * sub), BF16),
                vmem((sub * sub, 1024), BF16),
                vmem((2, sub * sub, 1024), BF16),
                vmem((2, sub, sub), F32),
                vmem((ext + 2, 64, LANES), F32),
                vmem((sub, 40, LANES), F32),
                vmem((ext + 1, wide, LANES), F32),
                vmem((ext, wide, LANES), F32),
                vmem((ext, wide, LANES), F32),
                vmem((ext, wide, LANES), F32),
                vmem((2, 2 * chunks, band, 40, LANES), F32),
                vmem((2, halo + 1, sub, LANES), F32),
                vmem((2, halo, sub, LANES), F32),
                vmem((2, halo, sub, LANES), F32),
                vmem((2, halo, sub, LANES), F32),
                vmem((2, 2 * chunks, band, sub, LANES), F32),
                vmem((2, chunks, band, wide, LANES), F32),
                vmem((2, 2 * chunks, 2, sub, LANES), BF16),
                vmem((2, chunks, 2, 2, sub, LANES), BF16),
                vmem((2, 2, 16, LANES), F32),
                vmem((2, 2, 16, LANES), F32),
                vmem((2, SWEEPS - 1, chunks, band, wide, LANES), BF16),
                vmem((2, SWEEPS - 1, chunks, band, wide, LANES), BF16),
                vmem((chunks, sub, sub, LANES), F32),
                dma, dma, dma, dma((chunks,)), dma, dma, dma, dma, dma, dma,
                dma((2,)), dma((2, chunks)), dma((2,)), dma((2,)), dma((2, chunks, 2)), dma,
            ],
            compiler_params=pltpu.CompilerParams(collective_id=0, has_side_effects=True,
                                                 vmem_limit_bytes=61000 * 1024),
        )(omega_relax.reshape(1), f_blk, u_blk, kappa_blk, mat_blk[0, 0].T)

    return jax.shard_map(device_fn, mesh=mesh,
                         in_specs=(grid_spec, grid_spec, P('row', 'col'), P('row', 'col', None, None), P()),
                         out_specs=grid_spec, check_vma=False)
```

```python
import functools
import math

import jax
import jax.numpy as jnp
from jax import lax
from jax.experimental import pallas as pl
from jax.experimental.pallas import tpu as pltpu
from jax.sharding import PartitionSpec as P

SWEEPS = 6
LANES = 128
MESH = pl.DeviceIdType.MESH
F32 = jnp.float32
BF16 = jnp.bfloat16


def kernel(row_count, sub, halo, chunks,
           om_ref, f_hbm, u_hbm, kap_hbm, mat_hbm, out_ref,
           u_sc, r_sc, v_sc, e_late, e_early, acc, m_raw, m_turn, m_perm,
           k_raw, kb, ko, fv, fw, fe, dg, u_band, pv, pw, pe, pd, i_send, i_recv, n_send, n_recv, a_send, a_recv,
           z_send, z_recv, u_fin,
           load_sem, band_sem, pair_send, pair_recv, mat_sem, mat_send, mat_recv, kap_loc, kap_send, kap_recv,
           ici_sem, ir_sem, far_sem, ar_sem, zr_sem, out_recv):
    wide = 2 * sub
    ext = sub + 2 * halo
    band = halo + 1
    late_k = 2 * band * 32
    early_rows = e_early.shape[0]
    half = chunks * LANES
    left = 8

    row = lax.axis_index('row')
    col = lax.axis_index('col')
    other = 1 - col
    mine = lax.rem(row + col, 2)
    theirs = 1 - mine
    has_up = row > 0
    has_dn = row < row_count - 1
    ways = ((0, has_up, jnp.maximum(row - 1, 0)), (1, has_dn, jnp.minimum(row + 1, row_count - 1)))
    up_row, dn_row = ways[0][2], ways[1][2]
    col_spans = [pl.ds(side * sub, sub) for side in range(2)]
    my_cols = pl.ds(pl.multiple_of(col * sub, 8), sub)
    other_cols = pl.ds(pl.multiple_of(other * sub, 8), sub)
    own_rows = pl.ds(halo, sub)

    def lanes_of(which, ch):
        return pl.ds(pl.multiple_of(which * half + ch * LANES, LANES), LANES)

    def local_bytes(ref, sem):
        return pltpu.make_async_copy(ref, ref, sem)

    def remote_bytes(ref, send_sem, recv_sem):
        return pltpu.make_async_remote_copy(src_ref=ref, dst_ref=ref, send_sem=send_sem, recv_sem=recv_sem,
                                            device_id=(other, row), device_id_type=MESH)

    barrier = pltpu.get_barrier_semaphore()

    def in_lanes(ch):
        return slice(ch * LANES, (ch + 1) * LANES)

    def greet(r_to, c_to):
        pl.semaphore_signal(barrier, inc=1, device_id=(c_to, r_to), device_id_type=MESH)

    for _, present, r_to in ways:
        @pl.when(present)
        def _():
            greet(r_to, col)
            greet(r_to, other)
    greet(row, other)

    kap_load = pltpu.make_async_copy(kap_hbm, k_raw.at[col], kap_loc)
    kap_load.start()

    def band_loads(way, g):
        lanes = pl.ds(g * LANES, LANES)
        u_from = pl.ds(0 if way == 0 else sub - band, band)
        f_from = pl.ds(0 if way == 0 else sub - halo, halo)
        return (pltpu.make_async_copy(u_hbm.at[u_from, :, lanes], u_band.at[way, g, :, 8:8 + sub, :],
                                      band_sem),
                pltpu.make_async_copy(f_hbm.at[f_from, :, lanes], i_send.at[way, g, pl.ds(1 - way, halo)],
                                      band_sem))

    for g in range(2 * chunks):
        for way in range(2):
            for load in band_loads(way, g):
                load.start()

    def u_load(ch):
        return pltpu.make_async_copy(u_hbm.at[:, :, lanes_of(mine, ch)], u_sc.at[ch, :, my_cols, :], load_sem)

    def f_load(ch):
        return pltpu.make_async_copy(f_hbm.at[:, :, lanes_of(mine, ch)], r_sc.at[ch, own_rows, my_cols, :],
                                     load_sem)

    mat_load = pltpu.make_async_copy(mat_hbm, m_raw.at[col], mat_sem)
    mat_load.start()
    for ch in range(chunks):
        u_load(ch).start()
        f_load(ch).start()

    def u_pair(ch, cols):
        return pltpu.make_async_remote_copy(
            src_ref=u_hbm.at[:, :, lanes_of(theirs, ch)], dst_ref=u_sc.at[ch, :, cols, :],
            send_sem=pair_send, recv_sem=pair_recv.at[ch],
            device_id=(other, row), device_id_type=MESH)

    def f_pair(ch, cols):
        return pltpu.make_async_remote_copy(
            src_ref=f_hbm.at[:, :, lanes_of(theirs, ch)], dst_ref=r_sc.at[ch, own_rows, cols, :],
            send_sem=pair_send, recv_sem=pair_recv.at[ch],
            device_id=(other, row), device_id_type=MESH)

    def mat_pair(slot):
        return pltpu.make_async_remote_copy(
            src_ref=mat_hbm, dst_ref=m_raw.at[slot],
            send_sem=mat_send, recv_sem=mat_recv,
            device_id=(other, row), device_id_type=MESH)

    def kap_pair(slot):
        return pltpu.make_async_remote_copy(
            src_ref=k_raw.at[col], dst_ref=k_raw.at[slot],
            send_sem=kap_send, recv_sem=kap_recv,
            device_id=(other, row), device_id_type=MESH)

    def half_at(core):
        return lax.rem(core + row + 1, 2)

    near_rows = (pl.ds(0, 2), pl.ds(2, 2))
    far_rows = (pl.ds(2, 2), pl.ds(0, 2))

    def init_send(way, r_to, core, ch, rows, recv_sem):
        g = half_at(core) * chunks + ch
        return pltpu.make_async_remote_copy(
            src_ref=i_send.at[way, g, rows], dst_ref=i_recv.at[way, ch, rows, my_cols, :],
            send_sem=ici_sem.at[way], recv_sem=recv_sem,
            device_id=(core, r_to), device_id_type=MESH)

    def narrow_send(way, r_to, core, ch):
        return pltpu.make_async_remote_copy(
            src_ref=n_send.at[way, half_at(core) * chunks + ch], dst_ref=n_recv.at[way, ch, col],
            send_sem=ici_sem.at[way], recv_sem=ir_sem.at[way, ch],
            device_id=(core, r_to), device_id_type=MESH)

    def aux_send(way, r_to, core):
        return pltpu.make_async_remote_copy(
            src_ref=a_send.at[way, half_at(core)], dst_ref=a_recv.at[way, col],
            send_sem=ici_sem.at[way], recv_sem=ar_sem.at[way],
            device_id=(core, r_to), device_id_type=MESH)

    def z_copy(t, ch, way, r_to):
        return pltpu.make_async_remote_copy(
            src_ref=z_send.at[way, t, ch], dst_ref=z_recv.at[way, t, ch],
            send_sem=ici_sem.at[way], recv_sem=zr_sem.at[t % 2, ch, way],
            device_id=(other, r_to), device_id_type=MESH)

    omega = om_ref[0]
    for way in range(2):
        for g in range(2 * chunks):
            u_band[way, g, :, 0:8] = jnp.zeros((band, 8, LANES), F32)
            u_band[way, g, :, 8 + sub:16 + sub] = jnp.zeros((band, 8, LANES), F32)
        for h in range(2):
            a_send[way, h] = jnp.zeros((16, LANES), F32)

    eye = lax.broadcasted_iota(jnp.int32, (sub, sub), 0) == lax.broadcasted_iota(jnp.int32, (sub, sub), 1)

    def spread(line):
        picked = jnp.where(eye, jnp.broadcast_to(line, (sub, sub)), 0.0)
        return jnp.broadcast_to(jnp.sum(picked, axis=1, keepdims=True), (sub, LANES))

    kap_load.wait()
    for k in range(sub):
        line = spread(k_raw[col, k:k + 1, :])
        ko[k, 8:8 + sub] = line
        ko[k, 7:8] = line[0:1]
        ko[k, 8 + sub:9 + sub] = line[sub - 1:sub]
    spot_col = lax.broadcasted_iota(jnp.int32, (sub, LANES), 0)
    cut_w = (spot_col == 0) & (col == 1)
    cut_e = (spot_col == sub - 1) & (col == 0)
    for way in range(2):
        first = 0 if way == 0 else sub - halo
        for k in range(halo):
            at = first + k
            mid = ko[at, 8:8 + sub]
            pw[way, k] = jnp.where(cut_w, 0.0, 0.5 * (mid + ko[at, 7:7 + sub]))
            pe[way, k] = jnp.where(cut_e, 0.0, 0.5 * (ko[at, 9:9 + sub] + mid))
            total = pw[way, k] + pe[way, k]
            if at > 0:
                pv[way, k] = 0.5 * (mid + ko[at - 1, 8:8 + sub])
                total = total + pv[way, k]
            if at < sub - 1:
                pv[way, k + 1] = 0.5 * (ko[at + 1, 8:8 + sub] + mid)
                total = total + pv[way, k + 1]
            pd[way, k] = total

    local_bytes(v_sc.at[0, 0:21], band_sem).wait()
    for way in range(2):
        for h in range(2):
            first = 0 if way == 0 else sub - band
            a_send[way, h, 12:12 + band, 0:sub] = k_raw[col, first:first + band]
    for g in range(2 * chunks):
        h, ch = g // chunks, g % chunks
        for way in range(2):
            shift = way
            for k in range(halo):
                line = shift + k
                at = k + 1 - way
                au = (pd[way, k] * u_band[way, g, line, 8:8 + sub]
                      - pw[way, k] * u_band[way, g, line, 7:7 + sub]
                      - pe[way, k] * u_band[way, g, line, 9:9 + sub])
                if line > 0:
                    au = au - pv[way, k] * u_band[way, g, line - 1, 8:8 + sub]
                if line < band - 1:
                    au = au - pv[way, k + 1] * u_band[way, g, line + 1, 8:8 + sub]
                part = i_send[way, g, at] - au
                i_send[way, g, at] = part
                edge = jnp.where(col == 0, u_band[way, g, line, 7 + sub:8 + sub], u_band[way, g, line, 8:9])
                slot = 5 * ch + k
                a_send[way, h, slot:slot + 1] = edge
                far = k - 1 + way
                if 0 <= far < 2:
                    n_send[way, g, far] = part.astype(BF16)
                    slot = 5 * ch + halo + far
                    a_send[way, h, slot:slot + 1] = jnp.where(col == 0, part[sub - 1:sub], part[0:1])
            i_send[way, g, halo * way] = u_band[way, g, halo * way, 8:8 + sub]

    pl.semaphore_wait(barrier, 1 + 2 * has_up.astype(jnp.int32) + 2 * has_dn.astype(jnp.int32))

    for way, present, r_to in ways:
        @pl.when(present)
        def _():
            def near(core, ch):
                init_send(way, r_to, core, ch, near_rows[way], ir_sem.at[way, ch]).start()
                narrow_send(way, r_to, core, ch).start()

            def far(core, ch, n):
                rows = pl.ds((2, 0)[way] + n, 1)
                init_send(way, r_to, core, ch, rows, far_sem.at[way]).start()

            first, second = way, 1 - way
            aux_send(way, r_to, first).start()
            for ch in range(chunks):
                near(first, ch)
            far(first, 0, 0)
            aux_send(way, r_to, second).start()
            for ch in range(chunks):
                near(second, ch)
            far(first, 0, 1)
            for ch in range(1, chunks):
                far(first, ch, 0)
                far(first, ch, 1)
            for ch in range(chunks):
                far(second, ch, 0)
                far(second, ch, 1)
    kap_pair(col).start()
    u_pair(0, my_cols).start()
    f_pair(0, my_cols).start()
    mat_pair(col).start()
    for ch in range(1, chunks):
        u_pair(ch, my_cols).start()
        f_pair(ch, my_cols).start()

    def clear(ch, carry):
        for i in list(range(band)) + list(range(band + sub, ext + 2)):
            v_sc[ch, i] = jnp.zeros(v_sc.shape[2:], F32)
        for i in range(band, band + sub):
            v_sc[ch, i, 0:8] = jnp.zeros((8, LANES), F32)
            v_sc[ch, i, 8 + wide:16 + wide] = jnp.zeros((8, LANES), F32)
        return carry
    lax.fori_loop(0, chunks, clear, 0)
    e_early[sub - 2:early_rows] = jnp.zeros((early_rows - sub + 2, wide, half), BF16)

    ext_cells = m_raw.shape[1]
    tile = 256
    lines_per_tile = tile // 32

    def permute(side):
        m_turn[:, 896:1024] = jnp.zeros((sub * sub, 128), BF16)
        m_turn[:, 0:ext_cells] = m_raw[side].T
        for n_tile in range(m_perm.shape[2] // tile):
            if n_tile == 0:
                spans = [(0, 128), (768, 1024)]
            else:
                first = band + lines_per_tile * (n_tile - 1)
                last = min(first + lines_per_tile, ext - band)
                spans = [(first * ext // 128 * 128, -(-last * ext // 128) * 128)]
            n_at = n_tile * tile + lax.broadcasted_iota(jnp.int32, (1, tile), 1)
            q = lax.shift_right_logical(n_at, 5)
            j = lax.bitwise_and(n_at, 31)
            line = jnp.where(q < band, q, jnp.where(q < 2 * band, q + (ext - 2 * band), q - band))
            ext_col = j + (halo - 8 * side)
            ok = (q < ext) & (ext_col >= 0) & (ext_col < ext)
            want = jnp.where(ok, line * ext + ext_col, -1)
            moved = None
            for lo, hi in spans:
                spot = lo + lax.broadcasted_iota(jnp.int32, (hi - lo, tile), 0)
                pick = jnp.where(spot == want, 1.0, 0.0).astype(BF16)
                part = jnp.dot(m_turn[:, lo:hi], pick, preferred_element_type=F32)
                moved = part if moved is None else moved + part
            m_perm[side, :, n_tile * tile:(n_tile + 1) * tile] = moved.astype(BF16)

    mat_load.wait()
    permute(col)

    kap_pair(other).wait_recv()

    def put_rows(take, at, count):
        for k in range(count):
            for side in range(2):
                line = spread(take(side, k))
                kb[at + k, left + side * sub:left + (side + 1) * sub] = line
                if side == 0:
                    kb[at + k, left - 1:left] = line[0:1]
                else:
                    kb[at + k, left + wide:left + wide + 1] = line[sub - 1:sub]

    def side_faces(e):
        k_mid = kb[e + 1, left:left + wide]
        fw[e] = 0.5 * (k_mid + kb[e + 1, left - 1:left + wide - 1])
        fe[e] = 0.5 * (kb[e + 1, left + 1:left + wide + 1] + k_mid)

    def diag_row(e):
        dg[e] = fv[e] + fv[e + 1] + fw[e] + fe[e]

    def face_row(i):
        fv[i] = 0.5 * (kb[i + 1, left:left + wide] + kb[i, left:left + wide])

    put_rows(lambda side, k: k_raw[side, k:k + 1, :], band, sub)
    fv[halo] = jnp.zeros((wide, LANES), F32)
    fv[halo + sub] = jnp.zeros((wide, LANES), F32)

    def own_face(i, carry):
        face_row(i)
        return carry
    lax.fori_loop(halo + 1, halo + sub, own_face, 0)

    def own_side(e, carry):
        side_faces(e)
        diag_row(e)
        return carry
    lax.fori_loop(halo, halo + sub, own_side, 0)

    def stencil(ch, e, n):
        rows = pl.ds(e, n)
        mid = pl.ds(e + 1, n)
        return (dg[rows] * v_sc[ch, mid, left:left + wide]
                - fv[rows] * v_sc[ch, pl.ds(e, n), left:left + wide]
                - fv[mid] * v_sc[ch, pl.ds(e + 2, n), left:left + wide]
                - fw[rows] * v_sc[ch, mid, left - 1:left + wide - 1]
                - fe[rows] * v_sc[ch, mid, left + 1:left + wide + 1])

    local_bytes(u_sc, load_sem).wait()

    def first_residual(ch):
        remote_bytes(u_fin, pair_send, pair_recv.at[ch]).wait_recv()

        def fill(i, c):
            rows = pl.ds(i * 6, 6)
            v_sc[ch, pl.ds(i * 6 + band, 6), left:left + wide] = u_sc[ch, rows]
            return c
        lax.fori_loop(0, sub // 6, fill, 0)

        def part(i, c):
            rows = pl.ds(halo + i * 6, 6)
            r_sc[ch, rows] = r_sc[ch, rows] - stencil(ch, halo + i * 6, 6)
            return c
        lax.fori_loop(0, sub // 6, part, 0)
        group = (sub - 2) // 2

        def to_e(i, c):
            e_early[pl.ds(i * group, group), :, in_lanes(ch)] = r_sc[ch, pl.ds(i * group + band, group)].astype(BF16)
            return c
        lax.fori_loop(0, 2, to_e, 0)

    first_residual(0)

    mat_pair(other).wait_recv()
    permute(other)

    for ch in range(1, chunks):
        first_residual(ch)

    def early_dot():
        for side in range(2):
            operand = e_early[:, 16 * side:16 * side + 32, :].reshape(early_rows * 32, half)
            acc[side] = jnp.dot(m_perm[side, :, late_k:late_k + early_rows * 32], operand,
                                preferred_element_type=F32)

    early_dot()

    for way, present, r_to in ways:
        @pl.when(present)
        def _():
            remote_bytes(a_recv.at[1 - way], ici_sem.at[way], ar_sem.at[1 - way]).wait_recv()
            put_rows(lambda side, k: a_recv[1 - way, side, 12 + k:13 + k, 0:sub], 0 if way == 0 else band + sub, band)

        @pl.when(jnp.logical_not(present))
        def _():
            for side in range(2):
                a_recv[1 - way, side] = jnp.zeros((16, LANES), F32)
            for i in range(band):
                if way == 0:
                    kb[i] = kb[band]
                else:
                    kb[band + sub + i] = kb[band + sub - 1]

    for i in range(halo + 1):
        face_row(i)
        face_row(halo + sub + i)
    for i in range(halo):
        side_faces(i)
        side_faces(halo + sub + i)
    for i in range(halo + 1):
        diag_row(i)
        diag_row(ext - 1 - i)

    def side_flux(sent, ch, k, e):
        slot = pl.ds(5 * ch + k, 1)
        return fe[e, sub - 1:sub] * (a_recv[sent, 1, slot] - a_recv[sent, 0, slot])

    def near_far(way):
        if way == 0:
            return (halo - 1, halo - 1), ((0, 0), (1, 1))
        return (halo + sub, 0), ((halo + sub + 1, 1), (halo + sub + 2, 2))

    wide_col = lax.broadcasted_iota(jnp.int32, (wide, LANES), 0)

    def late_first(ch):
        for way, present, r_to in ways:
            sent = 1 - way
            (e_near, k_near), far = near_far(way)
            near_at, u_at = (2, 3) if way == 0 else (1, 0)

            @pl.when(present)
            def _():
                remote_bytes(i_recv.at[sent, ch, 0:3], ici_sem.at[way], ir_sem.at[sent, ch]).wait_recv()
                r_sc[ch, e_near] = i_recv[sent, ch, near_at]
                flux = side_flux(sent, ch, k_near, e_near)
                r_sc[ch, e_near, sub - 1:sub] = r_sc[ch, e_near, sub - 1:sub] + flux
                r_sc[ch, e_near, sub:sub + 1] = r_sc[ch, e_near, sub:sub + 1] - flux
                for n in range(2):
                    e, k = far[n]
                    flux = side_flux(sent, ch, k, e)
                    slot = pl.ds(5 * ch + halo + n, 1)
                    got = jnp.concatenate([n_recv[sent, ch, side, n].astype(F32) for side in range(2)], axis=0)
                    got = jnp.where(wide_col == sub - 1, a_recv[sent, 0, slot] + flux, got)
                    got = jnp.where(wide_col == sub, a_recv[sent, 1, slot] - flux, got)
                    e_late[e if way == 0 else e - (ext - 2 * band), :, in_lanes(ch)] = got.astype(BF16)

            @pl.when(jnp.logical_not(present))
            def _():
                i_recv[sent, ch, u_at] = jnp.zeros((wide, LANES), F32)
                rows = pl.ds(0 if way == 0 else halo + sub, halo)
                r_sc[ch, rows] = jnp.zeros((halo, wide, LANES), F32)
                rows = pl.ds(0 if way == 0 else 2 * band - 2, 2)
                e_late[rows, :, in_lanes(ch)] = jnp.zeros((2, wide, LANES), BF16)

            face, e_own, own_line = (halo, halo, 0) if way == 0 else (halo + sub, halo + sub - 1, sub - 1)
            flux = fv[face] * (i_recv[sent, ch, u_at] - u_sc[ch, own_line])
            near = r_sc[ch, e_near] - flux
            own = r_sc[ch, e_own] + flux
            r_sc[ch, e_near] = near
            r_sc[ch, e_own] = own
            e_late[halo - 1 if way == 0 else band + 1, :, in_lanes(ch)] = near.astype(BF16)
            e_late[halo if way == 0 else band, :, in_lanes(ch)] = own.astype(BF16)

    def far_wait():
        for way, present, r_to in ways:
            @pl.when(present)
            def _():
                remote_bytes(i_recv.at[1 - way, :, 0:2], ici_sem.at[way], far_sem.at[1 - way]).wait_recv()

    def far_residual():
        for way, present, r_to in ways:
            sent = 1 - way
            _, far = near_far(way)

            @pl.when(present)
            def _():
                for ch in range(chunks):
                    for n in range(2):
                        e, k = far[n]
                        flux = side_flux(sent, ch, k, e)
                        r_sc[ch, e] = i_recv[sent, ch, n + 2 * way]
                        r_sc[ch, e, sub - 1:sub] = r_sc[ch, e, sub - 1:sub] + flux
                        r_sc[ch, e, sub:sub + 1] = r_sc[ch, e, sub:sub + 1] - flux

    def update(ch, e, n):
        r_new = r_sc[ch, pl.ds(e, n)] - omega * stencil(ch, e, n)
        r_sc[ch, pl.ds(e, n)] = r_new
        return r_new

    slow = lax.rem(row, 2)

    def towards(way):
        return jnp.where(way == 0, has_up, has_dn), jnp.where(way == 0, up_row, dn_row)

    def late_next(t, ch, ahead):
        for n, way in enumerate((1 - slow, slow)):
            present, r_to = towards(way)

            @pl.when(present)
            def _():
                z_copy(t, ch, 1 - way, r_to).wait_recv()
                v_sc[ch, pl.ds(way * (band + sub), band), left:left + wide] = z_recv[1 - way, t, ch].astype(F32)

            e_late[pl.ds(way * band, band), :, in_lanes(ch)] = update(ch, way * (ext - band), band).astype(BF16)
            if n == 0 and ahead:
                first = slow * (sub - band)
                rows = pl.ds(pl.multiple_of(first * sub, 32), band * sub)
                for side in range(2):
                    acc[side, rows, in_lanes(ch)] = solve(in_lanes(ch), side, first, band, way).reshape(band * sub, LANES)

    def solve(lanes, side, first, count, only=None):
        n = count * sub
        rows = pl.ds(first * sub if isinstance(first, int) else pl.multiple_of(first * sub, 32), n)
        cols = pl.ds(pl.multiple_of(16 * side, 16), 32)
        lines = slice(None) if only is None else pl.ds(only * band, band)
        depth = late_k if only is None else late_k // 2
        at = 0 if only is None else pl.multiple_of(only * depth, depth)
        operand = e_late[lines, cols, lanes]
        width = operand.shape[2]
        part = acc[side, rows, lanes] + jnp.dot(m_perm[side, rows, pl.ds(at, depth)],
                                                     operand.reshape(depth, width), preferred_element_type=F32)
        return part.reshape(count, sub, width)

    def solve_rows(lanes, first, count, only=None):
        return jnp.concatenate([solve(lanes, side, first, count, only) for side in range(2)], axis=1).astype(BF16)

    def keep_z(ch, first, count, z_bf):
        v_sc[ch, pl.ds(band + first, count), left:left + wide] = z_bf.astype(F32)

    def solve_and_send(t, ch, left_way):
        for n, way in enumerate((slow, 1 - slow)):
            present, r_to = towards(way)
            first = way * (sub - band)
            z_bf = solve_rows(in_lanes(ch), first, band, left_way if n == 0 else None)
            z_send[way, t, ch] = z_bf

            @pl.when(present)
            def _():
                z_copy(t, ch, way, r_to).start()

            keep_z(ch, first, band, z_bf)

    def interior():
        z_mid = solve_rows(slice(0, half), band, sub - 2 * band)
        for ch in range(chunks):
            keep_z(ch, band, sub - 2 * band, z_mid[:, :, in_lanes(ch)])
        group = (sub - 2) // 2
        for ch in range(chunks):
            def inner(i, c):
                e_early[pl.ds(i * group, group), :, in_lanes(ch)] = update(ch, band + i * group, group).astype(BF16)
                return c
            lax.fori_loop(0, 2, inner, 0)

            def add(i, c):
                rows = pl.ds(i * 6, 6)
                u_sc[ch, rows] = u_sc[ch, rows] + omega * v_sc[ch, pl.ds(i * 6 + band, 6), left:left + wide]
                return c
            lax.fori_loop(0, sub // 6, add, 0)
        early_dot()

    for ch in range(chunks):
        late_first(ch)
        solve_and_send(0, ch, None)
    interior()

    def sweep_next(t, carry):
        @pl.when(t == 0)
        def _():
            far_wait()
            far_residual()
        for ch in range(chunks):
            late_next(t, ch, True)
            solve_and_send(t + 1, ch, slow)
        interior()
        return carry
    lax.fori_loop(0, SWEEPS - 2, sweep_next, 0)

    cuts = (0, 16, sub)

    def out_pair(ch, n, which):
        rows = pl.ds(cuts[n], cuts[n + 1] - cuts[n])
        return pltpu.make_async_remote_copy(
            src_ref=u_fin.at[ch, rows], dst_ref=out_ref.at[rows, :, lanes_of(which, ch)],
            send_sem=pair_send, recv_sem=out_recv,
            device_id=(other, row), device_id_type=MESH)

    for ch in range(chunks):
        late_next(SWEEPS - 2, ch, False)
        for n in range(2):
            first, past = cuts[n], cuts[n + 1]
            z = solve(in_lanes(ch), other, first, past - first).astype(BF16).astype(F32)
            u_fin[ch, first:past] = u_sc[ch, first:past, other_cols] + omega * z
            out_pair(ch, n, mine).start()
    z_own = solve(slice(0, half), col, 0, sub).astype(BF16).astype(F32)
    for ch in range(chunks):
        out_ref[:, :, lanes_of(mine, ch)] = u_sc[ch, :, my_cols] + omega * z_own[:, :, in_lanes(ch)]

    kap_pair(col).wait_send()
    mat_pair(col).wait_send()
    for way, present, r_to in ways:
        @pl.when(present)
        def _():
            remote_bytes(v_sc.at[0, 0:23], ici_sem.at[way], ar_sem.at[way]).wait_send()
    remote_bytes(u_fin, pair_send, out_recv).wait_recv()
    remote_bytes(v_sc.at[:, 0:27], pair_send, out_recv).wait_send()


def solution(mesh):
    row_count = mesh.shape['row']
    grid_spec = P('row', 'col', None)

    def device_fn(f_blk, u_blk, kappa_blk, mat_blk, omega_relax):
        sub, _, rhs = u_blk.shape
        ext_cells = mat_blk.shape[3]
        ext = math.isqrt(ext_cells)
        halo = (ext - sub) // 2
        band = halo + 1
        chunks = rhs // (2 * LANES)
        wide = 2 * sub
        early_rows = 24
        hbm = pl.BlockSpec(memory_space=pl.ANY)
        vmem = pltpu.VMEM
        dma = pltpu.SemaphoreType.DMA
        return pl.pallas_call(
            functools.partial(kernel, row_count, sub, halo, chunks),
            out_shape=pltpu.VMEM(u_blk.shape, F32),
            in_specs=[pl.BlockSpec(memory_space=pltpu.SMEM), hbm, hbm, hbm, hbm],
            out_specs=pl.BlockSpec(memory_space=pltpu.VMEM),
            scratch_shapes=[
                vmem((chunks, sub, wide, LANES), F32),
                vmem((chunks, ext, wide, LANES), F32),
                vmem((chunks, ext + 2, 64, LANES), F32),
                vmem((2 * band, wide, chunks * LANES), BF16),
                vmem((early_rows, wide, chunks * LANES), BF16),
                vmem((2, sub * sub, chunks * LANES), F32),
                vmem((2, ext_cells, sub * sub), BF16),
                vmem((sub * sub, 1024), BF16),
                vmem((2, sub * sub, 1024), BF16),
                vmem((2, sub, sub), F32),
                vmem((ext + 2, 64, LANES), F32),
                vmem((sub, 40, LANES), F32),
                vmem((ext + 1, wide, LANES), F32),
                vmem((ext, wide, LANES), F32),
                vmem((ext, wide, LANES), F32),
                vmem((ext, wide, LANES), F32),
                vmem((2, 2 * chunks, band, 40, LANES), F32),
                vmem((2, halo + 1, sub, LANES), F32),
                vmem((2, halo, sub, LANES), F32),
                vmem((2, halo, sub, LANES), F32),
                vmem((2, halo, sub, LANES), F32),
                vmem((2, 2 * chunks, band, sub, LANES), F32),
                vmem((2, chunks, band, wide, LANES), F32),
                vmem((2, 2 * chunks, 2, sub, LANES), BF16),
                vmem((2, chunks, 2, 2, sub, LANES), BF16),
                vmem((2, 2, 16, LANES), F32),
                vmem((2, 2, 16, LANES), F32),
                vmem((2, SWEEPS - 1, chunks, band, wide, LANES), BF16),
                vmem((2, SWEEPS - 1, chunks, band, wide, LANES), BF16),
                vmem((chunks, sub, sub, LANES), F32),
                dma, dma, dma, dma((chunks,)), dma, dma, dma, dma, dma, dma,
                dma((2,)), dma((2, chunks)), dma((2,)), dma((2,)), dma((2, chunks, 2)), dma,
            ],
            compiler_params=pltpu.CompilerParams(collective_id=0, has_side_effects=True,
                                                 vmem_limit_bytes=61000 * 1024),
        )(omega_relax.reshape(1), f_blk, u_blk, kappa_blk, mat_blk[0, 0].T)

    return jax.shard_map(device_fn, mesh=mesh,
                         in_specs=(grid_spec, grid_spec, P('row', 'col'), P('row', 'col', None, None), P()),
                         out_specs=grid_spec, check_vma=False)
```

```python
import functools
import math

import jax
import jax.numpy as jnp
from jax import lax
from jax.experimental import pallas as pl
from jax.experimental.pallas import tpu as pltpu
from jax.sharding import PartitionSpec as P

SWEEPS = 6
LANES = 128
MESH = pl.DeviceIdType.MESH
F32 = jnp.float32
BF16 = jnp.bfloat16


def kernel(row_count, sub, halo, chunks,
           om_ref, f_hbm, u_hbm, kap_hbm, mat_hbm, out_ref,
           u_sc, r_sc, v_sc, e_late, e_early, acc, m_raw, m_turn, m_perm,
           k_raw, kb, ko, fv, fw, fe, dg, u_band, pv, pw, pe, pd, i_send, i_recv, n_send, n_recv, a_send, a_recv,
           z_send, z_recv, u_fin,
           load_sem, band_sem, pair_send, pair_recv, mat_sem, mat_send, mat_recv, kap_loc, kap_send, kap_recv,
           ici_sem, ir_sem, far_sem, ar_sem, zr_sem, out_recv):
    wide = 2 * sub
    ext = sub + 2 * halo
    band = halo + 1
    late_k = 2 * band * 32
    early_rows = e_early.shape[0]
    half = chunks * LANES
    left = 8

    row = lax.axis_index('row')
    col = lax.axis_index('col')
    other = 1 - col
    mine = lax.rem(row + col, 2)
    theirs = 1 - mine
    has_up = row > 0
    has_dn = row < row_count - 1
    ways = ((0, has_up, jnp.maximum(row - 1, 0)), (1, has_dn, jnp.minimum(row + 1, row_count - 1)))
    up_row, dn_row = ways[0][2], ways[1][2]
    col_spans = [pl.ds(side * sub, sub) for side in range(2)]
    my_cols = pl.ds(pl.multiple_of(col * sub, 8), sub)
    other_cols = pl.ds(pl.multiple_of(other * sub, 8), sub)
    own_rows = pl.ds(halo, sub)

    def lanes_of(which, ch):
        return pl.ds(pl.multiple_of(which * half + ch * LANES, LANES), LANES)

    def local_bytes(ref, sem):
        return pltpu.make_async_copy(ref, ref, sem)

    def remote_bytes(ref, send_sem, recv_sem):
        return pltpu.make_async_remote_copy(src_ref=ref, dst_ref=ref, send_sem=send_sem, recv_sem=recv_sem,
                                            device_id=(other, row), device_id_type=MESH)

    barrier = pltpu.get_barrier_semaphore()

    def in_lanes(ch):
        return slice(ch * LANES, (ch + 1) * LANES)

    def greet(r_to, c_to):
        pl.semaphore_signal(barrier, inc=1, device_id=(c_to, r_to), device_id_type=MESH)

    for _, present, r_to in ways:
        @pl.when(present)
        def _():
            greet(r_to, col)
            greet(r_to, other)
    greet(row, other)

    kap_load = pltpu.make_async_copy(kap_hbm, k_raw.at[col], kap_loc)
    kap_load.start()

    def band_loads(way, g):
        lanes = pl.ds(g * LANES, LANES)
        u_from = pl.ds(0 if way == 0 else sub - band, band)
        f_from = pl.ds(0 if way == 0 else sub - halo, halo)
        return (pltpu.make_async_copy(u_hbm.at[u_from, :, lanes], u_band.at[way, g, :, 8:8 + sub, :],
                                      band_sem),
                pltpu.make_async_copy(f_hbm.at[f_from, :, lanes], i_send.at[way, g, pl.ds(1 - way, halo)],
                                      band_sem))

    for g in range(2 * chunks):
        for way in range(2):
            for load in band_loads(way, g):
                load.start()

    def u_load(ch):
        return pltpu.make_async_copy(u_hbm.at[:, :, lanes_of(mine, ch)], u_sc.at[ch, :, my_cols, :], load_sem)

    def f_load(ch):
        return pltpu.make_async_copy(f_hbm.at[:, :, lanes_of(mine, ch)], r_sc.at[ch, own_rows, my_cols, :],
                                     load_sem)

    mat_load = pltpu.make_async_copy(mat_hbm, m_raw.at[col], mat_sem)
    mat_load.start()
    for ch in range(chunks):
        u_load(ch).start()
        f_load(ch).start()

    def u_pair(ch, cols):
        return pltpu.make_async_remote_copy(
            src_ref=u_hbm.at[:, :, lanes_of(theirs, ch)], dst_ref=u_sc.at[ch, :, cols, :],
            send_sem=pair_send, recv_sem=pair_recv.at[ch],
            device_id=(other, row), device_id_type=MESH)

    def f_pair(ch, cols):
        return pltpu.make_async_remote_copy(
            src_ref=f_hbm.at[:, :, lanes_of(theirs, ch)], dst_ref=r_sc.at[ch, own_rows, cols, :],
            send_sem=pair_send, recv_sem=pair_recv.at[ch],
            device_id=(other, row), device_id_type=MESH)

    def mat_pair(slot):
        return pltpu.make_async_remote_copy(
            src_ref=mat_hbm, dst_ref=m_raw.at[slot],
            send_sem=mat_send, recv_sem=mat_recv,
            device_id=(other, row), device_id_type=MESH)

    def kap_pair(slot):
        return pltpu.make_async_remote_copy(
            src_ref=k_raw.at[col], dst_ref=k_raw.at[slot],
            send_sem=kap_send, recv_sem=kap_recv,
            device_id=(other, row), device_id_type=MESH)

    def half_at(core):
        return lax.rem(core + row + 1, 2)

    near_rows = (pl.ds(0, 2), pl.ds(2, 2))
    far_rows = (pl.ds(2, 2), pl.ds(0, 2))

    def init_send(way, r_to, core, ch, rows, recv_sem):
        g = half_at(core) * chunks + ch
        return pltpu.make_async_remote_copy(
            src_ref=i_send.at[way, g, rows], dst_ref=i_recv.at[way, ch, rows, my_cols, :],
            send_sem=ici_sem.at[way], recv_sem=recv_sem,
            device_id=(core, r_to), device_id_type=MESH)

    def narrow_send(way, r_to, core, ch):
        return pltpu.make_async_remote_copy(
            src_ref=n_send.at[way, half_at(core) * chunks + ch], dst_ref=n_recv.at[way, ch, col],
            send_sem=ici_sem.at[way], recv_sem=ir_sem.at[way, ch],
            device_id=(core, r_to), device_id_type=MESH)

    def aux_send(way, r_to, core):
        return pltpu.make_async_remote_copy(
            src_ref=a_send.at[way, half_at(core)], dst_ref=a_recv.at[way, col],
            send_sem=ici_sem.at[way], recv_sem=ar_sem.at[way],
            device_id=(core, r_to), device_id_type=MESH)

    def z_copy(t, ch, way, r_to):
        return pltpu.make_async_remote_copy(
            src_ref=z_send.at[way, t, ch], dst_ref=z_recv.at[way, t, ch],
            send_sem=ici_sem.at[way], recv_sem=zr_sem.at[t % 2, ch, way],
            device_id=(other, r_to), device_id_type=MESH)

    omega = om_ref[0]
    for way in range(2):
        for g in range(2 * chunks):
            u_band[way, g, :, 0:8] = jnp.zeros((band, 8, LANES), F32)
            u_band[way, g, :, 8 + sub:16 + sub] = jnp.zeros((band, 8, LANES), F32)
        for h in range(2):
            a_send[way, h] = jnp.zeros((16, LANES), F32)

    eye = lax.broadcasted_iota(jnp.int32, (sub, sub), 0) == lax.broadcasted_iota(jnp.int32, (sub, sub), 1)

    def spread(line):
        picked = jnp.where(eye, jnp.broadcast_to(line, (sub, sub)), 0.0)
        return jnp.broadcast_to(jnp.sum(picked, axis=1, keepdims=True), (sub, LANES))

    kap_load.wait()
    for k in range(sub):
        line = spread(k_raw[col, k:k + 1, :])
        ko[k, 8:8 + sub] = line
        ko[k, 7:8] = line[0:1]
        ko[k, 8 + sub:9 + sub] = line[sub - 1:sub]
    spot_col = lax.broadcasted_iota(jnp.int32, (sub, LANES), 0)
    cut_w = (spot_col == 0) & (col == 1)
    cut_e = (spot_col == sub - 1) & (col == 0)
    for way in range(2):
        first = 0 if way == 0 else sub - halo
        for k in range(halo):
            at = first + k
            mid = ko[at, 8:8 + sub]
            pw[way, k] = jnp.where(cut_w, 0.0, 0.5 * (mid + ko[at, 7:7 + sub]))
            pe[way, k] = jnp.where(cut_e, 0.0, 0.5 * (ko[at, 9:9 + sub] + mid))
            total = pw[way, k] + pe[way, k]
            if at > 0:
                pv[way, k] = 0.5 * (mid + ko[at - 1, 8:8 + sub])
                total = total + pv[way, k]
            if at < sub - 1:
                pv[way, k + 1] = 0.5 * (ko[at + 1, 8:8 + sub] + mid)
                total = total + pv[way, k + 1]
            pd[way, k] = total

    local_bytes(v_sc.at[0, 0:21], band_sem).wait()
    for way in range(2):
        for h in range(2):
            first = 0 if way == 0 else sub - band
            a_send[way, h, 12:12 + band, 0:sub] = k_raw[col, first:first + band]
    for g in range(2 * chunks):
        h, ch = g // chunks, g % chunks
        for way in range(2):
            shift = way
            for k in range(halo):
                line = shift + k
                at = k + 1 - way
                au = (pd[way, k] * u_band[way, g, line, 8:8 + sub]
                      - pw[way, k] * u_band[way, g, line, 7:7 + sub]
                      - pe[way, k] * u_band[way, g, line, 9:9 + sub])
                if line > 0:
                    au = au - pv[way, k] * u_band[way, g, line - 1, 8:8 + sub]
                if line < band - 1:
                    au = au - pv[way, k + 1] * u_band[way, g, line + 1, 8:8 + sub]
                part = i_send[way, g, at] - au
                i_send[way, g, at] = part
                edge = jnp.where(col == 0, u_band[way, g, line, 7 + sub:8 + sub], u_band[way, g, line, 8:9])
                slot = 5 * ch + k
                a_send[way, h, slot:slot + 1] = edge
                far = k - 1 + way
                if 0 <= far < 2:
                    n_send[way, g, far] = part.astype(BF16)
                    slot = 5 * ch + halo + far
                    a_send[way, h, slot:slot + 1] = jnp.where(col == 0, part[sub - 1:sub], part[0:1])
            i_send[way, g, halo * way] = u_band[way, g, halo * way, 8:8 + sub]

    pl.semaphore_wait(barrier, 1 + 2 * has_up.astype(jnp.int32) + 2 * has_dn.astype(jnp.int32))

    for way, present, r_to in ways:
        @pl.when(present)
        def _():
            def near(core, ch):
                init_send(way, r_to, core, ch, near_rows[way], ir_sem.at[way, ch]).start()
                narrow_send(way, r_to, core, ch).start()

            def far(core, ch, n):
                rows = pl.ds((2, 0)[way] + n, 1)
                init_send(way, r_to, core, ch, rows, far_sem.at[way]).start()

            first, second = way, 1 - way
            aux_send(way, r_to, first).start()
            for ch in range(chunks):
                near(first, ch)
            far(first, 0, 0)
            aux_send(way, r_to, second).start()
            for ch in range(chunks):
                near(second, ch)
            far(first, 0, 1)
            for ch in range(1, chunks):
                far(first, ch, 0)
                far(first, ch, 1)
            for ch in range(chunks):
                far(second, ch, 0)
                far(second, ch, 1)
    kap_pair(col).start()
    u_pair(0, my_cols).start()
    f_pair(0, my_cols).start()
    mat_pair(col).start()
    for ch in range(1, chunks):
        u_pair(ch, my_cols).start()
        f_pair(ch, my_cols).start()

    def clear(ch, carry):
        for i in list(range(band)) + list(range(band + sub, ext + 2)):
            v_sc[ch, i] = jnp.zeros(v_sc.shape[2:], F32)
        for i in range(band, band + sub):
            v_sc[ch, i, 0:8] = jnp.zeros((8, LANES), F32)
            v_sc[ch, i, 8 + wide:16 + wide] = jnp.zeros((8, LANES), F32)
        return carry
    lax.fori_loop(0, chunks, clear, 0)
    e_early[sub - 2:early_rows] = jnp.zeros((early_rows - sub + 2, wide, half), BF16)

    ext_cells = m_raw.shape[1]
    tile = 256
    lines_per_tile = tile // 32

    def permute(side):
        m_turn[:, 896:1024] = jnp.zeros((sub * sub, 128), BF16)
        m_turn[:, 0:ext_cells] = m_raw[side].T
        for n_tile in range(m_perm.shape[2] // tile):
            if n_tile == 0:
                spans = [(0, 128), (768, 1024)]
            else:
                first = band + lines_per_tile * (n_tile - 1)
                last = min(first + lines_per_tile, ext - band)
                spans = [(first * ext // 128 * 128, -(-last * ext // 128) * 128)]
            n_at = n_tile * tile + lax.broadcasted_iota(jnp.int32, (1, tile), 1)
            q = lax.shift_right_logical(n_at, 5)
            j = lax.bitwise_and(n_at, 31)
            line = jnp.where(q < band, q, jnp.where(q < 2 * band, q + (ext - 2 * band), q - band))
            ext_col = j + (halo - 8 * side)
            ok = (q < ext) & (ext_col >= 0) & (ext_col < ext)
            want = jnp.where(ok, line * ext + ext_col, -1)
            moved = None
            for lo, hi in spans:
                spot = lo + lax.broadcasted_iota(jnp.int32, (hi - lo, tile), 0)
                pick = jnp.where(spot == want, 1.0, 0.0).astype(BF16)
                part = jnp.dot(m_turn[:, lo:hi], pick, preferred_element_type=F32)
                moved = part if moved is None else moved + part
            m_perm[side, :, n_tile * tile:(n_tile + 1) * tile] = moved.astype(BF16)

    mat_load.wait()
    permute(col)

    kap_pair(other).wait_recv()

    def put_rows(take, at, count):
        for k in range(count):
            for side in range(2):
                line = spread(take(side, k))
                kb[at + k, left + side * sub:left + (side + 1) * sub] = line
                if side == 0:
                    kb[at + k, left - 1:left] = line[0:1]
                else:
                    kb[at + k, left + wide:left + wide + 1] = line[sub - 1:sub]

    def side_faces(e):
        k_mid = kb[e + 1, left:left + wide]
        fw[e] = 0.5 * (k_mid + kb[e + 1, left - 1:left + wide - 1])
        fe[e] = 0.5 * (kb[e + 1, left + 1:left + wide + 1] + k_mid)

    def diag_row(e):
        dg[e] = fv[e] + fv[e + 1] + fw[e] + fe[e]

    def face_row(i):
        fv[i] = 0.5 * (kb[i + 1, left:left + wide] + kb[i, left:left + wide])

    put_rows(lambda side, k: k_raw[side, k:k + 1, :], band, sub)
    fv[halo] = jnp.zeros((wide, LANES), F32)
    fv[halo + sub] = jnp.zeros((wide, LANES), F32)

    def own_face(i, carry):
        face_row(i)
        return carry
    lax.fori_loop(halo + 1, halo + sub, own_face, 0)

    def own_side(e, carry):
        side_faces(e)
        diag_row(e)
        return carry
    lax.fori_loop(halo, halo + sub, own_side, 0)

    def stencil(ch, e, n):
        rows = pl.ds(e, n)
        mid = pl.ds(e + 1, n)
        return (dg[rows] * v_sc[ch, mid, left:left + wide]
                - fv[rows] * v_sc[ch, pl.ds(e, n), left:left + wide]
                - fv[mid] * v_sc[ch, pl.ds(e + 2, n), left:left + wide]
                - fw[rows] * v_sc[ch, mid, left - 1:left + wide - 1]
                - fe[rows] * v_sc[ch, mid, left + 1:left + wide + 1])

    local_bytes(u_sc, load_sem).wait()

    def first_residual(ch):
        remote_bytes(u_fin, pair_send, pair_recv.at[ch]).wait_recv()

        def fill(i, c):
            rows = pl.ds(i * 6, 6)
            v_sc[ch, pl.ds(i * 6 + band, 6), left:left + wide] = u_sc[ch, rows]
            return c
        lax.fori_loop(0, sub // 6, fill, 0)

        def part(i, c):
            rows = pl.ds(halo + i * 6, 6)
            r_sc[ch, rows] = r_sc[ch, rows] - stencil(ch, halo + i * 6, 6)
            return c
        lax.fori_loop(0, sub // 6, part, 0)
        group = (sub - 2) // 2

        def to_e(i, c):
            e_early[pl.ds(i * group, group), :, in_lanes(ch)] = r_sc[ch, pl.ds(i * group + band, group)].astype(BF16)
            return c
        lax.fori_loop(0, 2, to_e, 0)

    first_residual(0)

    mat_pair(other).wait_recv()
    permute(other)

    for ch in range(1, chunks):
        first_residual(ch)

    def early_dot():
        for side in range(2):
            operand = e_early[:, 16 * side:16 * side + 32, :].reshape(early_rows * 32, half)
            acc[side] = jnp.dot(m_perm[side, :, late_k:late_k + early_rows * 32], operand,
                                preferred_element_type=F32)

    early_dot()

    for way, present, r_to in ways:
        @pl.when(present)
        def _():
            remote_bytes(a_recv.at[1 - way], ici_sem.at[way], ar_sem.at[1 - way]).wait_recv()
            put_rows(lambda side, k: a_recv[1 - way, side, 12 + k:13 + k, 0:sub], 0 if way == 0 else band + sub, band)

        @pl.when(jnp.logical_not(present))
        def _():
            for side in range(2):
                a_recv[1 - way, side] = jnp.zeros((16, LANES), F32)
            for i in range(band):
                if way == 0:
                    kb[i] = kb[band]
                else:
                    kb[band + sub + i] = kb[band + sub - 1]

    for i in range(halo + 1):
        face_row(i)
        face_row(halo + sub + i)
    for i in range(halo):
        side_faces(i)
        side_faces(halo + sub + i)
    for i in range(halo + 1):
        diag_row(i)
        diag_row(ext - 1 - i)

    def side_flux(sent, ch, k, e):
        slot = pl.ds(5 * ch + k, 1)
        return fe[e, sub - 1:sub] * (a_recv[sent, 1, slot] - a_recv[sent, 0, slot])

    def near_far(way):
        if way == 0:
            return (halo - 1, halo - 1), ((0, 0), (1, 1))
        return (halo + sub, 0), ((halo + sub + 1, 1), (halo + sub + 2, 2))

    wide_col = lax.broadcasted_iota(jnp.int32, (wide, LANES), 0)

    def late_first(ch):
        for way, present, r_to in ways:
            sent = 1 - way
            (e_near, k_near), far = near_far(way)
            near_at, u_at = (2, 3) if way == 0 else (1, 0)

            @pl.when(present)
            def _():
                remote_bytes(i_recv.at[sent, ch, 0:3], ici_sem.at[way], ir_sem.at[sent, ch]).wait_recv()
                r_sc[ch, e_near] = i_recv[sent, ch, near_at]
                flux = side_flux(sent, ch, k_near, e_near)
                r_sc[ch, e_near, sub - 1:sub] = r_sc[ch, e_near, sub - 1:sub] + flux
                r_sc[ch, e_near, sub:sub + 1] = r_sc[ch, e_near, sub:sub + 1] - flux
                for n in range(2):
                    e, k = far[n]
                    flux = side_flux(sent, ch, k, e)
                    slot = pl.ds(5 * ch + halo + n, 1)
                    got = jnp.concatenate([n_recv[sent, ch, side, n].astype(F32) for side in range(2)], axis=0)
                    got = jnp.where(wide_col == sub - 1, a_recv[sent, 0, slot] + flux, got)
                    got = jnp.where(wide_col == sub, a_recv[sent, 1, slot] - flux, got)
                    e_late[e if way == 0 else e - (ext - 2 * band), :, in_lanes(ch)] = got.astype(BF16)

            @pl.when(jnp.logical_not(present))
            def _():
                i_recv[sent, ch, u_at] = jnp.zeros((wide, LANES), F32)
                rows = pl.ds(0 if way == 0 else halo + sub, halo)
                r_sc[ch, rows] = jnp.zeros((halo, wide, LANES), F32)
                rows = pl.ds(0 if way == 0 else 2 * band - 2, 2)
                e_late[rows, :, in_lanes(ch)] = jnp.zeros((2, wide, LANES), BF16)

            face, e_own, own_line = (halo, halo, 0) if way == 0 else (halo + sub, halo + sub - 1, sub - 1)
            flux = fv[face] * (i_recv[sent, ch, u_at] - u_sc[ch, own_line])
            near = r_sc[ch, e_near] - flux
            own = r_sc[ch, e_own] + flux
            r_sc[ch, e_near] = near
            r_sc[ch, e_own] = own
            e_late[halo - 1 if way == 0 else band + 1, :, in_lanes(ch)] = near.astype(BF16)
            e_late[halo if way == 0 else band, :, in_lanes(ch)] = own.astype(BF16)

    def far_wait():
        for way, present, r_to in ways:
            @pl.when(present)
            def _():
                remote_bytes(i_recv.at[1 - way, :, 0:2], ici_sem.at[way], far_sem.at[1 - way]).wait_recv()

    def far_residual():
        for way, present, r_to in ways:
            sent = 1 - way
            _, far = near_far(way)

            @pl.when(present)
            def _():
                for ch in range(chunks):
                    for n in range(2):
                        e, k = far[n]
                        flux = side_flux(sent, ch, k, e)
                        r_sc[ch, e] = i_recv[sent, ch, n + 2 * way]
                        r_sc[ch, e, sub - 1:sub] = r_sc[ch, e, sub - 1:sub] + flux
                        r_sc[ch, e, sub:sub + 1] = r_sc[ch, e, sub:sub + 1] - flux

    def update(ch, e, n):
        r_new = r_sc[ch, pl.ds(e, n)] - omega * stencil(ch, e, n)
        r_sc[ch, pl.ds(e, n)] = r_new
        return r_new

    slow = lax.rem(row, 2)

    def towards(way):
        return jnp.where(way == 0, has_up, has_dn), jnp.where(way == 0, up_row, dn_row)

    def late_part(t, ch, way):
        present, r_to = towards(way)

        @pl.when(present)
        def _():
            z_copy(t, ch, 1 - way, r_to).wait_recv()
            v_sc[ch, pl.ds(way * (band + sub), band), left:left + wide] = z_recv[1 - way, t, ch].astype(F32)

        e_late[pl.ds(way * band, band), :, in_lanes(ch)] = update(ch, way * (ext - band), band).astype(BF16)

    def late_next(t, ch):
        late_part(t, ch, 1 - slow)
        first = slow * (sub - band)
        rows = pl.ds(pl.multiple_of(first * sub, 32), band * sub)
        for side in range(2):
            acc[side, rows, in_lanes(ch)] = solve(in_lanes(ch), side, first, band, 1 - slow).reshape(band * sub, LANES)
        late_part(t, ch, slow)

    def solve(lanes, side, first, count, only=None):
        n = count * sub
        rows = pl.ds(first * sub if isinstance(first, int) else pl.multiple_of(first * sub, 32), n)
        cols = pl.ds(pl.multiple_of(16 * side, 16), 32)
        lines = slice(None) if only is None else pl.ds(only * band, band)
        depth = late_k if only is None else late_k // 2
        at = 0 if only is None else pl.multiple_of(only * depth, depth)
        operand = e_late[lines, cols, lanes]
        width = operand.shape[2]
        part = acc[side, rows, lanes] + jnp.dot(m_perm[side, rows, pl.ds(at, depth)],
                                                     operand.reshape(depth, width), preferred_element_type=F32)
        return part.reshape(count, sub, width)

    def solve_rows(lanes, first, count, only=None):
        return jnp.concatenate([solve(lanes, side, first, count, only) for side in range(2)], axis=1).astype(BF16)

    def keep_z(ch, first, count, z_bf):
        v_sc[ch, pl.ds(band + first, count), left:left + wide] = z_bf.astype(F32)

    def solve_and_send(t, ch, left_way):
        for n, way in enumerate((slow, 1 - slow)):
            present, r_to = towards(way)
            first = way * (sub - band)
            z_bf = solve_rows(in_lanes(ch), first, band, left_way if n == 0 else None)
            z_send[way, t, ch] = z_bf

            @pl.when(present)
            def _():
                z_copy(t, ch, way, r_to).start()

            keep_z(ch, first, band, z_bf)

    def interior():
        z_mid = solve_rows(slice(0, half), band, sub - 2 * band)
        for ch in range(chunks):
            keep_z(ch, band, sub - 2 * band, z_mid[:, :, in_lanes(ch)])
        group = (sub - 2) // 2
        for ch in range(chunks):
            def inner(i, c):
                e_early[pl.ds(i * group, group), :, in_lanes(ch)] = update(ch, band + i * group, group).astype(BF16)
                return c
            lax.fori_loop(0, 2, inner, 0)

            def add(i, c):
                rows = pl.ds(i * 6, 6)
                u_sc[ch, rows] = u_sc[ch, rows] + omega * v_sc[ch, pl.ds(i * 6 + band, 6), left:left + wide]
                return c
            lax.fori_loop(0, sub // 6, add, 0)
        early_dot()

    for ch in range(chunks):
        late_first(ch)
        solve_and_send(0, ch, None)
    interior()

    def sweep_next(t, carry):
        @pl.when(t == 0)
        def _():
            far_wait()
            far_residual()
        for ch in range(chunks):
            late_next(t, ch)
            solve_and_send(t + 1, ch, slow)
        interior()
        return carry
    lax.fori_loop(0, SWEEPS - 2, sweep_next, 0)

    cuts = (0, 16, sub)

    def out_pair(ch, n, which):
        rows = pl.ds(cuts[n], cuts[n + 1] - cuts[n])
        return pltpu.make_async_remote_copy(
            src_ref=u_fin.at[ch, rows], dst_ref=out_ref.at[rows, :, lanes_of(which, ch)],
            send_sem=pair_send, recv_sem=out_recv,
            device_id=(other, row), device_id_type=MESH)

    for ch in range(chunks):
        late_part(SWEEPS - 2, ch, 1 - slow)
    for side in range(2):
        acc[side] = solve(slice(0, half), side, 0, sub, 1 - slow).reshape(sub * sub, half)
    for ch in range(chunks):
        late_part(SWEEPS - 2, ch, slow)
        for n in range(2):
            first, past = cuts[n], cuts[n + 1]
            z = solve(in_lanes(ch), other, first, past - first, slow).astype(BF16).astype(F32)
            u_fin[ch, first:past] = u_sc[ch, first:past, other_cols] + omega * z
            out_pair(ch, n, mine).start()
    z_own = solve(slice(0, half), col, 0, sub, slow).astype(BF16).astype(F32)
    for ch in range(chunks):
        out_ref[:, :, lanes_of(mine, ch)] = u_sc[ch, :, my_cols] + omega * z_own[:, :, in_lanes(ch)]

    kap_pair(col).wait_send()
    mat_pair(col).wait_send()
    for way, present, r_to in ways:
        @pl.when(present)
        def _():
            remote_bytes(v_sc.at[0, 0:23], ici_sem.at[way], ar_sem.at[way]).wait_send()
    remote_bytes(u_fin, pair_send, out_recv).wait_recv()
    remote_bytes(v_sc.at[:, 0:27], pair_send, out_recv).wait_send()


def solution(mesh):
    row_count = mesh.shape['row']
    grid_spec = P('row', 'col', None)

    def device_fn(f_blk, u_blk, kappa_blk, mat_blk, omega_relax):
        sub, _, rhs = u_blk.shape
        ext_cells = mat_blk.shape[3]
        ext = math.isqrt(ext_cells)
        halo = (ext - sub) // 2
        band = halo + 1
        chunks = rhs // (2 * LANES)
        wide = 2 * sub
        early_rows = 24
        hbm = pl.BlockSpec(memory_space=pl.ANY)
        vmem = pltpu.VMEM
        dma = pltpu.SemaphoreType.DMA
        return pl.pallas_call(
            functools.partial(kernel, row_count, sub, halo, chunks),
            out_shape=pltpu.VMEM(u_blk.shape, F32),
            in_specs=[pl.BlockSpec(memory_space=pltpu.SMEM), hbm, hbm, hbm, hbm],
            out_specs=pl.BlockSpec(memory_space=pltpu.VMEM),
            scratch_shapes=[
                vmem((chunks, sub, wide, LANES), F32),
                vmem((chunks, ext, wide, LANES), F32),
                vmem((chunks, ext + 2, 64, LANES), F32),
                vmem((2 * band, wide, chunks * LANES), BF16),
                vmem((early_rows, wide, chunks * LANES), BF16),
                vmem((2, sub * sub, chunks * LANES), F32),
                vmem((2, ext_cells, sub * sub), BF16),
                vmem((sub * sub, 1024), BF16),
                vmem((2, sub * sub, 1024), BF16),
                vmem((2, sub, sub), F32),
                vmem((ext + 2, 64, LANES), F32),
                vmem((sub, 40, LANES), F32),
                vmem((ext + 1, wide, LANES), F32),
                vmem((ext, wide, LANES), F32),
                vmem((ext, wide, LANES), F32),
                vmem((ext, wide, LANES), F32),
                vmem((2, 2 * chunks, band, 40, LANES), F32),
                vmem((2, halo + 1, sub, LANES), F32),
                vmem((2, halo, sub, LANES), F32),
                vmem((2, halo, sub, LANES), F32),
                vmem((2, halo, sub, LANES), F32),
                vmem((2, 2 * chunks, band, sub, LANES), F32),
                vmem((2, chunks, band, wide, LANES), F32),
                vmem((2, 2 * chunks, 2, sub, LANES), BF16),
                vmem((2, chunks, 2, 2, sub, LANES), BF16),
                vmem((2, 2, 16, LANES), F32),
                vmem((2, 2, 16, LANES), F32),
                vmem((2, SWEEPS - 1, chunks, band, wide, LANES), BF16),
                vmem((2, SWEEPS - 1, chunks, band, wide, LANES), BF16),
                vmem((chunks, sub, sub, LANES), F32),
                dma, dma, dma, dma((chunks,)), dma, dma, dma, dma, dma, dma,
                dma((2,)), dma((2, chunks)), dma((2,)), dma((2,)), dma((2, chunks, 2)), dma,
            ],
            compiler_params=pltpu.CompilerParams(collective_id=0, has_side_effects=True,
                                                 vmem_limit_bytes=61000 * 1024),
        )(omega_relax.reshape(1), f_blk, u_blk, kappa_blk, mat_blk[0, 0].T)

    return jax.shard_map(device_fn, mesh=mesh,
                         in_specs=(grid_spec, grid_spec, P('row', 'col'), P('row', 'col', None, None), P()),
                         out_specs=grid_spec, check_vma=False)
```
